8 devices in a mesh: rep: 1 (over z), kv: 8 (over y, x, core).
Axes of the slice: x: 2, y: 2, z: 1, core: 2. Of those that a mesh axis runs over, the one named last changes fastest.
Arguments:
- embeds: bfloat16 [2, 512, 4096], P(None, ('rep', 'kv'))
- w_query: bfloat16 [2, 4096, 4096], replicated
- w_key: bfloat16 [2, 4096, 1024], replicated
- w_value: bfloat16 [2, 4096, 1024], replicated
- w_out: bfloat16 [2, 4096, 4096], replicated
- w_up: bfloat16 [2, 4096, 14336], replicated
- w_down: bfloat16 [2, 14336, 4096], replicated
- k_pool: bfloat16 [1536, 2, 16, 8, 128], P(('rep', 'kv'))
- v_pool: bfloat16 [1536, 2, 16, 8, 128], P(('rep', 'kv'))
- new_table: int32 [512, 2], P('rep')
- seq_lens: int32 [512], P('rep')
- mig_src: int32 [64], P('rep')
- mig_dst: int32 [64], P('rep')
Outputs:
- output 1: bfloat16 [2, 512, 4096], P(None, ('rep', 'kv'))
- output 2: bfloat16 [1536, 2, 16, 8, 128], P(('rep', 'kv'))
- output 3: bfloat16 [1536, 2, 16, 8, 128], P(('rep', 'kv'))
All inputs are finite; a program needn't handle non-finite values.
Results may differ from the reference program's by a relative error of at most 0.0168677.
Values are sent between devices in bfloat16 or wider.
A program may use at most 2.75 GiB of HBM per device.

```python
import jax
import jax.numpy as jnp
from jax import lax

D = 4096
HEADS = 32
KV_HEADS = 8
HEAD = 128
FF = 14336
PAGE = 16
LAYERS = 2
GROUP = 8
SEQ_DEV = 64
PAGES_SEQ = 2
MIG = 64
BATCH = GROUP * SEQ_DEV
SLOTS = PAGES_SEQ * SEQ_DEV + MIG


def draw_layout(layout_key):
    key_hot, key_shift, key_perm, key_rank, key_len = jax.random.split(layout_key, 5)
    hot_dev = jax.random.randint(key_hot, (), 0, GROUP)
    alt_dev = (hot_dev + GROUP // 2) % GROUP
    dev_shift = jax.random.randint(key_shift, (), 0, GROUP)
    slot_perm = jax.vmap(lambda sub_key: jax.random.permutation(sub_key, SLOTS))(jax.random.split(key_perm, GROUP))
    seq_ids = jnp.arange(BATCH)[:, None]
    page_ids = jnp.arange(PAGES_SEQ)[None, :]
    home_dev = seq_ids // SEQ_DEV
    base_dev = (home_dev + page_ids + dev_shift) % GROUP
    base_local = slot_perm[base_dev, page_ids * SEQ_DEV + seq_ids % SEQ_DEV]
    new_table = (base_dev * SLOTS + base_local).astype(jnp.int32)
    eligible = (base_dev != hot_dev) & (base_dev != alt_dev)
    is_last = jnp.broadcast_to(page_ids == PAGES_SEQ - 1, (BATCH, PAGES_SEQ))
    total_pages = BATCH * PAGES_SEQ
    rank_ids = jax.random.permutation(key_rank, total_pages).reshape(BATCH, PAGES_SEQ)
    priority = jnp.where(eligible, jnp.where(is_last, 0, total_pages), 2 * total_pages) + rank_ids
    chosen = jnp.argsort(priority.reshape(-1))[:MIG]
    entry_ids = jnp.arange(MIG)
    src_dev = jnp.where(entry_ids % 8 == 7, alt_dev, hot_dev)
    src_local = slot_perm[src_dev, PAGES_SEQ * SEQ_DEV + entry_ids]
    mig_src = (src_dev * SLOTS + src_local).astype(jnp.int32)
    mig_dst = new_table.reshape(-1)[chosen]
    len_offsets = jax.random.randint(key_len, (BATCH,), 0, PAGE - 1)
    len_offsets = len_offsets.at[0].set(PAGE - 2).at[1].set(0)
    seq_lens = ((PAGES_SEQ - 1) * PAGE + len_offsets).astype(jnp.int32)
    return new_table, seq_lens, mig_src, mig_dst


def setup_inputs(seed: int = 0, part: int = 0) -> dict:
    base_key = jax.random.key(seed)
    part_key = jax.random.fold_in(base_key, part)
    w_keys = jax.random.split(base_key, 6)
    p_keys = jax.random.split(part_key, 5)
    new_table, seq_lens, mig_src, mig_dst = draw_layout(p_keys[0])
    embeds = jax.random.normal(p_keys[1], (2, BATCH, D), jnp.float32).astype(jnp.bfloat16)
    out_scale = (PAGES_SEQ / (HEADS * HEAD)) ** 0.5
    w_query = (jax.random.normal(w_keys[0], (LAYERS, D, HEADS * HEAD), jnp.float32) * 0.5 * D ** -0.5).astype(jnp.bfloat16)
    w_key = (jax.random.normal(w_keys[1], (LAYERS, D, KV_HEADS * HEAD), jnp.float32) * D ** -0.5).astype(jnp.bfloat16)
    w_value = (jax.random.normal(w_keys[2], (LAYERS, D, KV_HEADS * HEAD), jnp.float32) * D ** -0.5).astype(jnp.bfloat16)
    w_out = (jax.random.normal(w_keys[3], (LAYERS, HEADS * HEAD, D), jnp.float32) * out_scale).astype(jnp.bfloat16)
    w_up = (jax.random.normal(w_keys[4], (LAYERS, D, FF), jnp.float32) * D ** -0.5).astype(jnp.bfloat16)
    w_down = (jax.random.normal(w_keys[5], (LAYERS, FF, D), jnp.float32) * FF ** -0.5).astype(jnp.bfloat16)
    pool_shape = (GROUP * SLOTS, LAYERS, PAGE, KV_HEADS, HEAD)
    k_pool = jax.random.normal(p_keys[2], pool_shape, jnp.float32).astype(jnp.bfloat16)
    slot_mean = jax.random.normal(p_keys[3], (GROUP * SLOTS, LAYERS, 1, KV_HEADS, HEAD), jnp.float32)
    v_pool = (0.5 * jax.random.normal(p_keys[4], pool_shape, jnp.float32) + slot_mean).astype(jnp.bfloat16)
    return {'embeds': embeds, 'w_query': w_query, 'w_key': w_key, 'w_value': w_value, 'w_out': w_out, 'w_up': w_up, 'w_down': w_down, 'k_pool': k_pool, 'v_pool': v_pool, 'new_table': new_table, 'seq_lens': seq_lens, 'mig_src': mig_src, 'mig_dst': mig_dst}


def attend_all(queries, k_layer, v_layer, new_table, seq_lens, step_idx):
    group_heads = HEADS // KV_HEADS
    positions = jnp.arange(PAGES_SEQ)[:, None] * PAGE + jnp.arange(PAGE)[None, :]

    def one_seq(args):
        q_row, row_slots, seq_len = args
        keys_f = k_layer[row_slots].astype(jnp.float32)
        vals_f = v_layer[row_slots].astype(jnp.float32)
        q_grp = q_row.astype(jnp.float32).reshape(KV_HEADS, group_heads, HEAD)
        scores = jnp.einsum('kgd,pikd->kgpi', q_grp, keys_f) * HEAD ** -0.5
        scores = jnp.where(positions <= seq_len + step_idx, scores, -jnp.inf)
        flat_scores = scores.reshape(KV_HEADS, group_heads, PAGES_SEQ * PAGE)
        probs_f = jax.nn.softmax(flat_scores, axis=-1).reshape(scores.shape)
        attn_f = jnp.einsum('kgpi,pikd->kgd', probs_f, vals_f)
        return attn_f.reshape(HEADS * HEAD).astype(jnp.bfloat16)

    return lax.map(one_seq, (queries, new_table, seq_lens))


def reference(embeds, w_query, w_key, w_value, w_out, w_up, w_down, k_pool, v_pool, new_table, seq_lens, mig_src, mig_dst):
    k_pool = k_pool.at[mig_dst].set(k_pool[mig_src]).at[mig_src].set(0)
    v_pool = v_pool.at[mig_dst].set(v_pool[mig_src]).at[mig_src].set(0)
    batch_rows = embeds.shape[1]
    step_outs = []
    for step_idx in range(2):
        hidden = embeds[step_idx]
        positions = seq_lens + step_idx
        slot_ids = jnp.take_along_axis(new_table, (positions // PAGE)[:, None], axis=1)[:, 0]
        offsets = positions % PAGE
        for layer_idx in range(LAYERS):
            queries = jnp.dot(hidden, w_query[layer_idx], preferred_element_type=jnp.float32).astype(jnp.bfloat16)
            new_keys = jnp.dot(hidden, w_key[layer_idx], preferred_element_type=jnp.float32).astype(jnp.bfloat16).reshape(batch_rows, KV_HEADS, HEAD)
            new_vals = jnp.dot(hidden, w_value[layer_idx], preferred_element_type=jnp.float32).astype(jnp.bfloat16).reshape(batch_rows, KV_HEADS, HEAD)
            k_pool = k_pool.at[slot_ids, layer_idx, offsets].set(new_keys)
            v_pool = v_pool.at[slot_ids, layer_idx, offsets].set(new_vals)
            attn_out = attend_all(queries.reshape(batch_rows, HEADS, HEAD), k_pool[:, layer_idx], v_pool[:, layer_idx], new_table, seq_lens, step_idx)
            hidden = (hidden.astype(jnp.float32) + jnp.dot(attn_out, w_out[layer_idx], preferred_element_type=jnp.float32)).astype(jnp.bfloat16)
            up_proj = jnp.dot(hidden, w_up[layer_idx], preferred_element_type=jnp.float32).astype(jnp.bfloat16)
            act_vals = jax.nn.gelu(up_proj.astype(jnp.float32), approximate=True).astype(jnp.bfloat16)
            hidden = (hidden.astype(jnp.float32) + jnp.dot(act_vals, w_down[layer_idx], preferred_element_type=jnp.float32)).astype(jnp.bfloat16)
        step_outs.append(hidden)
    return jnp.stack(step_outs), k_pool, v_pool
```

```python
import functools

import jax
import jax.numpy as jnp
from jax import lax
from jax.experimental import pallas as pl
from jax.experimental.pallas import tpu as pltpu
from jax.sharding import PartitionSpec as P

STEPS = 2
I32 = jnp.int32


def excl_cumsum(values):
    n = values.shape[0]
    before = jnp.arange(n)[None, :] < jnp.arange(n)[:, None]
    return jnp.sum(jnp.where(before, values[None, :], 0), axis=1)


def masked_pick(mask, values):
    return jnp.sum(jnp.where(mask, values, 0), axis=-1)


def place_sequences(pref, group_size, per_dev):
    count = pref.shape[0]
    ids = jnp.arange(count)
    earlier = ids[None, :] < ids[:, None]
    rank = jnp.sum((pref[None, :] == pref[:, None]) & earlier, axis=1)
    wanted = jnp.sum(pref[None, :] == jnp.arange(group_size)[:, None], axis=1)
    free = jnp.maximum(per_dev - wanted, 0)
    free_end = excl_cumsum(free) + free
    over = rank >= per_dev
    over_rank = jnp.sum(over[None, :] & earlier, axis=1)
    spill = jnp.sum(over_rank[:, None] >= free_end[None, :], axis=1)
    dev = jnp.where(over, spill, pref)
    pos = jnp.sum((dev[None, :] == dev[:, None]) & earlier, axis=1)
    return dev.astype(I32), pos.astype(I32)


def any_spec():
    return pl.BlockSpec(memory_space=pl.ANY)


def smem_spec():
    return pl.BlockSpec(memory_space=pltpu.SMEM)


def vmem_spec():
    return pl.BlockSpec(memory_space=pltpu.VMEM)


def start(copy):
    copy.start()


def wait(copy):
    copy.wait()


def for_all(count, table, row, make, act):
    def body(e, carry):
        @pl.when(table[row, e] >= 0)
        def _():
            for copy in make(e):
                act(copy)
        return carry
    lax.fori_loop(0, count, body, 0)


def pack_kernel(layers, rows, clear, meta, k_pool, v_pool, *rest):
    outs = rest[:layers]
    stage, in_sem, out_sem = rest[-3:]
    count = stage.shape[1]

    def fetch(layer):
        def make(e):
            slot = meta[0, e]
            return (pltpu.make_async_copy(k_pool.at[slot, layer, pl.ds(0, rows)], stage.at[layer, e, 0], in_sem.at[layer]),
                    pltpu.make_async_copy(v_pool.at[slot, layer, pl.ds(0, rows)], stage.at[layer, e, 1], in_sem.at[layer]))
        return make

    for layer in range(layers):
        for_all(count, meta, 0, fetch(layer), start)
    if clear:
        def wipe(e, carry):
            @pl.when(meta[0, e] < 0)
            def _():
                for layer in range(layers):
                    stage[layer, e] = jnp.zeros(stage.shape[2:], stage.dtype)
            return carry
        lax.fori_loop(0, count, wipe, 0)
    for layer in range(layers):
        for_all(count, meta, 0, fetch(layer), wait)
        pltpu.make_async_copy(stage.at[layer], outs[layer], out_sem.at[layer]).start()
    for layer in range(layers):
        pltpu.make_async_copy(stage.at[layer], outs[layer], out_sem.at[layer]).wait()


def pack(name, k_pool, v_pool, slot_of, rows, clear, spare=()):
    layers = k_pool.shape[1]
    shape = (slot_of.shape[0], 2, rows) + k_pool.shape[3:]
    outs = [jax.ShapeDtypeStruct(shape, k_pool.dtype)] * layers + [jax.ShapeDtypeStruct(s, k_pool.dtype) for s in spare]
    return pl.pallas_call(
        functools.partial(pack_kernel, layers, rows, clear),
        out_shape=outs,
        in_specs=[smem_spec(), any_spec(), any_spec()],
        out_specs=[any_spec()] * len(outs),
        scratch_shapes=[pltpu.VMEM((layers,) + shape, k_pool.dtype), pltpu.SemaphoreType.DMA((layers,)), pltpu.SemaphoreType.DMA((layers,))],
        name=name,
    )(slot_of[None, :].astype(I32), k_pool, v_pool)


LOCAL, MOVED, NEXT, OTHER = range(4)


def attend_kernel(layer, seqs, page_len, q_per_kv, unroll, meta, q_ref, new_ref, k_pool, v_pool, moved, near, other, out_ref, k_buf, v_buf, k_sem, v_sem):
    kv_heads, head_dim = k_buf.shape[2:]
    near_rows = near.shape[2]

    def fetch(j, act):
        for page in range(2):
            kind = meta[2 * page, j]
            index = meta[2 * page + 1, j]

            def both(k_src, v_src, rows):
                dst = pl.ds(page * page_len, rows)
                act(pltpu.make_async_copy(k_src, k_buf.at[j, dst], k_sem.at[j]))
                act(pltpu.make_async_copy(v_src, v_buf.at[j, dst], v_sem.at[j]))

            @pl.when(kind == LOCAL)
            def _():
                both(k_pool.at[index, layer], v_pool.at[index, layer], page_len)

            @pl.when(kind == MOVED)
            def _():
                both(moved.at[index, 0], moved.at[index, 1], page_len)

            @pl.when(kind == NEXT)
            def _():
                both(near.at[index, 0], near.at[index, 1], near_rows)

            @pl.when(kind == OTHER)
            def _():
                both(other.at[index, 0, layer], other.at[index, 1, layer], page_len)

    def launch(j, carry):
        fetch(j, start)
        return carry
    lax.fori_loop(0, seqs, launch, 0)

    rows = STEPS * kv_heads * q_per_kv
    cols = 2 * page_len * kv_heads
    row_id = lax.broadcasted_iota(I32, (rows, cols), 0)
    col_id = lax.broadcasted_iota(I32, (rows, cols), 1)
    row_step = row_id // (kv_heads * q_per_kv)
    own_head = (col_id % kv_heads) == (row_id % (kv_heads * q_per_kv)) // q_per_kv
    lag = jnp.where(own_head, col_id // kv_heads - row_step, 1 << 20)
    v_pos = lax.broadcasted_iota(I32, (cols, head_dim), 0) // kv_heads

    def body(i, carry):
        for u in range(unroll):
            fetch(i * unroll + u, wait)
        for u in range(unroll):
            j = i * unroll + u
            length = meta[4, j]
            for step in range(STEPS):
                k_buf[j, length + step] = new_ref[j, 0, step]
                v_buf[j, length + step] = new_ref[j, 1, step]
        for u in range(unroll):
            j = i * unroll + u
            length = meta[4, j]
            keys = k_buf[j].reshape(cols, head_dim)
            vals = v_buf[j].reshape(cols, head_dim)
            vals = jnp.where(v_pos <= length + (STEPS - 1), vals.astype(jnp.float32), 0.0).astype(vals.dtype)
            query = q_ref[j].reshape(rows, head_dim)
            scores = lax.dot_general(query, keys, (((1,), (1,)), ((), ())), preferred_element_type=jnp.float32)
            scores = jnp.where(lag <= length, scores * head_dim ** -0.5, -jnp.inf)
            top = jnp.max(scores, axis=1, keepdims=True)
            probs = jnp.exp(scores - top)
            total = jnp.sum(probs, axis=1, keepdims=True)
            out = jnp.dot(probs.astype(vals.dtype), vals, preferred_element_type=jnp.float32) / total
            out_ref[j] = out.astype(out_ref.dtype).reshape(out_ref.shape[1:])
        return carry
    lax.fori_loop(0, seqs // unroll, body, 0)


def attend(layer, queries, new_rows, k_pool, v_pool, moved, near, other, meta):
    seqs = queries.shape[0]
    page_len, kv_heads, head_dim = k_pool.shape[2:]
    num_heads = queries.shape[2]
    buf = pltpu.VMEM((seqs, 2 * page_len, kv_heads, head_dim), k_pool.dtype)
    return pl.pallas_call(
        functools.partial(attend_kernel, layer, seqs, page_len, num_heads // kv_heads, 4),
        out_shape=jax.ShapeDtypeStruct(queries.shape, queries.dtype),
        in_specs=[smem_spec(), vmem_spec(), vmem_spec()] + [any_spec()] * 5,
        out_specs=vmem_spec(),
        scratch_shapes=[buf, buf, pltpu.SemaphoreType.DMA((seqs,)), pltpu.SemaphoreType.DMA((seqs,))],
        cost_estimate=pl.CostEstimate(flops=10 ** 10, bytes_accessed=10 ** 7, transcendentals=10 ** 6),
        name=f'attend_{layer}',
    )(meta, queries, new_rows, k_pool, v_pool, moved, near, other)


def finish_kernel(layers, slots, entries, mig, owner, k_in, v_in, *rest):
    del k_in, v_in
    moved = rest[:layers]
    rows = rest[layers:2 * layers]
    k_out, v_out, zeros, stage, row_stage, zero_sem, in_sem, out_sem, row_in_sem, row_sem = rest[2 * layers:]
    zeros[...] = jnp.zeros_like(zeros)

    def fetch(e):
        return [pltpu.make_async_copy(moved[layer].at[e], stage.at[layer, e], in_sem.at[e]) for layer in range(layers)]

    def put(e):
        out = []
        for layer in range(layers):
            out.append(pltpu.make_async_copy(stage.at[layer, e, 0], k_out.at[mig[1, e], layer], out_sem.at[0]))
            out.append(pltpu.make_async_copy(stage.at[layer, e, 1], v_out.at[mig[1, e], layer], out_sem.at[0]))
        return out

    def clear(e):
        return (pltpu.make_async_copy(zeros, k_out.at[mig[0, e]], zero_sem.at[0]),
                pltpu.make_async_copy(zeros, v_out.at[mig[0, e]], zero_sem.at[0]))

    def load(layer):
        return pltpu.make_async_copy(rows[layer], row_stage.at[layer], row_in_sem.at[layer])

    def fill(j):
        out = []
        for layer in range(layers):
            src = row_stage.at[layer, owner[0, j]]
            dst = pl.ds(owner[1, j], STEPS)
            out.append(pltpu.make_async_copy(src.at[0], k_out.at[j, layer, dst], row_sem.at[0]))
            out.append(pltpu.make_async_copy(src.at[1], v_out.at[j, layer, dst], row_sem.at[0]))
        return out

    for_all(entries, mig, 1, fetch, start)
    for layer in range(layers):
        load(layer).start()

    def relay(e, carry):
        @pl.when(mig[1, e] >= 0)
        def _():
            for copy in fetch(e):
                copy.wait()
            for copy in put(e):
                copy.start()
        return carry
    lax.fori_loop(0, entries, relay, 0)
    for_all(entries, mig, 0, clear, start)
    for_all(entries, mig, 1, put, wait)
    for layer in range(layers):
        load(layer).wait()
    for_all(slots, owner, 0, fill, start)
    for_all(entries, mig, 0, clear, wait)
    for_all(slots, owner, 0, fill, wait)


def finish_pools(k_pool, v_pool, moved, rows, mig, owner):
    slots, layers = k_pool.shape[:2]
    entries = mig.shape[1]
    pool = jax.ShapeDtypeStruct(k_pool.shape, k_pool.dtype)
    return pl.pallas_call(
        functools.partial(finish_kernel, layers, slots, entries),
        out_shape=[pool, pool],
        in_specs=[smem_spec(), smem_spec()] + [any_spec()] * (2 + 2 * layers),
        out_specs=[any_spec(), any_spec()],
        input_output_aliases={2: 0, 3: 1},
        scratch_shapes=[
            pltpu.VMEM(k_pool.shape[1:], k_pool.dtype),
            pltpu.VMEM((layers,) + moved[0].shape, k_pool.dtype),
            pltpu.VMEM((layers,) + rows[0].shape, k_pool.dtype),
            pltpu.SemaphoreType.DMA((1,)),
            pltpu.SemaphoreType.DMA((entries,)),
            pltpu.SemaphoreType.DMA((1,)),
            pltpu.SemaphoreType.DMA((layers,)),
            pltpu.SemaphoreType.DMA((1,)),
        ],
        name='finish_pools',
    )(mig, owner, k_pool, v_pool, *moved, *rows)


def dense(hidden, weight):
    return jnp.dot(hidden, weight, preferred_element_type=jnp.float32)


def shift_by(count, distance):
    return [(i, (i + distance) % count) for i in range(count)]


ROUND_PAGES = 8


def other_pages(k_pool, v_pool, buffer, src, slot, dst, target, wanted, me, group_size):
    entry_ids = jnp.arange(src.shape[0])
    rank = masked_pick((src[None, :] == src[:, None]) & wanted[None, :] & (entry_ids[None, :] < entry_ids[:, None]), 1)
    most = jnp.max(jnp.where(wanted, rank + 1, 0))
    seat = jnp.where(wanted, src * src.shape[0] + rank, -1)

    def body(carry):
        done, buf = carry
        seats = ((jnp.arange(group_size) * src.shape[0])[:, None] + done + jnp.arange(ROUND_PAGES)[None, :]).reshape(-1)
        hit = seat[None, :] == seats[:, None]
        seat_slot = masked_pick(hit, slot[None, :])
        seat_target = jnp.where(jnp.any(hit & (dst == me)[None, :], axis=1), masked_pick(hit, target[None, :]), buf.shape[0])
        my_slots = lax.dynamic_slice_in_dim(seat_slot, me * ROUND_PAGES, ROUND_PAGES)
        pages = jnp.stack([jnp.take(k_pool, my_slots, axis=0), jnp.take(v_pool, my_slots, axis=0)], axis=1)
        gathered = lax.all_gather(pages, 'kv', axis=0, tiled=True)
        return done + ROUND_PAGES, buf.at[seat_target].set(gathered, mode='drop')

    return lax.while_loop(lambda carry: carry[0] < most, body, (jnp.zeros((), I32), buffer))[1]


def solution(mesh):
    group_size = mesh.shape['kv']
    pool_spec = P(('rep', 'kv'))
    tok_spec = P(None, ('rep', 'kv'), None)

    def device_fn(embeds, w_query, w_key, w_value, w_out, w_up, w_down, k_pool, v_pool, new_table, seq_lens, mig_src, mig_dst):
        me = lax.axis_index('kv')
        slots, layers, page_len, kv_heads, head_dim = k_pool.shape
        per_dev, width = embeds.shape[1:]
        seq_count, page_count = new_table.shape
        num_heads = w_query.shape[2] // head_dim

        remap = new_table[:, :, None] == mig_dst
        is_moved = jnp.any(remap, axis=-1)
        move_id = masked_pick(remap, jnp.arange(mig_src.shape[0], dtype=I32))
        old_table = jnp.where(is_moved, masked_pick(remap, mig_src), new_table)
        page_src = old_table // slots
        page_slot = old_table % slots
        dev, pos = place_sequences(page_src[:, 0], group_size, per_dev)
        place = dev * per_dev + pos

        src_dev, dst_dev = mig_src // slots, mig_dst // slots
        clear_slot = jnp.where(src_dev == me, mig_src % slots, -1)
        fill_slot = jnp.where(dst_dev == me, mig_dst % slots, -1)
        mig_meta = jnp.stack([clear_slot, fill_slot]).astype(I32)
        moved = [lax.psum(pages, 'kv') for pages in pack('pack_moved', k_pool, v_pool, clear_slot, page_len, True)]

        prev = (me + group_size - 1) % group_size
        prev_seat = prev * per_dev + jnp.arange(per_dev, dtype=I32)
        from_here = (place[None, :] == prev_seat[:, None]) & ((page_src[:, 1] == me) & ~is_moved[:, 1])[None, :]
        near_slot = masked_pick(from_here, page_slot[None, :, 1] + 1) - 1
        other_shape = (per_dev * page_count, 2) + k_pool.shape[1:]
        *near_out, other = pack('pack_near', k_pool, v_pool, near_slot, page_len - 2, False, [other_shape])
        near = [lax.ppermute(pages, 'kv', shift_by(group_size, -1)) for pages in near_out]

        my_dev = lax.dynamic_slice_in_dim(dev, me * per_dev, per_dev)
        my_pos = lax.dynamic_slice_in_dim(pos, me * per_dev, per_dev)
        home = jnp.arange(seq_count, dtype=I32) // per_dev
        distance = (dev - home) % group_size
        my_distance = (my_dev - me) % group_size
        at_pos = my_pos[None, :] == jnp.arange(per_dev, dtype=I32)[:, None]

        def send_embeds(step_away, hidden):
            sel = (at_pos & (my_distance == step_away)[None, :]).astype(embeds.dtype)
            rows = jnp.einsum('pb,tbd->ptd', sel, embeds, preferred_element_type=jnp.float32).astype(embeds.dtype)
            if step_away:
                rows = lax.ppermute(rows, 'kv', shift_by(group_size, step_away))
            return hidden + rows

        hidden = jnp.zeros((per_dev, STEPS, width), embeds.dtype)
        for step_away in range(group_size):
            hidden = lax.cond(jnp.any(distance == step_away), functools.partial(send_embeds, step_away), lambda same: same, hidden)
        hidden = hidden.reshape(per_dev * STEPS, width)

        page_ids = jnp.arange(page_count, dtype=I32)[None, :]
        is_near = (page_ids == 1) & (page_src == ((dev + 1) % group_size)[:, None]) & ~is_moved
        is_local = page_src == dev[:, None]
        wanted = ~(is_local | is_moved | is_near)
        kind = jnp.where(is_local, LOCAL, jnp.where(is_moved, MOVED, jnp.where(is_near, NEXT, OTHER)))
        target = pos[:, None] * page_count + page_ids
        index = jnp.where(is_local, page_slot, jnp.where(is_moved, move_id, jnp.where(is_near, pos[:, None], target)))
        entry_dst = jnp.broadcast_to(dev[:, None], page_src.shape)
        other = other_pages(k_pool, v_pool, other, page_src.reshape(-1), page_slot.reshape(-1), entry_dst.reshape(-1), target.reshape(-1), wanted.reshape(-1), me, group_size)
        mine = place[None, :] == (me * per_dev + jnp.arange(per_dev, dtype=I32))[:, None]
        facts = jnp.stack([kind[:, 0], index[:, 0], kind[:, 1], index[:, 1], seq_lens])
        attend_meta = masked_pick(mine[None, :, :], facts[:, None, :]).astype(I32)

        writes = new_table[None, :, 1] == (me * slots + jnp.arange(slots, dtype=I32))[:, None]
        owner_place = masked_pick(writes, place[None, :] + 1) - 1
        owner_off = masked_pick(writes, seq_lens[None, :] - page_len)
        owner_meta = jnp.stack([owner_place, owner_off]).astype(I32)

        new_all = []
        for layer in range(layers):
            queries = dense(hidden, w_query[layer]).astype(jnp.bfloat16)
            new_keys = dense(hidden, w_key[layer]).astype(jnp.bfloat16)
            new_vals = dense(hidden, w_value[layer]).astype(jnp.bfloat16)
            rows = jnp.stack([new_keys, new_vals]).reshape(2, per_dev, STEPS, kv_heads, head_dim).transpose(1, 0, 2, 3, 4)
            new_all.append(lax.all_gather(rows, 'kv', axis=0, tiled=True))
            q_rows = queries.reshape(per_dev, STEPS, num_heads, head_dim)
            attn = attend(layer, q_rows, rows, k_pool, v_pool, moved[layer], near[layer], other, attend_meta).reshape(per_dev * STEPS, num_heads * head_dim)
            hidden = (hidden.astype(jnp.float32) + dense(attn, w_out[layer])).astype(jnp.bfloat16)
            up_proj = dense(hidden, w_up[layer]).astype(jnp.bfloat16)
            act = jax.nn.gelu(up_proj.astype(jnp.float32), approximate=True).astype(jnp.bfloat16)
            hidden = (hidden.astype(jnp.float32) + dense(act, w_down[layer])).astype(jnp.bfloat16)

        k_out, v_out = finish_pools(k_pool, v_pool, moved, new_all, mig_meta, owner_meta)

        hidden = hidden.reshape(per_dev, STEPS, width)

        def bring_home(step_away, total):
            rows = lax.ppermute(hidden, 'kv', shift_by(group_size, -step_away)) if step_away else hidden
            sel = (at_pos & (my_distance == step_away)[None, :]).astype(hidden.dtype)
            return total + jnp.einsum('pb,ptd->tbd', sel, rows, preferred_element_type=jnp.float32).astype(hidden.dtype)

        y_out = jnp.zeros((STEPS, per_dev, width), hidden.dtype)
        for step_away in range(group_size):
            y_out = lax.cond(jnp.any(distance == step_away), functools.partial(bring_home, step_away), lambda same: same, y_out)
        return y_out, k_out, v_out

    return jax.shard_map(device_fn, mesh=mesh, in_specs=(tok_spec, P(), P(), P(), P(), P(), P(), pool_spec, pool_spec, P('rep', None), P('rep'), P('rep'), P('rep')), out_specs=(tok_spec, pool_spec, pool_spec), check_vma=False)
```

```python
import functools

import jax
import jax.numpy as jnp
from jax import lax
from jax.experimental import pallas as pl
from jax.experimental.pallas import tpu as pltpu
from jax.sharding import PartitionSpec as P

STEPS = 2
I32 = jnp.int32


def excl_cumsum(values):
    n = values.shape[0]
    before = jnp.arange(n)[None, :] < jnp.arange(n)[:, None]
    return jnp.sum(jnp.where(before, values[None, :], 0), axis=1)


def masked_pick(mask, values):
    return jnp.sum(jnp.where(mask, values, 0), axis=-1)


def place_sequences(pref, group_size, per_dev):
    count = pref.shape[0]
    ids = jnp.arange(count)
    earlier = ids[None, :] < ids[:, None]
    rank = jnp.sum((pref[None, :] == pref[:, None]) & earlier, axis=1)
    wanted = jnp.sum(pref[None, :] == jnp.arange(group_size)[:, None], axis=1)
    free = jnp.maximum(per_dev - wanted, 0)
    free_end = excl_cumsum(free) + free
    over = rank >= per_dev
    over_rank = jnp.sum(over[None, :] & earlier, axis=1)
    spill = jnp.sum(over_rank[:, None] >= free_end[None, :], axis=1)
    dev = jnp.where(over, spill, pref)
    pos = jnp.sum((dev[None, :] == dev[:, None]) & earlier, axis=1)
    return dev.astype(I32), pos.astype(I32)


def any_spec():
    return pl.BlockSpec(memory_space=pl.ANY)


def smem_spec():
    return pl.BlockSpec(memory_space=pltpu.SMEM)


def vmem_spec():
    return pl.BlockSpec(memory_space=pltpu.VMEM)


def start(copy):
    copy.start()


def wait(copy):
    copy.wait()


def for_all(count, table, row, make, act):
    def body(e, carry):
        @pl.when(table[row, e] >= 0)
        def _():
            for copy in make(e):
                act(copy)
        return carry
    lax.fori_loop(0, count, body, 0)


def pack_kernel(layers, rows, clear, meta, k_pool, v_pool, *rest):
    outs = rest[:len(layers)]
    stage, in_sem, out_sem = rest[-3:]
    count = stage.shape[1]

    def fetch(at):
        def make(e):
            slot = meta[0, e]
            return (pltpu.make_async_copy(k_pool.at[slot, layers[at], pl.ds(0, rows)], stage.at[at, e, 0], in_sem.at[at]),
                    pltpu.make_async_copy(v_pool.at[slot, layers[at], pl.ds(0, rows)], stage.at[at, e, 1], in_sem.at[at]))
        return make

    for at in range(len(layers)):
        for_all(count, meta, 0, fetch(at), start)
    if clear:
        def wipe(e, carry):
            @pl.when(meta[0, e] < 0)
            def _():
                for at in range(len(layers)):
                    stage[at, e] = jnp.zeros(stage.shape[2:], stage.dtype)
            return carry
        lax.fori_loop(0, count, wipe, 0)
    for at in range(len(layers)):
        for_all(count, meta, 0, fetch(at), wait)
        pltpu.make_async_copy(stage.at[at], outs[at], out_sem.at[at]).start()
    for at in range(len(layers)):
        pltpu.make_async_copy(stage.at[at], outs[at], out_sem.at[at]).wait()


def pack(name, layers, k_pool, v_pool, slot_of, rows, clear, spare=()):
    shape = (slot_of.shape[0], 2, rows) + k_pool.shape[3:]
    outs = [jax.ShapeDtypeStruct(shape, k_pool.dtype)] * len(layers) + [jax.ShapeDtypeStruct(s, k_pool.dtype) for s in spare]
    return pl.pallas_call(
        functools.partial(pack_kernel, layers, rows, clear),
        out_shape=outs,
        in_specs=[smem_spec(), any_spec(), any_spec()],
        out_specs=[any_spec()] * len(outs),
        scratch_shapes=[pltpu.VMEM((len(layers),) + shape, k_pool.dtype), pltpu.SemaphoreType.DMA((len(layers),)), pltpu.SemaphoreType.DMA((len(layers),))],
        name=name,
    )(slot_of[None, :].astype(I32), k_pool, v_pool)


LOCAL, MOVED, NEXT, OTHER = range(4)


def attend_kernel(layer, seqs, page_len, q_per_kv, unroll, meta, q_ref, new_ref, k_pool, v_pool, moved, near, other, out_ref, k_buf, v_buf, k_sem, v_sem):
    kv_heads, head_dim = k_buf.shape[2:]
    near_rows = near.shape[2]

    def fetch(j, act):
        for page in range(2):
            kind = meta[2 * page, j]
            index = meta[2 * page + 1, j]

            def both(k_src, v_src, rows):
                dst = pl.ds(page * page_len, rows)
                act(pltpu.make_async_copy(k_src, k_buf.at[j, dst], k_sem.at[j]))
                act(pltpu.make_async_copy(v_src, v_buf.at[j, dst], v_sem.at[j]))

            @pl.when(kind == LOCAL)
            def _():
                both(k_pool.at[index, layer], v_pool.at[index, layer], page_len)

            @pl.when(kind == MOVED)
            def _():
                both(moved.at[index, 0], moved.at[index, 1], page_len)

            @pl.when(kind == NEXT)
            def _():
                both(near.at[index, 0], near.at[index, 1], near_rows)

            @pl.when(kind == OTHER)
            def _():
                both(other.at[index, 0, layer], other.at[index, 1, layer], page_len)

    def launch(j, carry):
        fetch(j, start)
        return carry
    lax.fori_loop(0, seqs, launch, 0)

    rows = STEPS * kv_heads * q_per_kv
    cols = 2 * page_len * kv_heads
    row_id = lax.broadcasted_iota(I32, (rows, cols), 0)
    col_id = lax.broadcasted_iota(I32, (rows, cols), 1)
    row_step = row_id // (kv_heads * q_per_kv)
    own_head = (col_id % kv_heads) == (row_id % (kv_heads * q_per_kv)) // q_per_kv
    lag = jnp.where(own_head, col_id // kv_heads - row_step, 1 << 20)

    def body(i, carry):
        for u in range(unroll):
            fetch(i * unroll + u, wait)
        for u in range(unroll):
            j = i * unroll + u
            length = meta[4, j]
            for row in range(2 * page_len - STEPS, 2 * page_len):
                v_buf[j, row] = jnp.zeros((kv_heads, head_dim), v_buf.dtype)
            for step in range(STEPS):
                k_buf[j, length + step] = new_ref[j, 0, step]
                v_buf[j, length + step] = new_ref[j, 1, step]
        for u in range(unroll):
            j = i * unroll + u
            length = meta[4, j]
            keys = k_buf[j].reshape(cols, head_dim)
            vals = v_buf[j].reshape(cols, head_dim)
            query = q_ref[j].reshape(rows, head_dim)
            scores = lax.dot_general(query, keys, (((1,), (1,)), ((), ())), preferred_element_type=jnp.float32)
            scores = jnp.where(lag <= length, scores * head_dim ** -0.5, -jnp.inf)
            top = jnp.max(scores, axis=1, keepdims=True)
            probs = jnp.exp(scores - top)
            total = jnp.sum(probs, axis=1, keepdims=True)
            out = jnp.dot(probs.astype(vals.dtype), vals, preferred_element_type=jnp.float32) / total
            out_ref[j] = out.astype(out_ref.dtype).reshape(out_ref.shape[1:])
        return carry
    lax.fori_loop(0, seqs // unroll, body, 0)


def attend(layer, queries, new_rows, k_pool, v_pool, moved, near, other, meta):
    seqs = queries.shape[0]
    page_len, kv_heads, head_dim = k_pool.shape[2:]
    num_heads = queries.shape[2]
    buf = pltpu.VMEM((seqs, 2 * page_len, kv_heads, head_dim), k_pool.dtype)
    return pl.pallas_call(
        functools.partial(attend_kernel, layer, seqs, page_len, num_heads // kv_heads, 4),
        out_shape=jax.ShapeDtypeStruct(queries.shape, queries.dtype),
        in_specs=[smem_spec(), vmem_spec(), vmem_spec()] + [any_spec()] * 5,
        out_specs=vmem_spec(),
        scratch_shapes=[buf, buf, pltpu.SemaphoreType.DMA((seqs,)), pltpu.SemaphoreType.DMA((seqs,))],
        cost_estimate=pl.CostEstimate(flops=10 ** 10, bytes_accessed=10 ** 7, transcendentals=10 ** 6),
        name=f'attend_{layer}',
    )(meta, queries, new_rows, k_pool, v_pool, moved, near, other)


COPY_SLOTS = 16


def copy_kernel(k_pool, v_pool, k_out, v_out, stage, in_sem, out_sem):
    chunks = k_pool.shape[0] // COPY_SLOTS
    for pool, out, which in ((k_pool, k_out, 0), (v_pool, v_out, 1)):
        for c in range(chunks):
            part = pl.ds(c * COPY_SLOTS, COPY_SLOTS)
            pltpu.make_async_copy(pool.at[part], stage.at[which, part], in_sem.at[which, c]).start()
    for pool, out, which in ((k_pool, k_out, 0), (v_pool, v_out, 1)):
        for c in range(chunks):
            part = pl.ds(c * COPY_SLOTS, COPY_SLOTS)
            pltpu.make_async_copy(pool.at[part], stage.at[which, part], in_sem.at[which, c]).wait()
            pltpu.make_async_copy(stage.at[which, part], out.at[part], out_sem.at[which, c]).start()
    for pool, out, which in ((k_pool, k_out, 0), (v_pool, v_out, 1)):
        for c in range(chunks):
            part = pl.ds(c * COPY_SLOTS, COPY_SLOTS)
            pltpu.make_async_copy(stage.at[which, part], out.at[part], out_sem.at[which, c]).wait()


def copy_pools(k_pool, v_pool):
    chunks = k_pool.shape[0] // COPY_SLOTS
    pool = jax.ShapeDtypeStruct(k_pool.shape, k_pool.dtype)
    return pl.pallas_call(
        copy_kernel,
        out_shape=[pool, pool],
        in_specs=[any_spec(), any_spec()],
        out_specs=[any_spec(), any_spec()],
        scratch_shapes=[pltpu.VMEM((2,) + k_pool.shape, k_pool.dtype), pltpu.SemaphoreType.DMA((2, chunks)), pltpu.SemaphoreType.DMA((2, chunks))],
        name='copy_pools',
    )(k_pool, v_pool)


def finish_kernel(layers, slots, entries, mig, owner, k_in, v_in, *rest):
    del k_in, v_in
    moved = rest[:layers]
    rows = rest[layers:2 * layers]
    k_out, v_out, zeros, stage, row_stage, zero_sem, in_sem, out_sem, row_in_sem, row_sem = rest[2 * layers:]
    zeros[...] = jnp.zeros_like(zeros)

    def fetch(e):
        return [pltpu.make_async_copy(moved[layer].at[e], stage.at[layer, e], in_sem.at[e]) for layer in range(layers)]

    def put(e):
        out = []
        for layer in range(layers):
            out.append(pltpu.make_async_copy(stage.at[layer, e, 0], k_out.at[mig[1, e], layer], out_sem.at[0]))
            out.append(pltpu.make_async_copy(stage.at[layer, e, 1], v_out.at[mig[1, e], layer], out_sem.at[0]))
        return out

    def clear(e):
        return (pltpu.make_async_copy(zeros, k_out.at[mig[0, e]], zero_sem.at[0]),
                pltpu.make_async_copy(zeros, v_out.at[mig[0, e]], zero_sem.at[0]))

    def load(layer):
        return pltpu.make_async_copy(rows[layer], row_stage.at[layer], row_in_sem.at[layer])

    def fill(j):
        out = []
        for layer in range(layers):
            src = row_stage.at[layer, owner[0, j]]
            dst = pl.ds(owner[1, j], STEPS)
            out.append(pltpu.make_async_copy(src.at[0], k_out.at[j, layer, dst], row_sem.at[0]))
            out.append(pltpu.make_async_copy(src.at[1], v_out.at[j, layer, dst], row_sem.at[0]))
        return out

    for_all(entries, mig, 1, fetch, start)
    for layer in range(layers):
        load(layer).start()

    def relay(e, carry):
        @pl.when(mig[1, e] >= 0)
        def _():
            for copy in fetch(e):
                copy.wait()
            for copy in put(e):
                copy.start()
        return carry
    lax.fori_loop(0, entries, relay, 0)
    for_all(entries, mig, 0, clear, start)
    for_all(entries, mig, 1, put, wait)
    for layer in range(layers):
        load(layer).wait()
    for_all(slots, owner, 0, fill, start)
    for_all(entries, mig, 0, clear, wait)
    for_all(slots, owner, 0, fill, wait)


def finish_pools(k_pool, v_pool, moved, rows, mig, owner):
    slots, layers = k_pool.shape[:2]
    entries = mig.shape[1]
    pool = jax.ShapeDtypeStruct(k_pool.shape, k_pool.dtype)
    return pl.pallas_call(
        functools.partial(finish_kernel, layers, slots, entries),
        out_shape=[pool, pool],
        in_specs=[smem_spec(), smem_spec()] + [any_spec()] * (2 + 2 * layers),
        out_specs=[any_spec(), any_spec()],
        input_output_aliases={2: 0, 3: 1},
        scratch_shapes=[
            pltpu.VMEM(k_pool.shape[1:], k_pool.dtype),
            pltpu.VMEM((layers,) + moved[0].shape, k_pool.dtype),
            pltpu.VMEM((layers,) + rows[0].shape, k_pool.dtype),
            pltpu.SemaphoreType.DMA((1,)),
            pltpu.SemaphoreType.DMA((entries,)),
            pltpu.SemaphoreType.DMA((1,)),
            pltpu.SemaphoreType.DMA((layers,)),
            pltpu.SemaphoreType.DMA((1,)),
        ],
        name='finish_pools',
    )(mig, owner, k_pool, v_pool, *moved, *rows)


def dense(hidden, weight):
    return jnp.dot(hidden, weight, preferred_element_type=jnp.float32)


def pair_mlp(hidden, w_up, w_down, layer, core, pairs):
    rows = hidden.shape[0]
    width, full = w_up.shape[1:]
    half = full // 2
    both = jnp.concatenate([hidden, lax.ppermute(hidden, 'kv', pairs)])
    up_proj = dense(both, lax.dynamic_slice(w_up, (layer, 0, core * half), (1, width, half))[0]).astype(jnp.bfloat16)
    act = jax.nn.gelu(up_proj.astype(jnp.float32), approximate=True).astype(jnp.bfloat16)
    part = dense(act, lax.dynamic_slice(w_down, (layer, core * half, 0), (1, half, width))[0])
    rest = lax.ppermute(part[rows:], 'kv', pairs)
    return (hidden.astype(jnp.float32) + (part[:rows] + rest)).astype(jnp.bfloat16)


def shift_by(count, distance):
    return [(i, (i + distance) % count) for i in range(count)]


ROUND_PAGES = 8


def other_pages(k_pool, v_pool, buffer, src, slot, dst, target, wanted, me, group_size):
    entry_ids = jnp.arange(src.shape[0])
    rank = masked_pick((src[None, :] == src[:, None]) & wanted[None, :] & (entry_ids[None, :] < entry_ids[:, None]), 1)
    most = jnp.max(jnp.where(wanted, rank + 1, 0))
    seat = jnp.where(wanted, src * src.shape[0] + rank, -1)

    def body(carry):
        done, buf = carry
        seats = ((jnp.arange(group_size) * src.shape[0])[:, None] + done + jnp.arange(ROUND_PAGES)[None, :]).reshape(-1)
        hit = seat[None, :] == seats[:, None]
        seat_slot = masked_pick(hit, slot[None, :])
        seat_target = jnp.where(jnp.any(hit & (dst == me)[None, :], axis=1), masked_pick(hit, target[None, :]), buf.shape[0])
        my_slots = lax.dynamic_slice_in_dim(seat_slot, me * ROUND_PAGES, ROUND_PAGES)
        pages = jnp.stack([jnp.take(k_pool, my_slots, axis=0), jnp.take(v_pool, my_slots, axis=0)], axis=1)
        gathered = lax.all_gather(pages, 'kv', axis=0, tiled=True)
        return done + ROUND_PAGES, buf.at[seat_target].set(gathered, mode='drop')

    return lax.while_loop(lambda carry: carry[0] < most, body, (jnp.zeros((), I32), buffer))[1]


def solution(mesh):
    group_size = mesh.shape['kv']
    pool_spec = P(('rep', 'kv'))
    tok_spec = P(None, ('rep', 'kv'), None)

    def device_fn(embeds, w_query, w_key, w_value, w_out, w_up, w_down, k_pool, v_pool, new_table, seq_lens, mig_src, mig_dst):
        me = lax.axis_index('kv')
        slots, layers, page_len, kv_heads, head_dim = k_pool.shape
        per_dev, width = embeds.shape[1:]
        seq_count, page_count = new_table.shape
        num_heads = w_query.shape[2] // head_dim
        pairs = [(i, i ^ 1) for i in range(group_size)]

        remap = new_table[:, :, None] == mig_dst
        is_moved = jnp.any(remap, axis=-1)
        move_id = masked_pick(remap, jnp.arange(mig_src.shape[0], dtype=I32))
        old_table = jnp.where(is_moved, masked_pick(remap, mig_src), new_table)
        page_src = old_table // slots
        page_slot = old_table % slots
        dev, pos = place_sequences(page_src[:, 0], group_size, per_dev)
        place = dev * per_dev + pos

        src_dev, dst_dev = mig_src // slots, mig_dst // slots
        clear_slot = jnp.where(src_dev == me, mig_src % slots, -1)
        fill_slot = jnp.where(dst_dev == me, mig_dst % slots, -1)
        mig_meta = jnp.stack([clear_slot, fill_slot]).astype(I32)
        moved = [lax.psum(pack('pack_moved_0', (0,), k_pool, v_pool, clear_slot, page_len, True)[0], 'kv')]

        prev = (me + group_size - 1) % group_size
        prev_seat = prev * per_dev + jnp.arange(per_dev, dtype=I32)
        from_here = (place[None, :] == prev_seat[:, None]) & ((page_src[:, 1] == me) & ~is_moved[:, 1])[None, :]
        near_slot = masked_pick(from_here, page_slot[None, :, 1] + 1) - 1
        other_shape = (per_dev * page_count, 2) + k_pool.shape[1:]
        *near_out, other = pack('pack_near', tuple(range(layers)), k_pool, v_pool, near_slot, page_len - 2, False, [other_shape])

        my_dev = lax.dynamic_slice_in_dim(dev, me * per_dev, per_dev)
        my_pos = lax.dynamic_slice_in_dim(pos, me * per_dev, per_dev)
        home = jnp.arange(seq_count, dtype=I32) // per_dev
        distance = (dev - home) % group_size
        my_distance = (my_dev - me) % group_size
        at_pos = my_pos[None, :] == jnp.arange(per_dev, dtype=I32)[:, None]

        def send_embeds(step_away, hidden):
            sel = (at_pos & (my_distance == step_away)[None, :]).astype(embeds.dtype)
            rows = jnp.einsum('pb,tbd->ptd', sel, embeds, preferred_element_type=jnp.float32).astype(embeds.dtype)
            if step_away:
                rows = lax.ppermute(rows, 'kv', shift_by(group_size, step_away))
            return hidden + rows

        hidden = jnp.zeros((per_dev, STEPS, width), embeds.dtype)
        for step_away in range(group_size):
            hidden = lax.cond(jnp.any(distance == step_away), functools.partial(send_embeds, step_away), lambda same: same, hidden)
        hidden = hidden.reshape(per_dev * STEPS, width)
        near_out[0], hidden = lax.optimization_barrier((near_out[0], hidden))
        near = [lax.ppermute(near_out[0], 'kv', shift_by(group_size, -1))]

        page_ids = jnp.arange(page_count, dtype=I32)[None, :]
        is_near = (page_ids == 1) & (page_src == ((dev + 1) % group_size)[:, None]) & ~is_moved
        is_local = page_src == dev[:, None]
        wanted = ~(is_local | is_moved | is_near)
        kind = jnp.where(is_local, LOCAL, jnp.where(is_moved, MOVED, jnp.where(is_near, NEXT, OTHER)))
        target = pos[:, None] * page_count + page_ids
        index = jnp.where(is_local, page_slot, jnp.where(is_moved, move_id, jnp.where(is_near, pos[:, None], target)))
        entry_dst = jnp.broadcast_to(dev[:, None], page_src.shape)
        other = other_pages(k_pool, v_pool, other, page_src.reshape(-1), page_slot.reshape(-1), entry_dst.reshape(-1), target.reshape(-1), wanted.reshape(-1), me, group_size)
        mine = place[None, :] == (me * per_dev + jnp.arange(per_dev, dtype=I32))[:, None]
        facts = jnp.stack([kind[:, 0], index[:, 0], kind[:, 1], index[:, 1], seq_lens])
        attend_meta = masked_pick(mine[None, :, :], facts[:, None, :]).astype(I32)

        writes = new_table[None, :, 1] == (me * slots + jnp.arange(slots, dtype=I32))[:, None]
        owner_place = masked_pick(writes, place[None, :] + 1) - 1
        owner_off = masked_pick(writes, seq_lens[None, :] - page_len)
        owner_meta = jnp.stack([owner_place, owner_off]).astype(I32)

        new_all = []
        for layer in range(layers):
            queries = dense(hidden, w_query[layer]).astype(jnp.bfloat16)
            new_keys = dense(hidden, w_key[layer]).astype(jnp.bfloat16)
            new_vals = dense(hidden, w_value[layer]).astype(jnp.bfloat16)
            rows = jnp.stack([new_keys, new_vals]).reshape(2, per_dev, STEPS, kv_heads, head_dim).transpose(1, 0, 2, 3, 4)
            new_all.append(lax.all_gather(rows, 'kv', axis=0, tiled=True))
            q_rows = queries.reshape(per_dev, STEPS, num_heads, head_dim)
            if layer == 0:
                k_src, v_src, q_rows = lax.optimization_barrier((k_pool, v_pool, q_rows))
                k_base, v_base = copy_pools(k_src, v_src)
                q_rows, k_base, v_base = lax.optimization_barrier((q_rows, k_base, v_base))
            if layer + 1 < layers:
                near_next, moved[layer], near[layer], clear_next = lax.optimization_barrier((near_out[layer + 1], moved[layer], near[layer], clear_slot))
                near.append(lax.ppermute(near_next, 'kv', shift_by(group_size, -1)))
                moved.append(lax.psum(pack(f'pack_moved_{layer + 1}', (layer + 1,), k_pool, v_pool, clear_next, page_len, True)[0], 'kv'))
            attn = attend(layer, q_rows, rows, k_pool, v_pool, moved[layer], near[layer], other, attend_meta).reshape(per_dev * STEPS, num_heads * head_dim)
            hidden = (hidden.astype(jnp.float32) + dense(attn, w_out[layer])).astype(jnp.bfloat16)
            hidden = pair_mlp(hidden, w_up, w_down, layer, me % 2, pairs)

        k_out, v_out = finish_pools(k_base, v_base, moved, new_all, mig_meta, owner_meta)

        hidden = hidden.reshape(per_dev, STEPS, width)

        def bring_home(step_away, total):
            rows = lax.ppermute(hidden, 'kv', shift_by(group_size, -step_away)) if step_away else hidden
            sel = (at_pos & (my_distance == step_away)[None, :]).astype(hidden.dtype)
            return total + jnp.einsum('pb,ptd->tbd', sel, rows, preferred_element_type=jnp.float32).astype(hidden.dtype)

        y_out = jnp.zeros((STEPS, per_dev, width), hidden.dtype)
        for step_away in range(group_size):
            y_out = lax.cond(jnp.any(distance == step_away), functools.partial(bring_home, step_away), lambda same: same, y_out)
        return y_out, k_out, v_out

    return jax.shard_map(device_fn, mesh=mesh, in_specs=(tok_spec, P(), P(), P(), P(), P(), P(), pool_spec, pool_spec, P('rep', None), P('rep'), P('rep'), P('rep')), out_specs=(tok_spec, pool_spec, pool_spec), check_vma=False)
```

```python
import functools

import jax
import jax.numpy as jnp
from jax import lax
from jax.experimental import pallas as pl
from jax.experimental.pallas import tpu as pltpu
from jax.sharding import PartitionSpec as P


STEPS = 2
I32 = jnp.int32


def excl_cumsum(values):
    n = values.shape[0]
    before = jnp.arange(n)[None, :] < jnp.arange(n)[:, None]
    return jnp.sum(jnp.where(before, values[None, :], 0), axis=1)


def masked_pick(mask, values):
    return jnp.sum(jnp.where(mask, values, 0), axis=-1)


def place_sequences(pref, group_size, per_dev):
    count = pref.shape[0]
    ids = jnp.arange(count)
    earlier = ids[None, :] < ids[:, None]
    rank = jnp.sum((pref[None, :] == pref[:, None]) & earlier, axis=1)
    wanted = jnp.sum(pref[None, :] == jnp.arange(group_size)[:, None], axis=1)
    free = jnp.maximum(per_dev - wanted, 0)
    free_end = excl_cumsum(free) + free
    over = rank >= per_dev
    over_rank = jnp.sum(over[None, :] & earlier, axis=1)
    spill = jnp.sum(over_rank[:, None] >= free_end[None, :], axis=1)
    dev = jnp.where(over, spill, pref)
    pos = jnp.sum((dev[None, :] == dev[:, None]) & earlier, axis=1)
    return dev.astype(I32), pos.astype(I32)


def any_spec():
    return pl.BlockSpec(memory_space=pl.ANY)


def smem_spec():
    return pl.BlockSpec(memory_space=pltpu.SMEM)


def vmem_spec():
    return pl.BlockSpec(memory_space=pltpu.VMEM)


def start(copy):
    copy.start()


def wait(copy):
    copy.wait()


def for_all(count, table, row, make, act):
    def body(e, carry):
        @pl.when(table[row, e] >= 0)
        def _():
            for copy in make(e):
                act(copy)

        return carry

    lax.fori_loop(0, count, body, 0)


def page_copies(layer, k_pool, v_pool, slot, k_dst, v_dst, sem):
    return (pltpu.make_async_copy(k_pool.at[slot, layer], k_dst, sem), pltpu.make_async_copy(v_pool.at[slot, layer], v_dst, sem))


def pack_pages_kernel(layers, meta, k_pool, v_pool, *rest):
    outs = rest[:len(layers)]
    stage, in_sem, out_sem = rest[-3:]
    page_len = k_pool.shape[2]
    count = stage.shape[2] // page_len

    def fetch(at):
        def make(e):
            part = pl.ds(e * page_len, page_len)
            return page_copies(layers[at], k_pool, v_pool, meta[0, e], stage.at[at, 0, part], stage.at[at, 1, part], in_sem.at[at])

        return make

    for at in range(len(layers)):
        for_all(count, meta, 0, fetch(at), start)

    def wipe(e, carry):
        @pl.when(meta[0, e] < 0)
        def _():
            for at in range(len(layers)):
                for which in range(2):
                    stage[at, which, pl.ds(e * page_len, page_len)] = jnp.zeros((page_len,) + stage.shape[3:], stage.dtype)

        return carry

    lax.fori_loop(0, count, wipe, 0)
    for at in range(len(layers)):
        for_all(count, meta, 0, fetch(at), wait)
        pltpu.make_async_copy(stage.at[at], outs[at], out_sem.at[at]).start()
    for at in range(len(layers)):
        pltpu.make_async_copy(stage.at[at], outs[at], out_sem.at[at]).wait()


def pack_pages(layers, k_pool, v_pool, slot_of):
    shape = (2, slot_of.shape[0] * k_pool.shape[2]) + k_pool.shape[3:]
    return pl.pallas_call(
        functools.partial(pack_pages_kernel, layers),
        out_shape=[jax.ShapeDtypeStruct(shape, k_pool.dtype)] * len(layers),
        in_specs=[smem_spec(), any_spec(), any_spec()],
        out_specs=[any_spec()] * len(layers),
        scratch_shapes=[pltpu.VMEM((len(layers),) + shape, k_pool.dtype), pltpu.SemaphoreType.DMA((len(layers),)), pltpu.SemaphoreType.DMA((len(layers),))],
    )(slot_of[None, :].astype(I32), k_pool, v_pool)


def pack_rows_kernel(layers, meta, k_pool, v_pool, *rest):
    outs = rest[:len(layers)]
    pages, stage, in_sem, out_sem = rest[-4:]
    count = pages.shape[1]
    page_len = k_pool.shape[2]

    def fetch(at):
        return lambda e: page_copies(layers[at], k_pool, v_pool, meta[0, e], pages.at[at, e, 0], pages.at[at, e, 1], in_sem.at[at])

    for at in range(len(layers)):
        for_all(count, meta, 0, fetch(at), start)
    nothing = jnp.zeros((page_len,) + stage.shape[3:], stage.dtype)

    def wipe(i, carry):
        for at in range(len(layers)):
            for which in range(2):
                stage[at, which, pl.ds(i * page_len, page_len)] = nothing
        return carry

    lax.fori_loop(0, stage.shape[2] // page_len, wipe, 0)
    for at in range(len(layers)):
        for_all(count, meta, 0, fetch(at), wait)

        def place(e, carry):
            @pl.when(meta[0, e] >= 0)
            def _():
                for which in range(2):
                    stage[at, which, pl.ds(meta[1, e], page_len)] = pages[at, e, which]
                    stage[at, which, pl.ds(meta[1, e] + meta[2, e], page_len)] = nothing

            return carry

        lax.fori_loop(0, count, place, 0)
        pltpu.make_async_copy(stage.at[at], outs[at], out_sem.at[at]).start()
    for at in range(len(layers)):
        pltpu.make_async_copy(stage.at[at], outs[at], out_sem.at[at]).wait()


def pack_rows(layers, k_pool, v_pool, meta, cap, spare=()):
    count = meta.shape[1]
    page_len = k_pool.shape[2]
    shape = (2, cap + 2 * page_len) + k_pool.shape[3:]
    outs = [jax.ShapeDtypeStruct(shape, k_pool.dtype)] * len(layers) + [jax.ShapeDtypeStruct(s, k_pool.dtype) for s in spare]
    return pl.pallas_call(
        functools.partial(pack_rows_kernel, layers),
        out_shape=outs,
        in_specs=[smem_spec(), any_spec(), any_spec()],
        out_specs=[any_spec()] * len(outs),
        scratch_shapes=[
            pltpu.VMEM((len(layers), count, 2) + k_pool.shape[2:], k_pool.dtype),
            pltpu.VMEM((len(layers),) + shape, k_pool.dtype),
            pltpu.SemaphoreType.DMA((len(layers),)),
            pltpu.SemaphoreType.DMA((len(layers),)),
        ],
    )(meta.astype(I32), k_pool, v_pool)


LOCAL, MOVED, NEXT, OTHER = range(4)
MOVED_ROWS = 10
NEAR_ROWS = 9


def attend_kernel(layer, seqs, page_len, q_per_kv, unroll, meta, q_ref, new_ref, k_pool, v_pool, moved, near, other, out_ref, k_buf, v_buf, k_sem, v_sem):
    kv_heads, head_dim = k_buf.shape[2:]

    def launch(j, carry):
        for page in range(2):
            kind = meta[2 * page, j]
            index = meta[2 * page + 1, j]

            def both(k_src, v_src):
                dst = pl.ds(page * page_len, page_len)
                pltpu.make_async_copy(k_src, k_buf.at[j, dst], k_sem.at[j]).start()
                pltpu.make_async_copy(v_src, v_buf.at[j, dst], v_sem.at[j]).start()

            @pl.when(kind == LOCAL)
            def _():
                both(k_pool.at[index, layer], v_pool.at[index, layer])

            @pl.when(kind > LOCAL)
            def _():
                part = pl.ds(index, page_len)

                @pl.when(kind == MOVED)
                def _():
                    both(moved.at[0, part], moved.at[1, part])

                @pl.when(kind == NEXT)
                def _():
                    both(near.at[0, part], near.at[1, part])

                @pl.when(kind == OTHER)
                def _():
                    both(other.at[index, 0, layer], other.at[index, 1, layer])
        return carry

    lax.fori_loop(0, seqs, launch, 0)

    rows = STEPS * kv_heads * q_per_kv
    cols = 2 * page_len * kv_heads
    row_id = lax.broadcasted_iota(I32, (rows, cols), 0)
    col_id = lax.broadcasted_iota(I32, (rows, cols), 1)
    row_step = row_id // (kv_heads * q_per_kv)
    own_head = (col_id % kv_heads) == (row_id % (kv_heads * q_per_kv)) // q_per_kv
    lag = jnp.where(own_head, col_id // kv_heads - row_step, 1 << 20)

    def body(i, carry):
        for u in range(unroll):
            j = i * unroll + u
            pltpu.make_async_copy(k_buf.at[j], k_buf.at[j], k_sem.at[j]).wait()
            pltpu.make_async_copy(v_buf.at[j], v_buf.at[j], v_sem.at[j]).wait()
        for u in range(unroll):
            j = i * unroll + u
            length = meta[4, j]
            for step in range(STEPS):
                k_buf[j, length + step] = new_ref[j, 0, step]
                v_buf[j, length + step] = new_ref[j, 1, step]
        for u in range(unroll):
            j = i * unroll + u
            length = meta[4, j]
            keys = k_buf[j].reshape(cols, head_dim)
            vals = v_buf[j].reshape(cols, head_dim)
            query = q_ref[j].reshape(rows, head_dim)
            scores = lax.dot_general(query, keys, (((1,), (1,)), ((), ())), preferred_element_type=jnp.float32)
            scores = jnp.where(lag <= length, scores * head_dim ** -0.5, -jnp.inf)
            top = jnp.max(scores, axis=1, keepdims=True)
            probs = jnp.exp(scores - top)
            total = jnp.sum(probs, axis=1, keepdims=True)
            out = jnp.dot(probs.astype(vals.dtype), vals, preferred_element_type=jnp.float32) / total
            out_ref[j] = out.astype(out_ref.dtype).reshape(out_ref.shape[1:])
        return carry

    lax.fori_loop(0, seqs // unroll, body, 0)


def attend(layer, queries, new_rows, k_pool, v_pool, moved, near, other, meta):
    seqs = queries.shape[0]
    page_len, kv_heads, head_dim = k_pool.shape[2:]
    num_heads = queries.shape[2]
    buf = pltpu.VMEM((seqs, 2 * page_len, kv_heads, head_dim), k_pool.dtype)
    return pl.pallas_call(
        functools.partial(attend_kernel, layer, seqs, page_len, num_heads // kv_heads, 4),
        out_shape=jax.ShapeDtypeStruct(queries.shape, queries.dtype),
        in_specs=[smem_spec(), vmem_spec(), vmem_spec()] + [any_spec()] * 5,
        out_specs=vmem_spec(),
        scratch_shapes=[buf, buf, pltpu.SemaphoreType.DMA((seqs,)), pltpu.SemaphoreType.DMA((seqs,))],
        cost_estimate=pl.CostEstimate(flops=10 ** 10, bytes_accessed=10 ** 7, transcendentals=10 ** 6),
    )(meta, queries, new_rows, k_pool, v_pool, moved, near, other)


COPY_SLOTS = 16


def copy_kernel(k_pool, v_pool, k_out, v_out, stage, in_sem, out_sem):
    chunks = k_pool.shape[0] // COPY_SLOTS
    for pool, which in ((k_pool, 0), (v_pool, 1)):
        for c in range(chunks):
            part = pl.ds(c * COPY_SLOTS, COPY_SLOTS)
            pltpu.make_async_copy(pool.at[part], stage.at[which, part], in_sem.at[which, c]).start()
    for pool, out, which in ((k_pool, k_out, 0), (v_pool, v_out, 1)):
        for c in range(chunks):
            part = pl.ds(c * COPY_SLOTS, COPY_SLOTS)
            pltpu.make_async_copy(pool.at[part], stage.at[which, part], in_sem.at[which, c]).wait()
            pltpu.make_async_copy(stage.at[which, part], out.at[part], out_sem.at[which, c]).start()
    for out, which in ((k_out, 0), (v_out, 1)):
        for c in range(chunks):
            part = pl.ds(c * COPY_SLOTS, COPY_SLOTS)
            pltpu.make_async_copy(stage.at[which, part], out.at[part], out_sem.at[which, c]).wait()


def copy_pools(k_pool, v_pool):
    chunks = k_pool.shape[0] // COPY_SLOTS
    pool = jax.ShapeDtypeStruct(k_pool.shape, k_pool.dtype)
    return pl.pallas_call(
        copy_kernel,
        out_shape=[pool, pool],
        in_specs=[any_spec(), any_spec()],
        out_specs=[any_spec(), any_spec()],
        scratch_shapes=[pltpu.VMEM((2,) + k_pool.shape, k_pool.dtype), pltpu.SemaphoreType.DMA((2, chunks)), pltpu.SemaphoreType.DMA((2, chunks))],
        name='copy_pools',
    )(k_pool, v_pool)


def finish_kernel(layers, slots, entries, mig, owner, k_in, v_in, *rest):
    del k_in, v_in
    moved, own, prev, far = (rest[i * layers:(i + 1) * layers] for i in range(4))
    k_out, v_out, zeros, stage, row_stage, far_stage, zero_sem, in_sem, out_sem, row_in_sem, row_sem, far_sem = rest[4 * layers:]
    page_len = k_out.shape[2]
    seats = own[0].shape[0]

    def fetch(e):
        part = pl.ds(e * page_len, page_len)
        return [pltpu.make_async_copy(moved[layer].at[which, part], stage.at[e, layer, which], in_sem.at[e]) for layer in range(layers) for which in range(2)]

    def put(e):
        return [pltpu.make_async_copy(stage.at[e, layer, which], out.at[mig[1, e], layer], out_sem.at[0]) for layer in range(layers) for which, out in enumerate((k_out, v_out))]

    def clear(e):
        return [pltpu.make_async_copy(zeros, out.at[mig[0, e]], zero_sem.at[0]) for out in (k_out, v_out)]

    def load(layer):
        return (pltpu.make_async_copy(own[layer], row_stage.at[layer, pl.ds(0, seats)], row_in_sem.at[layer]),
                pltpu.make_async_copy(prev[layer], row_stage.at[layer, pl.ds(seats, seats)], row_in_sem.at[layer]))

    def fill(j):
        dst = pl.ds(owner[1, j], STEPS)
        return [pltpu.make_async_copy(row_stage.at[layer, owner[0, j], which], out.at[j, layer, dst], row_sem.at[0]) for layer in range(layers) for which, out in enumerate((k_out, v_out))]

    for_all(entries, mig, 1, fetch, start)
    for layer in range(layers):
        for copy in load(layer):
            copy.start()
    zeros[...] = jnp.zeros_like(zeros)

    def relay(e, carry):
        @pl.when(mig[1, e] >= 0)
        def _():
            for copy in fetch(e):
                copy.wait()
            for copy in put(e):
                copy.start()

        return carry

    lax.fori_loop(0, entries, relay, 0)
    for_all(entries, mig, 0, clear, start)
    for_all(entries, mig, 1, put, wait)
    for layer in range(layers):
        for copy in load(layer):
            copy.wait()
    for_all(slots, owner, 0, fill, start)

    def from_far(j, carry):
        @pl.when(owner[2, j] >= 0)
        def _():
            dst = pl.ds(owner[1, j], STEPS)
            for layer in range(layers):
                copy = pltpu.make_async_copy(far[layer].at[owner[2, j]], far_stage, far_sem.at[0])
                copy.start()
                copy.wait()
                for which, out in enumerate((k_out, v_out)):
                    copy = pltpu.make_async_copy(far_stage.at[which], out.at[j, layer, dst], far_sem.at[0])
                    copy.start()
                    copy.wait()

        return carry

    lax.fori_loop(0, slots, from_far, 0)
    for_all(entries, mig, 0, clear, wait)
    for_all(slots, owner, 0, fill, wait)


def finish_pools(k_pool, v_pool, moved, own, prev, far, mig, owner):
    slots, layers = k_pool.shape[:2]
    entries = mig.shape[1]
    pool = jax.ShapeDtypeStruct(k_pool.shape, k_pool.dtype)
    row_shape = own[0].shape
    return pl.pallas_call(
        functools.partial(finish_kernel, layers, slots, entries),
        out_shape=[pool, pool],
        in_specs=[smem_spec(), smem_spec()] + [any_spec()] * (2 + 4 * layers),
        out_specs=[any_spec(), any_spec()],
        input_output_aliases={2: 0, 3: 1},
        scratch_shapes=[
            pltpu.VMEM(k_pool.shape[1:], k_pool.dtype),
            pltpu.VMEM((entries, layers, 2) + k_pool.shape[2:], k_pool.dtype),
            pltpu.VMEM((layers, 2 * row_shape[0]) + row_shape[1:], k_pool.dtype),
            pltpu.VMEM(row_shape[1:], k_pool.dtype),
            pltpu.SemaphoreType.DMA((1,)),
            pltpu.SemaphoreType.DMA((entries,)),
            pltpu.SemaphoreType.DMA((1,)),
            pltpu.SemaphoreType.DMA((layers,)),
            pltpu.SemaphoreType.DMA((1,)),
            pltpu.SemaphoreType.DMA((1,)),
        ],
        name='finish_pools',
    )(mig, owner, k_pool, v_pool, *moved, *own, *prev, *far)


def dense(hidden, weight):
    return jnp.dot(hidden, weight, preferred_element_type=jnp.float32)


def pair_mlp(hidden, w_up, w_down, layer, core, pairs):
    rows = hidden.shape[0]
    width, full = w_up.shape[1:]
    half = full // 2
    both = jnp.concatenate([hidden, lax.ppermute(hidden, 'kv', pairs)])
    up_proj = dense(both, lax.dynamic_slice(w_up, (layer, 0, core * half), (1, width, half))[0]).astype(jnp.bfloat16)
    act = jax.nn.gelu(up_proj.astype(jnp.float32), approximate=True).astype(jnp.bfloat16)
    part = dense(act, lax.dynamic_slice(w_down, (layer, core * half, 0), (1, half, width))[0])
    rest = lax.ppermute(part[rows:], 'kv', pairs)
    return (hidden.astype(jnp.float32) + (part[:rows] + rest)).astype(jnp.bfloat16)


def shift_by(count, distance):
    return [(i, (i + distance) % count) for i in range(count)]


ROUND_PAGES = 8


def other_pages(k_pool, v_pool, buffer, src, slot, dst, target, wanted, me, group_size):
    entry_ids = jnp.arange(src.shape[0])
    rank = masked_pick((src[None, :] == src[:, None]) & wanted[None, :] & (entry_ids[None, :] < entry_ids[:, None]), 1)
    most = jnp.max(jnp.where(wanted, rank + 1, 0))
    seat = jnp.where(wanted, src * src.shape[0] + rank, -1)

    def body(carry):
        done, buf = carry
        seats = ((jnp.arange(group_size) * src.shape[0])[:, None] + done + jnp.arange(ROUND_PAGES)[None, :]).reshape(-1)
        hit = seat[None, :] == seats[:, None]
        seat_slot = masked_pick(hit, slot[None, :])
        seat_target = jnp.where(jnp.any(hit & (dst == me)[None, :], axis=1), masked_pick(hit, target[None, :]), buf.shape[0])
        my_slots = lax.dynamic_slice_in_dim(seat_slot, me * ROUND_PAGES, ROUND_PAGES)
        pages = jnp.stack([jnp.take(k_pool, my_slots, axis=0), jnp.take(v_pool, my_slots, axis=0)], axis=1)
        gathered = lax.all_gather(pages, 'kv', axis=0, tiled=True)
        return done + ROUND_PAGES, buf.at[seat_target].set(gathered, mode='drop')

    return lax.while_loop(lambda carry: carry[0] < most, body, (jnp.zeros((), I32), buffer))[1]


def solution(mesh):
    group_size = mesh.shape['kv']
    pool_spec = P(('rep', 'kv'))
    tok_spec = P(None, ('rep', 'kv'), None)

    def device_fn(embeds, w_query, w_key, w_value, w_out, w_up, w_down, k_pool, v_pool, new_table, seq_lens, mig_src, mig_dst):
        me = lax.axis_index('kv')
        slots, layers, page_len, kv_heads, head_dim = k_pool.shape
        per_dev, width = embeds.shape[1:]
        seq_count, page_count = new_table.shape
        num_heads = w_query.shape[2] // head_dim
        pairs = [(i, i ^ 1) for i in range(group_size)]

        remap = new_table[:, :, None] == mig_dst
        is_moved = jnp.any(remap, axis=-1)
        old_table = jnp.where(is_moved, masked_pick(remap, mig_src), new_table)
        page_src = old_table // slots
        page_slot = old_table % slots
        dev, pos = place_sequences(page_src[:, 0], group_size, per_dev)
        place = dev * per_dev + pos

        page_ids = jnp.arange(page_count, dtype=I32)[None, :]
        page_rows = jnp.where(page_ids == 0, page_len, seq_lens[:, None] - page_len)

        src_dev, dst_dev = mig_src // slots, mig_dst // slots
        clear_slot = jnp.where(src_dev == me, mig_src % slots, -1)
        fill_slot = jnp.where(dst_dev == me, mig_dst % slots, -1)
        mig_meta = jnp.stack([clear_slot, fill_slot]).astype(I32)
        moved_cap = mig_src.shape[0] * MOVED_ROWS
        moved_rows = jnp.sum(jnp.where(remap, page_rows[:, :, None], 0), axis=(0, 1))
        moved_first = excl_cumsum(moved_rows)
        moved_fits = moved_first + moved_rows <= moved_cap
        moved_meta = jnp.stack([jnp.where(moved_fits, clear_slot, -1), moved_first, moved_rows])
        moved = [lax.psum(pack_rows((0,), k_pool, v_pool, moved_meta, moved_cap)[0], 'kv')]

        is_local = page_src == dev[:, None]
        in_moved = jnp.any(remap & moved_fits, axis=-1) & ~is_local
        same_dev_earlier = (dev[None, :] == dev[:, None]) & (pos[None, :] < pos[:, None])
        near_cap = per_dev * NEAR_ROWS
        by_next = (page_src[:, 1] == (dev + 1) % group_size) & ~is_moved[:, 1]
        near_first = masked_pick(same_dev_earlier & by_next[None, :], page_rows[None, :, 1])
        by_next = by_next & (near_first + page_rows[:, 1] <= near_cap)
        is_near = (page_ids == 1) & by_next[:, None]

        prev = (me + group_size - 1) % group_size
        prev_seat = prev * per_dev + jnp.arange(per_dev, dtype=I32)
        from_here = (place[None, :] == prev_seat[:, None]) & by_next[None, :]
        near_facts = jnp.stack([page_slot[:, 1] + 1, near_first, page_rows[:, 1]])
        near_meta = masked_pick(from_here[None, :, :], near_facts[:, None, :]) - jnp.array([[1], [0], [0]])
        other_shape = (per_dev * page_count, 2) + k_pool.shape[1:]
        far_shape = (seq_count, 2, STEPS, kv_heads, head_dim)
        *near_out, other, far_0, far_1 = pack_rows(tuple(range(layers)), k_pool, v_pool, near_meta, near_cap, [other_shape, far_shape, far_shape])

        my_dev = lax.dynamic_slice_in_dim(dev, me * per_dev, per_dev)
        my_pos = lax.dynamic_slice_in_dim(pos, me * per_dev, per_dev)
        home = jnp.arange(seq_count, dtype=I32) // per_dev
        distance = (dev - home) % group_size
        my_distance = (my_dev - me) % group_size
        at_pos = my_pos[None, :] == jnp.arange(per_dev, dtype=I32)[:, None]

        def send_embeds(step_away, hidden):
            sel = (at_pos & (my_distance == step_away)[None, :]).astype(embeds.dtype)
            rows = jnp.einsum('pb,tbd->ptd', sel, embeds, preferred_element_type=jnp.float32).astype(embeds.dtype)
            if step_away:
                rows = lax.ppermute(rows, 'kv', shift_by(group_size, step_away))
            return hidden + rows

        hidden = jnp.zeros((per_dev, STEPS, width), embeds.dtype)
        for step_away in range(group_size):
            hidden = lax.cond(jnp.any(distance == step_away), functools.partial(send_embeds, step_away), lambda same: same, hidden)
        hidden = hidden.reshape(per_dev * STEPS, width)
        near_out[0], hidden = lax.optimization_barrier((near_out[0], hidden))
        near = [lax.ppermute(near_out[0], 'kv', shift_by(group_size, -1))]

        wanted = ~(is_local | in_moved | is_near)
        kind = jnp.where(is_local, LOCAL, jnp.where(in_moved, MOVED, jnp.where(is_near, NEXT, OTHER)))
        target = pos[:, None] * page_count + page_ids
        entry_dst = jnp.broadcast_to(dev[:, None], page_src.shape)
        other = other_pages(k_pool, v_pool, other, page_src.reshape(-1), page_slot.reshape(-1), entry_dst.reshape(-1), target.reshape(-1), wanted.reshape(-1), me, group_size)
        mine = place[None, :] == (me * per_dev + jnp.arange(per_dev, dtype=I32))[:, None]
        facts = []
        for layer in range(layers):
            moved_at = masked_pick(remap, moved_first) if layer == 0 else masked_pick(remap, jnp.arange(mig_src.shape[0], dtype=I32)) * page_len
            index = jnp.where(is_local, page_slot, jnp.where(in_moved, moved_at, jnp.where(is_near, near_first[:, None], target)))
            facts.append(jnp.stack([kind[:, 0], index[:, 0], kind[:, 1], index[:, 1], seq_lens]))
        attend_meta = masked_pick(mine[None, None, :, :], jnp.stack(facts)[:, :, None, :]).astype(I32)

        row_dst = new_table[:, 1] // slots
        is_far = (row_dst != dev) & (row_dst != (dev + 1) % group_size)
        writes = new_table[None, :, 1] == (me * slots + jnp.arange(slots, dtype=I32))[:, None]
        owner_facts = jnp.stack([jnp.where(is_far, 0, 1 + pos + jnp.where(row_dst == dev, 0, per_dev)), seq_lens - page_len, jnp.where(is_far, 1 + place, 0)])
        owner_meta = (masked_pick(writes[None, :, :], owner_facts[:, None, :]) - jnp.array([[1], [0], [1]])).astype(I32)

        own_rows, prev_rows = [], []
        for layer in range(layers):
            queries = dense(hidden, w_query[layer]).astype(jnp.bfloat16)
            new_keys = dense(hidden, w_key[layer]).astype(jnp.bfloat16)
            new_vals = dense(hidden, w_value[layer]).astype(jnp.bfloat16)
            rows = jnp.stack([new_keys, new_vals]).reshape(2, per_dev, STEPS, kv_heads, head_dim).transpose(1, 0, 2, 3, 4)
            own_rows.append(rows)
            prev_rows.append(lax.ppermute(rows, 'kv', shift_by(group_size, 1)))
            q_rows = queries.reshape(per_dev, STEPS, num_heads, head_dim)
            if layer == 0:
                k_src, v_src, q_rows = lax.optimization_barrier((k_pool, v_pool, q_rows))
                k_base, v_base = copy_pools(k_src, v_src)
                q_rows, k_base, v_base = lax.optimization_barrier((q_rows, k_base, v_base))
            if layer == 0:
                full_out = list(pack_pages(tuple(range(layers)), k_pool, v_pool, clear_slot))
                for after in range(layers - 1, -1, -1):
                    full_out[after], moved[-1] = lax.optimization_barrier((full_out[after], moved[-1]))
                    moved.append(lax.psum(full_out[after], 'kv'))
                moved = [moved[0]] + moved[:0:-1]
            if layer + 1 < layers:
                near_next, near[layer] = lax.optimization_barrier((near_out[layer + 1], near[layer]))
                near.append(lax.ppermute(near_next, 'kv', shift_by(group_size, -1)))
            attn = attend(layer, q_rows, rows, k_pool, v_pool, moved[layer if layer == 0 else layer + 1], near[layer], other, attend_meta[layer]).reshape(per_dev * STEPS, num_heads * head_dim)
            hidden = (hidden.astype(jnp.float32) + dense(attn, w_out[layer])).astype(jnp.bfloat16)
            hidden = pair_mlp(hidden, w_up, w_down, layer, me % 2, pairs)

        far_rows = [lax.cond(jnp.any(is_far), lambda own, far: lax.all_gather(own, 'kv', axis=0, tiled=True), lambda own, far: far, own, far) for own, far in zip(own_rows, (far_0, far_1))]
        k_out, v_out = finish_pools(k_base, v_base, moved[1:], own_rows, prev_rows, far_rows, mig_meta, owner_meta)

        hidden = hidden.reshape(per_dev, STEPS, width)

        def bring_home(step_away, total):
            rows = lax.ppermute(hidden, 'kv', shift_by(group_size, -step_away)) if step_away else hidden
            sel = (at_pos & (my_distance == step_away)[None, :]).astype(hidden.dtype)
            return total + jnp.einsum('pb,ptd->tbd', sel, rows, preferred_element_type=jnp.float32).astype(hidden.dtype)

        y_out = jnp.zeros((STEPS, per_dev, width), hidden.dtype)
        for step_away in range(group_size):
            y_out = lax.cond(jnp.any(distance == step_away), functools.partial(bring_home, step_away), lambda same: same, y_out)
        return y_out, k_out, v_out

    return jax.shard_map(device_fn, mesh=mesh, in_specs=(tok_spec, P(), P(), P(), P(), P(), P(), pool_spec, pool_spec, P('rep', None), P('rep'), P('rep'), P('rep')), out_specs=(tok_spec, pool_spec, pool_spec), check_vma=False)
```

```python
import functools

import jax
import jax.numpy as jnp
from jax import lax
from jax.experimental import pallas as pl
from jax.experimental.pallas import tpu as pltpu
from jax.sharding import PartitionSpec as P


STEPS = 2
I32 = jnp.int32


def excl_cumsum(values):
    n = values.shape[0]
    before = jnp.arange(n)[None, :] < jnp.arange(n)[:, None]
    return jnp.sum(jnp.where(before, values[None, :], 0), axis=1)


def masked_pick(mask, values):
    return jnp.sum(jnp.where(mask, values, 0), axis=-1)


def place_sequences(pref, group_size, per_dev):
    count = pref.shape[0]
    ids = jnp.arange(count)
    earlier = ids[None, :] < ids[:, None]
    rank = jnp.sum((pref[None, :] == pref[:, None]) & earlier, axis=1)
    wanted = jnp.sum(pref[None, :] == jnp.arange(group_size)[:, None], axis=1)
    free = jnp.maximum(per_dev - wanted, 0)
    free_end = excl_cumsum(free) + free
    over = rank >= per_dev
    over_rank = jnp.sum(over[None, :] & earlier, axis=1)
    spill = jnp.sum(over_rank[:, None] >= free_end[None, :], axis=1)
    dev = jnp.where(over, spill, pref)
    pos = jnp.sum((dev[None, :] == dev[:, None]) & earlier, axis=1)
    return dev.astype(I32), pos.astype(I32)


def any_spec():
    return pl.BlockSpec(memory_space=pl.ANY)


def smem_spec():
    return pl.BlockSpec(memory_space=pltpu.SMEM)


def vmem_spec():
    return pl.BlockSpec(memory_space=pltpu.VMEM)


def start(copy):
    copy.start()


def wait(copy):
    copy.wait()


def for_all(count, table, row, make, act):
    def body(e, carry):
        @pl.when(table[row, e] >= 0)
        def _():
            for copy in make(e):
                act(copy)

        return carry

    lax.fori_loop(0, count, body, 0)


def page_copies(layer, k_pool, v_pool, slot, k_dst, v_dst, sem):
    return (pltpu.make_async_copy(k_pool.at[slot, layer], k_dst, sem), pltpu.make_async_copy(v_pool.at[slot, layer], v_dst, sem))


def pack_pages_kernel(layers, meta, k_pool, v_pool, *rest):
    outs = rest[:len(layers)]
    stage, in_sem, out_sem = rest[-3:]
    page_len = k_pool.shape[2]
    count = stage.shape[2] // page_len

    def fetch(at):
        def make(e):
            part = pl.ds(e * page_len, page_len)
            return page_copies(layers[at], k_pool, v_pool, meta[0, e], stage.at[at, 0, part], stage.at[at, 1, part], in_sem.at[at])

        return make

    for at in range(len(layers)):
        for_all(count, meta, 0, fetch(at), start)

    def wipe(e, carry):
        @pl.when(meta[0, e] < 0)
        def _():
            for at in range(len(layers)):
                for which in range(2):
                    stage[at, which, pl.ds(e * page_len, page_len)] = jnp.zeros((page_len,) + stage.shape[3:], stage.dtype)

        return carry

    lax.fori_loop(0, count, wipe, 0)
    for at in range(len(layers)):
        for_all(count, meta, 0, fetch(at), wait)
        pltpu.make_async_copy(stage.at[at], outs[at], out_sem.at[at]).start()
    for at in range(len(layers)):
        pltpu.make_async_copy(stage.at[at], outs[at], out_sem.at[at]).wait()


def pack_pages(layers, k_pool, v_pool, slot_of):
    shape = (2, slot_of.shape[0] * k_pool.shape[2]) + k_pool.shape[3:]
    return pl.pallas_call(
        functools.partial(pack_pages_kernel, layers),
        out_shape=[jax.ShapeDtypeStruct(shape, k_pool.dtype)] * len(layers),
        in_specs=[smem_spec(), any_spec(), any_spec()],
        out_specs=[any_spec()] * len(layers),
        scratch_shapes=[pltpu.VMEM((len(layers),) + shape, k_pool.dtype), pltpu.SemaphoreType.DMA((len(layers),)), pltpu.SemaphoreType.DMA((len(layers),))],
    )(slot_of[None, :].astype(I32), k_pool, v_pool)


def pack_rows_kernel(layers, meta, k_pool, v_pool, *rest):
    outs = rest[:len(layers)]
    pages, stage, in_sem, out_sem = rest[-4:]
    count = pages.shape[1]
    page_len = k_pool.shape[2]

    def fetch(at):
        return lambda e: page_copies(layers[at], k_pool, v_pool, meta[0, e], pages.at[at, e, 0], pages.at[at, e, 1], in_sem.at[at])

    for at in range(len(layers)):
        for_all(count, meta, 0, fetch(at), start)
    nothing = jnp.zeros((page_len,) + stage.shape[3:], stage.dtype)

    def wipe(i, carry):
        for at in range(len(layers)):
            for which in range(2):
                stage[at, which, pl.ds(i * page_len, page_len)] = nothing
        return carry

    lax.fori_loop(0, stage.shape[2] // page_len, wipe, 0)
    for at in range(len(layers)):
        for_all(count, meta, 0, fetch(at), wait)

        def place(e, carry):
            @pl.when(meta[0, e] >= 0)
            def _():
                for which in range(2):
                    stage[at, which, pl.ds(meta[1, e], page_len)] = pages[at, e, which]
                    stage[at, which, pl.ds(meta[1, e] + meta[2, e], page_len)] = nothing

            return carry

        lax.fori_loop(0, count, place, 0)
        pltpu.make_async_copy(stage.at[at], outs[at], out_sem.at[at]).start()
    for at in range(len(layers)):
        pltpu.make_async_copy(stage.at[at], outs[at], out_sem.at[at]).wait()


def pack_rows(layers, k_pool, v_pool, meta, cap, spare=()):
    count = meta.shape[1]
    page_len = k_pool.shape[2]
    shape = (2, cap + 2 * page_len) + k_pool.shape[3:]
    outs = [jax.ShapeDtypeStruct(shape, k_pool.dtype)] * len(layers) + [jax.ShapeDtypeStruct(s, k_pool.dtype) for s in spare]
    return pl.pallas_call(
        functools.partial(pack_rows_kernel, layers),
        out_shape=outs,
        in_specs=[smem_spec(), any_spec(), any_spec()],
        out_specs=[any_spec()] * len(outs),
        scratch_shapes=[
            pltpu.VMEM((len(layers), count, 2) + k_pool.shape[2:], k_pool.dtype),
            pltpu.VMEM((len(layers),) + shape, k_pool.dtype),
            pltpu.SemaphoreType.DMA((len(layers),)),
            pltpu.SemaphoreType.DMA((len(layers),)),
        ],
    )(meta.astype(I32), k_pool, v_pool)


LOCAL, MOVED, NEXT, OTHER = range(4)
MOVED_ROWS = 10
NEAR_ROWS = 9


def attend_kernel(layer, seqs, page_len, q_per_kv, unroll, meta, q_ref, new_ref, k_pool, v_pool, moved, near, other, out_ref, k_buf, v_buf, k_sem, v_sem):
    kv_heads, head_dim = k_buf.shape[2:]

    def launch(j, carry):
        for page in range(2):
            kind = meta[2 * page, j]
            index = meta[2 * page + 1, j]

            def both(k_src, v_src):
                dst = pl.ds(page * page_len, page_len)
                pltpu.make_async_copy(k_src, k_buf.at[j, dst], k_sem.at[j]).start()
                pltpu.make_async_copy(v_src, v_buf.at[j, dst], v_sem.at[j]).start()

            @pl.when(kind == LOCAL)
            def _():
                both(k_pool.at[index, layer], v_pool.at[index, layer])

            @pl.when(kind > LOCAL)
            def _():
                part = pl.ds(index, page_len)

                @pl.when(kind == MOVED)
                def _():
                    both(moved.at[0, part], moved.at[1, part])

                @pl.when(kind == NEXT)
                def _():
                    both(near.at[0, part], near.at[1, part])

                @pl.when(kind == OTHER)
                def _():
                    both(other.at[index, 0, layer], other.at[index, 1, layer])
        return carry

    lax.fori_loop(0, seqs, launch, 0)

    rows = STEPS * kv_heads * q_per_kv
    cols = 2 * page_len * kv_heads
    row_id = lax.broadcasted_iota(I32, (rows, cols), 0)
    col_id = lax.broadcasted_iota(I32, (rows, cols), 1)
    row_step = row_id // (kv_heads * q_per_kv)
    own_head = (col_id % kv_heads) == (row_id % (kv_heads * q_per_kv)) // q_per_kv
    lag = jnp.where(own_head, col_id // kv_heads - row_step, 1 << 20)

    def body(i, carry):
        for u in range(unroll):
            j = i * unroll + u
            pltpu.make_async_copy(k_buf.at[j], k_buf.at[j], k_sem.at[j]).wait()
            pltpu.make_async_copy(v_buf.at[j], v_buf.at[j], v_sem.at[j]).wait()
        for u in range(unroll):
            j = i * unroll + u
            length = meta[4, j]
            for step in range(STEPS):
                k_buf[j, length + step] = new_ref[j, 0, step]
                v_buf[j, length + step] = new_ref[j, 1, step]
        for u in range(unroll):
            j = i * unroll + u
            length = meta[4, j]
            keys = k_buf[j].reshape(cols, head_dim)
            vals = v_buf[j].reshape(cols, head_dim)
            query = q_ref[j].reshape(rows, head_dim)
            scores = lax.dot_general(query, keys, (((1,), (1,)), ((), ())), preferred_element_type=jnp.float32)
            scores = jnp.where(lag <= length, scores * head_dim ** -0.5, -jnp.inf)
            top = jnp.max(scores, axis=1, keepdims=True)
            probs = jnp.exp(scores - top)
            total = jnp.sum(probs, axis=1, keepdims=True)
            out = jnp.dot(probs.astype(vals.dtype), vals, preferred_element_type=jnp.float32) / total
            out_ref[j] = out.astype(out_ref.dtype).reshape(out_ref.shape[1:])
        return carry

    lax.fori_loop(0, seqs // unroll, body, 0)


def attend(layer, queries, new_rows, k_pool, v_pool, moved, near, other, meta):
    seqs = queries.shape[0]
    page_len, kv_heads, head_dim = k_pool.shape[2:]
    num_heads = queries.shape[2]
    buf = pltpu.VMEM((seqs, 2 * page_len, kv_heads, head_dim), k_pool.dtype)
    return pl.pallas_call(
        functools.partial(attend_kernel, layer, seqs, page_len, num_heads // kv_heads, 4),
        out_shape=jax.ShapeDtypeStruct(queries.shape, queries.dtype),
        in_specs=[smem_spec(), vmem_spec(), vmem_spec()] + [any_spec()] * 5,
        out_specs=vmem_spec(),
        scratch_shapes=[buf, buf, pltpu.SemaphoreType.DMA((seqs,)), pltpu.SemaphoreType.DMA((seqs,))],
        cost_estimate=pl.CostEstimate(flops=10 ** 10, bytes_accessed=10 ** 7, transcendentals=10 ** 6),
    )(meta, queries, new_rows, k_pool, v_pool, moved, near, other)


COPY_SLOTS = 16


def copy_kernel(k_pool, v_pool, k_out, v_out, stage, in_sem, out_sem):
    chunks = k_pool.shape[0] // COPY_SLOTS
    for pool, which in ((k_pool, 0), (v_pool, 1)):
        for c in range(chunks):
            part = pl.ds(c * COPY_SLOTS, COPY_SLOTS)
            pltpu.make_async_copy(pool.at[part], stage.at[which, part], in_sem.at[which, c]).start()
    for pool, out, which in ((k_pool, k_out, 0), (v_pool, v_out, 1)):
        for c in range(chunks):
            part = pl.ds(c * COPY_SLOTS, COPY_SLOTS)
            pltpu.make_async_copy(pool.at[part], stage.at[which, part], in_sem.at[which, c]).wait()
            pltpu.make_async_copy(stage.at[which, part], out.at[part], out_sem.at[which, c]).start()
    for out, which in ((k_out, 0), (v_out, 1)):
        for c in range(chunks):
            part = pl.ds(c * COPY_SLOTS, COPY_SLOTS)
            pltpu.make_async_copy(stage.at[which, part], out.at[part], out_sem.at[which, c]).wait()


def copy_pools(k_pool, v_pool):
    chunks = k_pool.shape[0] // COPY_SLOTS
    pool = jax.ShapeDtypeStruct(k_pool.shape, k_pool.dtype)
    return pl.pallas_call(
        copy_kernel,
        out_shape=[pool, pool],
        in_specs=[any_spec(), any_spec()],
        out_specs=[any_spec(), any_spec()],
        scratch_shapes=[pltpu.VMEM((2,) + k_pool.shape, k_pool.dtype), pltpu.SemaphoreType.DMA((2, chunks)), pltpu.SemaphoreType.DMA((2, chunks))],
        name='copy_pools',
    )(k_pool, v_pool)


def finish_kernel(layers, slots, entries, mig, owner, k_in, v_in, *rest):
    del k_in, v_in
    moved, own, prev, far = (rest[i * layers:(i + 1) * layers] for i in range(4))
    k_out, v_out, zeros, stage, row_stage, far_stage, zero_sem, in_sem, out_sem, row_in_sem, row_sem, far_sem = rest[4 * layers:]
    page_len = k_out.shape[2]
    seats = own[0].shape[0]

    def fetch(e):
        part = pl.ds(e * page_len, page_len)
        return [pltpu.make_async_copy(moved[layer].at[which, part], stage.at[e, layer, which], in_sem.at[e]) for layer in range(layers) for which in range(2)]

    def put(e):
        return [pltpu.make_async_copy(stage.at[e, layer, which], out.at[mig[1, e], layer], out_sem.at[0]) for layer in range(layers) for which, out in enumerate((k_out, v_out))]

    def clear(e):
        return [pltpu.make_async_copy(zeros, out.at[mig[0, e]], zero_sem.at[0]) for out in (k_out, v_out)]

    def load(layer):
        return (pltpu.make_async_copy(own[layer], row_stage.at[layer, pl.ds(0, seats)], row_in_sem.at[layer]),
                pltpu.make_async_copy(prev[layer], row_stage.at[layer, pl.ds(seats, seats)], row_in_sem.at[layer]))

    def fill(j):
        dst = pl.ds(owner[1, j], STEPS)
        return [pltpu.make_async_copy(row_stage.at[layer, owner[0, j], which], out.at[j, layer, dst], row_sem.at[0]) for layer in range(layers) for which, out in enumerate((k_out, v_out))]

    for_all(entries, mig, 1, fetch, start)
    for layer in range(layers):
        for copy in load(layer):
            copy.start()
    zeros[...] = jnp.zeros_like(zeros)

    def relay(e, carry):
        @pl.when(mig[1, e] >= 0)
        def _():
            for copy in fetch(e):
                copy.wait()
            for copy in put(e):
                copy.start()

        return carry

    lax.fori_loop(0, entries, relay, 0)
    for_all(entries, mig, 0, clear, start)
    for_all(entries, mig, 1, put, wait)
    for layer in range(layers):
        for copy in load(layer):
            copy.wait()
    for_all(slots, owner, 0, fill, start)

    def from_far(j, carry):
        @pl.when(owner[2, j] >= 0)
        def _():
            dst = pl.ds(owner[1, j], STEPS)
            for layer in range(layers):
                copy = pltpu.make_async_copy(far[layer].at[owner[2, j]], far_stage, far_sem.at[0])
                copy.start()
                copy.wait()
                for which, out in enumerate((k_out, v_out)):
                    copy = pltpu.make_async_copy(far_stage.at[which], out.at[j, layer, dst], far_sem.at[0])
                    copy.start()
                    copy.wait()

        return carry

    lax.fori_loop(0, slots, from_far, 0)
    for_all(entries, mig, 0, clear, wait)
    for_all(slots, owner, 0, fill, wait)


def finish_pools(k_pool, v_pool, moved, own, prev, far, mig, owner):
    slots, layers = k_pool.shape[:2]
    entries = mig.shape[1]
    pool = jax.ShapeDtypeStruct(k_pool.shape, k_pool.dtype)
    row_shape = own[0].shape
    return pl.pallas_call(
        functools.partial(finish_kernel, layers, slots, entries),
        out_shape=[pool, pool],
        in_specs=[smem_spec(), smem_spec()] + [any_spec()] * (2 + 4 * layers),
        out_specs=[any_spec(), any_spec()],
        input_output_aliases={2: 0, 3: 1},
        scratch_shapes=[
            pltpu.VMEM(k_pool.shape[1:], k_pool.dtype),
            pltpu.VMEM((entries, layers, 2) + k_pool.shape[2:], k_pool.dtype),
            pltpu.VMEM((layers, 2 * row_shape[0]) + row_shape[1:], k_pool.dtype),
            pltpu.VMEM(row_shape[1:], k_pool.dtype),
            pltpu.SemaphoreType.DMA((1,)),
            pltpu.SemaphoreType.DMA((entries,)),
            pltpu.SemaphoreType.DMA((1,)),
            pltpu.SemaphoreType.DMA((layers,)),
            pltpu.SemaphoreType.DMA((1,)),
            pltpu.SemaphoreType.DMA((1,)),
        ],
        cost_estimate=pl.CostEstimate(flops=10 ** 10, bytes_accessed=10 ** 7, transcendentals=0),
        name='finish_pools',
    )(mig, owner, k_pool, v_pool, *moved, *own, *prev, *far)


def dense(hidden, weight):
    return jnp.dot(hidden, weight, preferred_element_type=jnp.float32)


def pair_mlp(hidden, w_up, w_down, layer, core, pairs):
    rows = hidden.shape[0]
    width, full = w_up.shape[1:]
    half = full // 2
    both = jnp.concatenate([hidden, lax.ppermute(hidden, 'kv', pairs)])
    up_proj = dense(both, lax.dynamic_slice(w_up, (layer, 0, core * half), (1, width, half))[0]).astype(jnp.bfloat16)
    act = jax.nn.gelu(up_proj.astype(jnp.float32), approximate=True).astype(jnp.bfloat16)
    part = dense(act, lax.dynamic_slice(w_down, (layer, core * half, 0), (1, half, width))[0])
    rest = lax.ppermute(part[rows:], 'kv', pairs)
    return (hidden.astype(jnp.float32) + (part[:rows] + rest)).astype(jnp.bfloat16)


def shift_by(count, distance):
    return [(i, (i + distance) % count) for i in range(count)]


ROUND_PAGES = 8


def other_pages(k_pool, v_pool, buffer, src, slot, dst, target, wanted, me, group_size):
    entry_ids = jnp.arange(src.shape[0])
    rank = masked_pick((src[None, :] == src[:, None]) & wanted[None, :] & (entry_ids[None, :] < entry_ids[:, None]), 1)
    most = jnp.max(jnp.where(wanted, rank + 1, 0))
    seat = jnp.where(wanted, src * src.shape[0] + rank, -1)

    def body(carry):
        done, buf = carry
        seats = ((jnp.arange(group_size) * src.shape[0])[:, None] + done + jnp.arange(ROUND_PAGES)[None, :]).reshape(-1)
        hit = seat[None, :] == seats[:, None]
        seat_slot = masked_pick(hit, slot[None, :])
        seat_target = jnp.where(jnp.any(hit & (dst == me)[None, :], axis=1), masked_pick(hit, target[None, :]), buf.shape[0])
        my_slots = lax.dynamic_slice_in_dim(seat_slot, me * ROUND_PAGES, ROUND_PAGES)
        pages = jnp.stack([jnp.take(k_pool, my_slots, axis=0), jnp.take(v_pool, my_slots, axis=0)], axis=1)
        gathered = lax.all_gather(pages, 'kv', axis=0, tiled=True)
        return done + ROUND_PAGES, buf.at[seat_target].set(gathered, mode='drop')

    return lax.while_loop(lambda carry: carry[0] < most, body, (jnp.zeros((), I32), buffer))[1]


def solution(mesh):
    group_size = mesh.shape['kv']
    pool_spec = P(('rep', 'kv'))
    tok_spec = P(None, ('rep', 'kv'), None)

    def device_fn(embeds, w_query, w_key, w_value, w_out, w_up, w_down, k_pool, v_pool, new_table, seq_lens, mig_src, mig_dst):
        me = lax.axis_index('kv')
        slots, layers, page_len, kv_heads, head_dim = k_pool.shape
        per_dev, width = embeds.shape[1:]
        seq_count, page_count = new_table.shape
        num_heads = w_query.shape[2] // head_dim
        pairs = [(i, i ^ 1) for i in range(group_size)]

        remap = new_table[:, :, None] == mig_dst
        is_moved = jnp.any(remap, axis=-1)
        old_table = jnp.where(is_moved, masked_pick(remap, mig_src), new_table)
        page_src = old_table // slots
        page_slot = old_table % slots

        page_ids = jnp.arange(page_count, dtype=I32)[None, :]
        page_rows = jnp.where(page_ids == 0, page_len, seq_lens[:, None] - page_len)

        src_dev, dst_dev = mig_src // slots, mig_dst // slots
        clear_slot = jnp.where(src_dev == me, mig_src % slots, -1)
        fill_slot = jnp.where(dst_dev == me, mig_dst % slots, -1)
        mig_meta = jnp.stack([clear_slot, fill_slot]).astype(I32)
        moved_cap = mig_src.shape[0] * MOVED_ROWS
        moved_rows = jnp.sum(jnp.where(remap, page_rows[:, :, None], 0), axis=(0, 1))
        moved_first = excl_cumsum(moved_rows)
        moved_fits = moved_first + moved_rows <= moved_cap
        moved_meta = jnp.stack([jnp.where(moved_fits, clear_slot, -1), moved_first, moved_rows])
        moved_out = pack_rows((0,), k_pool, v_pool, moved_meta, moved_cap)[0]
        moved_out, new_table, page_src, page_slot = lax.optimization_barrier((moved_out, new_table, page_src, page_slot))
        moved = [lax.psum(moved_out, 'kv')]

        dev, pos = place_sequences(page_src[:, 0], group_size, per_dev)
        place = dev * per_dev + pos

        is_local = page_src == dev[:, None]
        in_moved = jnp.any(remap & moved_fits, axis=-1) & ~is_local
        same_dev_earlier = (dev[None, :] == dev[:, None]) & (pos[None, :] < pos[:, None])
        near_cap = per_dev * NEAR_ROWS
        by_next = (page_src[:, 1] == (dev + 1) % group_size) & ~is_moved[:, 1]
        near_first = masked_pick(same_dev_earlier & by_next[None, :], page_rows[None, :, 1])
        by_next = by_next & (near_first + page_rows[:, 1] <= near_cap)
        is_near = (page_ids == 1) & by_next[:, None]

        prev = (me + group_size - 1) % group_size
        prev_seat = prev * per_dev + jnp.arange(per_dev, dtype=I32)
        from_here = (place[None, :] == prev_seat[:, None]) & by_next[None, :]
        near_facts = jnp.stack([page_slot[:, 1] + 1, near_first, page_rows[:, 1]])
        near_meta = masked_pick(from_here[None, :, :], near_facts[:, None, :]) - jnp.array([[1], [0], [0]])
        other_shape = (per_dev * page_count, 2) + k_pool.shape[1:]
        far_shape = (seq_count, 2, STEPS, kv_heads, head_dim)
        *near_out, other, far_0, far_1 = pack_rows(tuple(range(layers)), k_pool, v_pool, near_meta, near_cap, [other_shape, far_shape, far_shape])
        near_out[0], embeds = lax.optimization_barrier((near_out[0], embeds))

        my_dev = lax.dynamic_slice_in_dim(dev, me * per_dev, per_dev)
        my_pos = lax.dynamic_slice_in_dim(pos, me * per_dev, per_dev)
        home = jnp.arange(seq_count, dtype=I32) // per_dev
        distance = (dev - home) % group_size
        my_distance = (my_dev - me) % group_size
        at_pos = my_pos[None, :] == jnp.arange(per_dev, dtype=I32)[:, None]

        def send_embeds(step_away, hidden):
            sel = (at_pos & (my_distance == step_away)[None, :]).astype(embeds.dtype)
            rows = jnp.einsum('pb,tbd->ptd', sel, embeds, preferred_element_type=jnp.float32).astype(embeds.dtype)
            if step_away:
                rows = lax.ppermute(rows, 'kv', shift_by(group_size, step_away))
            return hidden + rows

        hidden = jnp.zeros((per_dev, STEPS, width), embeds.dtype)
        for step_away in range(group_size):
            hidden = lax.cond(jnp.any(distance == step_away), functools.partial(send_embeds, step_away), lambda same: same, hidden)
        hidden = hidden.reshape(per_dev * STEPS, width)
        near_out[0], hidden = lax.optimization_barrier((near_out[0], hidden))
        near = [lax.ppermute(near_out[0], 'kv', shift_by(group_size, -1))]

        wanted = ~(is_local | in_moved | is_near)
        kind = jnp.where(is_local, LOCAL, jnp.where(in_moved, MOVED, jnp.where(is_near, NEXT, OTHER)))
        target = pos[:, None] * page_count + page_ids
        entry_dst = jnp.broadcast_to(dev[:, None], page_src.shape)
        other = other_pages(k_pool, v_pool, other, page_src.reshape(-1), page_slot.reshape(-1), entry_dst.reshape(-1), target.reshape(-1), wanted.reshape(-1), me, group_size)
        mine = place[None, :] == (me * per_dev + jnp.arange(per_dev, dtype=I32))[:, None]
        facts = []
        for layer in range(layers):
            moved_at = masked_pick(remap, moved_first) if layer == 0 else masked_pick(remap, jnp.arange(mig_src.shape[0], dtype=I32)) * page_len
            index = jnp.where(is_local, page_slot, jnp.where(in_moved, moved_at, jnp.where(is_near, near_first[:, None], target)))
            facts.append(jnp.stack([kind[:, 0], index[:, 0], kind[:, 1], index[:, 1], seq_lens]))
        attend_meta = masked_pick(mine[None, None, :, :], jnp.stack(facts)[:, :, None, :]).astype(I32)

        row_dst = new_table[:, 1] // slots
        is_far = (row_dst != dev) & (row_dst != (dev + 1) % group_size)
        writes = new_table[None, :, 1] == (me * slots + jnp.arange(slots, dtype=I32))[:, None]
        owner_facts = jnp.stack([jnp.where(is_far, 0, 1 + pos + jnp.where(row_dst == dev, 0, per_dev)), seq_lens - page_len, jnp.where(is_far, 1 + place, 0)])
        owner_meta = (masked_pick(writes[None, :, :], owner_facts[:, None, :]) - jnp.array([[1], [0], [1]])).astype(I32)

        own_rows, prev_rows = [], []
        for layer in range(layers):
            queries = dense(hidden, w_query[layer]).astype(jnp.bfloat16)
            new_keys = dense(hidden, w_key[layer]).astype(jnp.bfloat16)
            new_vals = dense(hidden, w_value[layer]).astype(jnp.bfloat16)
            rows = jnp.stack([new_keys, new_vals]).reshape(2, per_dev, STEPS, kv_heads, head_dim).transpose(1, 0, 2, 3, 4)
            own_rows.append(rows)
            prev_rows.append(lax.ppermute(rows, 'kv', shift_by(group_size, 1)))
            q_rows = queries.reshape(per_dev, STEPS, num_heads, head_dim)
            if layer == 0:
                k_src, v_src, q_rows = lax.optimization_barrier((k_pool, v_pool, q_rows))
                k_base, v_base = copy_pools(k_src, v_src)
                q_rows, k_base, v_base = lax.optimization_barrier((q_rows, k_base, v_base))
            if layer == 0:
                full_out = list(pack_pages(tuple(range(layers)), k_pool, v_pool, clear_slot))
                for after in range(layers - 1, -1, -1):
                    full_out[after], moved[-1] = lax.optimization_barrier((full_out[after], moved[-1]))
                    moved.append(lax.psum(full_out[after], 'kv'))
                moved = [moved[0]] + moved[:0:-1]
            if layer + 1 < layers:
                near_next, near[layer] = lax.optimization_barrier((near_out[layer + 1], near[layer]))
                near.append(lax.ppermute(near_next, 'kv', shift_by(group_size, -1)))
            attn = attend(layer, q_rows, rows, k_pool, v_pool, moved[layer if layer == 0 else layer + 1], near[layer], other, attend_meta[layer]).reshape(per_dev * STEPS, num_heads * head_dim)
            hidden = (hidden.astype(jnp.float32) + dense(attn, w_out[layer])).astype(jnp.bfloat16)
            hidden = pair_mlp(hidden, w_up, w_down, layer, me % 2, pairs)

        hidden, moved[1], *far_in = lax.optimization_barrier((hidden, moved[1], *own_rows))
        far_rows = lax.cond(jnp.any(is_far), lambda own, far: [lax.all_gather(rows, 'kv', axis=0, tiled=True) for rows in own], lambda own, far: far, far_in, [far_0, far_1])
        hidden = hidden.reshape(per_dev, STEPS, width)

        def bring_home(step_away, total):
            rows = lax.ppermute(hidden, 'kv', shift_by(group_size, -step_away)) if step_away else hidden
            sel = (at_pos & (my_distance == step_away)[None, :]).astype(hidden.dtype)
            return total + jnp.einsum('pb,ptd->tbd', sel, rows, preferred_element_type=jnp.float32).astype(hidden.dtype)

        def bring_most(step_away, k_base, v_base):
            rows = lax.ppermute(hidden, 'kv', shift_by(group_size, -step_away)) if step_away else hidden
            k_out, v_out = finish_pools(k_base, v_base, moved[1:], own_rows, prev_rows, far_rows, mig_meta, owner_meta)
            sel = (at_pos & (my_distance == step_away)[None, :]).astype(hidden.dtype)
            return jnp.einsum('pb,ptd->tbd', sel, rows, preferred_element_type=jnp.float32).astype(hidden.dtype), k_out, v_out

        counts = jnp.sum(distance[None, :] == jnp.arange(group_size, dtype=I32)[:, None], axis=1)
        most = jnp.argmax(counts).astype(I32)
        y_out, k_out, v_out = lax.switch(most, [functools.partial(bring_most, step_away) for step_away in range(group_size)], k_base, v_base)
        for step_away in range(group_size):
            y_out = lax.cond((counts[step_away] > 0) & (most != step_away), functools.partial(bring_home, step_away), lambda same: same, y_out)
        return y_out, k_out, v_out

    return jax.shard_map(device_fn, mesh=mesh, in_specs=(tok_spec, P(), P(), P(), P(), P(), P(), pool_spec, pool_spec, P('rep', None), P('rep'), P('rep'), P('rep')), out_specs=(tok_spec, pool_spec, pool_spec), check_vma=False)
```

```python
import functools

import jax
import jax.numpy as jnp
from jax import lax
from jax.experimental import pallas as pl
from jax.experimental.pallas import tpu as pltpu
from jax.sharding import PartitionSpec as P


STEPS = 2
I32 = jnp.int32


def excl_cumsum(values):
    n = values.shape[0]
    before = jnp.arange(n)[None, :] < jnp.arange(n)[:, None]
    return jnp.sum(jnp.where(before, values[None, :], 0), axis=1)


def masked_pick(mask, values):
    return jnp.sum(jnp.where(mask, values, 0), axis=-1)


def place_sequences(pref, group_size, per_dev):
    count = pref.shape[0]
    ids = jnp.arange(count)
    earlier = ids[None, :] < ids[:, None]
    rank = jnp.sum((pref[None, :] == pref[:, None]) & earlier, axis=1)
    wanted = jnp.sum(pref[None, :] == jnp.arange(group_size)[:, None], axis=1)
    free = jnp.maximum(per_dev - wanted, 0)
    free_end = excl_cumsum(free) + free
    over = rank >= per_dev
    over_rank = jnp.sum(over[None, :] & earlier, axis=1)
    spill = jnp.sum(over_rank[:, None] >= free_end[None, :], axis=1)
    dev = jnp.where(over, spill, pref)
    pos = jnp.sum((dev[None, :] == dev[:, None]) & earlier, axis=1)
    return dev.astype(I32), pos.astype(I32)


def any_spec():
    return pl.BlockSpec(memory_space=pl.ANY)


def smem_spec():
    return pl.BlockSpec(memory_space=pltpu.SMEM)


def vmem_spec():
    return pl.BlockSpec(memory_space=pltpu.VMEM)


def start(copy):
    copy.start()


def wait(copy):
    copy.wait()


def for_all(count, table, row, make, act):
    def body(e, carry):
        @pl.when(table[row, e] >= 0)
        def _():
            for copy in make(e):
                act(copy)

        return carry

    lax.fori_loop(0, count, body, 0)


def page_copies(layer, k_pool, v_pool, slot, k_dst, v_dst, sem):
    return (pltpu.make_async_copy(k_pool.at[slot, layer], k_dst, sem), pltpu.make_async_copy(v_pool.at[slot, layer], v_dst, sem))


def pack_pages_kernel(layers, meta, k_pool, v_pool, *rest):
    outs = rest[:len(layers)]
    stage, in_sem, out_sem = rest[-3:]
    page_len = k_pool.shape[2]
    count = stage.shape[2] // page_len

    def fetch(at):
        def make(e):
            part = pl.ds(e * page_len, page_len)
            return page_copies(layers[at], k_pool, v_pool, meta[0, e], stage.at[at, 0, part], stage.at[at, 1, part], in_sem.at[at])

        return make

    for at in range(len(layers)):
        for_all(count, meta, 0, fetch(at), start)

    def wipe(e, carry):
        @pl.when(meta[0, e] < 0)
        def _():
            for at in range(len(layers)):
                for which in range(2):
                    stage[at, which, pl.ds(e * page_len, page_len)] = jnp.zeros((page_len,) + stage.shape[3:], stage.dtype)

        return carry

    lax.fori_loop(0, count, wipe, 0)
    for at in range(len(layers)):
        for_all(count, meta, 0, fetch(at), wait)
        pltpu.make_async_copy(stage.at[at], outs[at], out_sem.at[at]).start()
    for at in range(len(layers)):
        pltpu.make_async_copy(stage.at[at], outs[at], out_sem.at[at]).wait()


def pack_pages(layers, k_pool, v_pool, slot_of):
    shape = (2, slot_of.shape[0] * k_pool.shape[2]) + k_pool.shape[3:]
    return pl.pallas_call(
        functools.partial(pack_pages_kernel, layers),
        out_shape=[jax.ShapeDtypeStruct(shape, k_pool.dtype)] * len(layers),
        in_specs=[smem_spec(), any_spec(), any_spec()],
        out_specs=[any_spec()] * len(layers),
        scratch_shapes=[pltpu.VMEM((len(layers),) + shape, k_pool.dtype), pltpu.SemaphoreType.DMA((len(layers),)), pltpu.SemaphoreType.DMA((len(layers),))],
        cost_estimate=pl.CostEstimate(flops=10 ** 10, bytes_accessed=10 ** 7, transcendentals=0),
    )(slot_of[None, :].astype(I32), k_pool, v_pool)


def pack_rows_kernel(layers, meta, k_pool, v_pool, *rest):
    outs = rest[:len(layers)]
    pages, stage, in_sem, out_sem = rest[-4:]
    count = pages.shape[1]
    page_len = k_pool.shape[2]

    def fetch(at):
        return lambda e: page_copies(layers[at], k_pool, v_pool, meta[0, e], pages.at[at, e, 0], pages.at[at, e, 1], in_sem.at[at])

    for at in range(len(layers)):
        for_all(count, meta, 0, fetch(at), start)
    nothing = jnp.zeros((page_len,) + stage.shape[3:], stage.dtype)

    def wipe(i, carry):
        for at in range(len(layers)):
            for which in range(2):
                stage[at, which, pl.ds(i * page_len, page_len)] = nothing
        return carry

    lax.fori_loop(0, stage.shape[2] // page_len, wipe, 0)
    for at in range(len(layers)):
        for_all(count, meta, 0, fetch(at), wait)

        def place(e, carry):
            @pl.when(meta[0, e] >= 0)
            def _():
                for which in range(2):
                    stage[at, which, pl.ds(meta[1, e], page_len)] = pages[at, e, which]
                    stage[at, which, pl.ds(meta[1, e] + meta[2, e], page_len)] = nothing

            return carry

        lax.fori_loop(0, count, place, 0)
        pltpu.make_async_copy(stage.at[at], outs[at], out_sem.at[at]).start()
    for at in range(len(layers)):
        pltpu.make_async_copy(stage.at[at], outs[at], out_sem.at[at]).wait()


def pack_rows(layers, k_pool, v_pool, meta, cap, spare=()):
    count = meta.shape[1]
    page_len = k_pool.shape[2]
    shape = (2, cap + 2 * page_len) + k_pool.shape[3:]
    outs = [jax.ShapeDtypeStruct(shape, k_pool.dtype)] * len(layers) + [jax.ShapeDtypeStruct(s, k_pool.dtype) for s in spare]
    return pl.pallas_call(
        functools.partial(pack_rows_kernel, layers),
        out_shape=outs,
        in_specs=[smem_spec(), any_spec(), any_spec()],
        out_specs=[any_spec()] * len(outs),
        scratch_shapes=[
            pltpu.VMEM((len(layers), count, 2) + k_pool.shape[2:], k_pool.dtype),
            pltpu.VMEM((len(layers),) + shape, k_pool.dtype),
            pltpu.SemaphoreType.DMA((len(layers),)),
            pltpu.SemaphoreType.DMA((len(layers),)),
        ],
        cost_estimate=pl.CostEstimate(flops=10 ** 10, bytes_accessed=10 ** 7, transcendentals=0),
    )(meta.astype(I32), k_pool, v_pool)


def gate(value):
    def kernel(src, dst):
        dst[...] = src[...]

    return pl.pallas_call(kernel, out_shape=jax.ShapeDtypeStruct(value.shape, value.dtype), name='gate')(value)


LOCAL, MOVED, NEXT, OTHER = range(4)
MOVED_ROWS = 10
NEAR_ROWS = 9


def attend_kernel(layer, seqs, page_len, q_per_kv, unroll, meta, q_ref, new_ref, k_pool, v_pool, moved, near, other, out_ref, k_buf, v_buf, k_sem, v_sem):
    kv_heads, head_dim = k_buf.shape[2:]

    def launch(j, carry):
        for page in range(2):
            kind = meta[2 * page, j]
            index = meta[2 * page + 1, j]

            def both(k_src, v_src):
                dst = pl.ds(page * page_len, page_len)
                pltpu.make_async_copy(k_src, k_buf.at[j, dst], k_sem.at[j]).start()
                pltpu.make_async_copy(v_src, v_buf.at[j, dst], v_sem.at[j]).start()

            @pl.when(kind == LOCAL)
            def _():
                both(k_pool.at[index, layer], v_pool.at[index, layer])

            @pl.when(kind > LOCAL)
            def _():
                part = pl.ds(index, page_len)

                @pl.when(kind == MOVED)
                def _():
                    both(moved.at[0, part], moved.at[1, part])

                @pl.when(kind == NEXT)
                def _():
                    both(near.at[0, part], near.at[1, part])

                @pl.when(kind == OTHER)
                def _():
                    both(other.at[index, 0, layer], other.at[index, 1, layer])
        return carry

    lax.fori_loop(0, seqs, launch, 0)

    rows = STEPS * kv_heads * q_per_kv
    cols = 2 * page_len * kv_heads
    row_id = lax.broadcasted_iota(I32, (rows, cols), 0)
    col_id = lax.broadcasted_iota(I32, (rows, cols), 1)
    row_step = row_id // (kv_heads * q_per_kv)
    own_head = (col_id % kv_heads) == (row_id % (kv_heads * q_per_kv)) // q_per_kv
    lag = jnp.where(own_head, col_id // kv_heads - row_step, 1 << 20)

    def body(i, carry):
        for u in range(unroll):
            j = i * unroll + u
            pltpu.make_async_copy(k_buf.at[j], k_buf.at[j], k_sem.at[j]).wait()
            pltpu.make_async_copy(v_buf.at[j], v_buf.at[j], v_sem.at[j]).wait()
        for u in range(unroll):
            j = i * unroll + u
            length = meta[4, j]
            for step in range(STEPS):
                k_buf[j, length + step] = new_ref[j, 0, step]
                v_buf[j, length + step] = new_ref[j, 1, step]
        for u in range(unroll):
            j = i * unroll + u
            length = meta[4, j]
            keys = k_buf[j].reshape(cols, head_dim)
            vals = v_buf[j].reshape(cols, head_dim)
            query = q_ref[j].reshape(rows, head_dim)
            scores = lax.dot_general(query, keys, (((1,), (1,)), ((), ())), preferred_element_type=jnp.float32)
            scores = jnp.where(lag <= length, scores * head_dim ** -0.5, -jnp.inf)
            top = jnp.max(scores, axis=1, keepdims=True)
            probs = jnp.exp(scores - top)
            total = jnp.sum(probs, axis=1, keepdims=True)
            out = jnp.dot(probs.astype(vals.dtype), vals, preferred_element_type=jnp.float32) / total
            out_ref[j] = out.astype(out_ref.dtype).reshape(out_ref.shape[1:])
        return carry

    lax.fori_loop(0, seqs // unroll, body, 0)


def attend(layer, queries, new_rows, k_pool, v_pool, moved, near, other, meta):
    seqs = queries.shape[0]
    page_len, kv_heads, head_dim = k_pool.shape[2:]
    num_heads = queries.shape[2]
    buf = pltpu.VMEM((seqs, 2 * page_len, kv_heads, head_dim), k_pool.dtype)
    return pl.pallas_call(
        functools.partial(attend_kernel, layer, seqs, page_len, num_heads // kv_heads, 4),
        out_shape=jax.ShapeDtypeStruct(queries.shape, queries.dtype),
        in_specs=[smem_spec(), vmem_spec(), vmem_spec()] + [any_spec()] * 5,
        out_specs=vmem_spec(),
        scratch_shapes=[buf, buf, pltpu.SemaphoreType.DMA((seqs,)), pltpu.SemaphoreType.DMA((seqs,))],
        cost_estimate=pl.CostEstimate(flops=10 ** 10, bytes_accessed=10 ** 7, transcendentals=10 ** 6),
    )(meta, queries, new_rows, k_pool, v_pool, moved, near, other)


COPY_SLOTS = 16


def copy_kernel(k_pool, v_pool, k_out, v_out, stage, in_sem, out_sem):
    chunks = k_pool.shape[0] // COPY_SLOTS
    for pool, which in ((k_pool, 0), (v_pool, 1)):
        for c in range(chunks):
            part = pl.ds(c * COPY_SLOTS, COPY_SLOTS)
            pltpu.make_async_copy(pool.at[part], stage.at[which, part], in_sem.at[which, c]).start()
    for pool, out, which in ((k_pool, k_out, 0), (v_pool, v_out, 1)):
        for c in range(chunks):
            part = pl.ds(c * COPY_SLOTS, COPY_SLOTS)
            pltpu.make_async_copy(pool.at[part], stage.at[which, part], in_sem.at[which, c]).wait()
            pltpu.make_async_copy(stage.at[which, part], out.at[part], out_sem.at[which, c]).start()
    for out, which in ((k_out, 0), (v_out, 1)):
        for c in range(chunks):
            part = pl.ds(c * COPY_SLOTS, COPY_SLOTS)
            pltpu.make_async_copy(stage.at[which, part], out.at[part], out_sem.at[which, c]).wait()


def copy_pools(k_pool, v_pool):
    chunks = k_pool.shape[0] // COPY_SLOTS
    pool = jax.ShapeDtypeStruct(k_pool.shape, k_pool.dtype)
    return pl.pallas_call(
        copy_kernel,
        out_shape=[pool, pool],
        in_specs=[any_spec(), any_spec()],
        out_specs=[any_spec(), any_spec()],
        scratch_shapes=[pltpu.VMEM((2,) + k_pool.shape, k_pool.dtype), pltpu.SemaphoreType.DMA((2, chunks)), pltpu.SemaphoreType.DMA((2, chunks))],
        cost_estimate=pl.CostEstimate(flops=10 ** 10, bytes_accessed=10 ** 7, transcendentals=0),
        name='copy_pools',
    )(k_pool, v_pool)


def finish_kernel(layers, slots, entries, mig, owner, k_in, v_in, *rest):
    del k_in, v_in
    moved, own, prev, far = (rest[i * layers:(i + 1) * layers] for i in range(4))
    k_out, v_out, zeros, stage, row_stage, far_stage, zero_sem, in_sem, out_sem, row_in_sem, row_sem, far_sem = rest[4 * layers:]
    page_len = k_out.shape[2]
    seats = own[0].shape[0]

    def fetch(e):
        part = pl.ds(e * page_len, page_len)
        return [pltpu.make_async_copy(moved[layer].at[which, part], stage.at[e, layer, which], in_sem.at[e]) for layer in range(layers) for which in range(2)]

    def put(e):
        return [pltpu.make_async_copy(stage.at[e, layer, which], out.at[mig[1, e], layer], out_sem.at[0]) for layer in range(layers) for which, out in enumerate((k_out, v_out))]

    def clear(e):
        return [pltpu.make_async_copy(zeros, out.at[mig[0, e]], zero_sem.at[0]) for out in (k_out, v_out)]

    def load(layer):
        return (pltpu.make_async_copy(own[layer], row_stage.at[layer, pl.ds(0, seats)], row_in_sem.at[layer]),
                pltpu.make_async_copy(prev[layer], row_stage.at[layer, pl.ds(seats, seats)], row_in_sem.at[layer]))

    def fill(j):
        dst = pl.ds(owner[1, j], STEPS)
        return [pltpu.make_async_copy(row_stage.at[layer, owner[0, j], which], out.at[j, layer, dst], row_sem.at[0]) for layer in range(layers) for which, out in enumerate((k_out, v_out))]

    for_all(entries, mig, 1, fetch, start)
    for layer in range(layers):
        for copy in load(layer):
            copy.start()
    zeros[...] = jnp.zeros_like(zeros)

    def relay(e, carry):
        @pl.when(mig[1, e] >= 0)
        def _():
            for copy in fetch(e):
                copy.wait()
            for copy in put(e):
                copy.start()

        return carry

    lax.fori_loop(0, entries, relay, 0)
    for_all(entries, mig, 0, clear, start)
    for_all(entries, mig, 1, put, wait)
    for layer in range(layers):
        for copy in load(layer):
            copy.wait()
    for_all(slots, owner, 0, fill, start)

    def from_far(j, carry):
        @pl.when(owner[2, j] >= 0)
        def _():
            dst = pl.ds(owner[1, j], STEPS)
            for layer in range(layers):
                copy = pltpu.make_async_copy(far[layer].at[owner[2, j]], far_stage, far_sem.at[0])
                copy.start()
                copy.wait()
                for which, out in enumerate((k_out, v_out)):
                    copy = pltpu.make_async_copy(far_stage.at[which], out.at[j, layer, dst], far_sem.at[0])
                    copy.start()
                    copy.wait()

        return carry

    lax.fori_loop(0, slots, from_far, 0)
    for_all(entries, mig, 0, clear, wait)
    for_all(slots, owner, 0, fill, wait)


def finish_pools(k_pool, v_pool, moved, own, prev, far, mig, owner):
    slots, layers = k_pool.shape[:2]
    entries = mig.shape[1]
    pool = jax.ShapeDtypeStruct(k_pool.shape, k_pool.dtype)
    row_shape = own[0].shape
    return pl.pallas_call(
        functools.partial(finish_kernel, layers, slots, entries),
        out_shape=[pool, pool],
        in_specs=[smem_spec(), smem_spec()] + [any_spec()] * (2 + 4 * layers),
        out_specs=[any_spec(), any_spec()],
        input_output_aliases={2: 0, 3: 1},
        scratch_shapes=[
            pltpu.VMEM(k_pool.shape[1:], k_pool.dtype),
            pltpu.VMEM((entries, layers, 2) + k_pool.shape[2:], k_pool.dtype),
            pltpu.VMEM((layers, 2 * row_shape[0]) + row_shape[1:], k_pool.dtype),
            pltpu.VMEM(row_shape[1:], k_pool.dtype),
            pltpu.SemaphoreType.DMA((1,)),
            pltpu.SemaphoreType.DMA((entries,)),
            pltpu.SemaphoreType.DMA((1,)),
            pltpu.SemaphoreType.DMA((layers,)),
            pltpu.SemaphoreType.DMA((1,)),
            pltpu.SemaphoreType.DMA((1,)),
        ],
        cost_estimate=pl.CostEstimate(flops=10 ** 10, bytes_accessed=10 ** 7, transcendentals=0),
        name='finish_pools',
    )(mig, owner, k_pool, v_pool, *moved, *own, *prev, *far)


def dense(hidden, weight):
    return jnp.dot(hidden, weight, preferred_element_type=jnp.float32)


def pair_mlp(hidden, w_up, w_down, layer, core, pairs):
    rows = hidden.shape[0]
    width, full = w_up.shape[1:]
    half = full // 2
    both = jnp.concatenate([hidden, lax.ppermute(hidden, 'kv', pairs)])
    up_proj = dense(both, lax.dynamic_slice(w_up, (layer, 0, core * half), (1, width, half))[0]).astype(jnp.bfloat16)
    act = jax.nn.gelu(up_proj.astype(jnp.float32), approximate=True).astype(jnp.bfloat16)
    outs = []
    for first in range(0, width, width // 2):
        part = dense(act, lax.dynamic_slice(w_down, (layer, core * half, first), (1, half, width // 2))[0])
        rest = lax.ppermute(part[rows:], 'kv', pairs)
        outs.append((hidden[:, first:first + width // 2].astype(jnp.float32) + (part[:rows] + rest)).astype(jnp.bfloat16))
    return jnp.concatenate(outs, axis=1)


def shift_by(count, distance):
    return [(i, (i + distance) % count) for i in range(count)]


ROUND_PAGES = 8


def other_pages(k_pool, v_pool, buffer, src, slot, dst, target, wanted, me, group_size):
    entry_ids = jnp.arange(src.shape[0])
    rank = masked_pick((src[None, :] == src[:, None]) & wanted[None, :] & (entry_ids[None, :] < entry_ids[:, None]), 1)
    most = jnp.max(jnp.where(wanted, rank + 1, 0))
    seat = jnp.where(wanted, src * src.shape[0] + rank, -1)

    def body(carry):
        done, buf = carry
        seats = ((jnp.arange(group_size) * src.shape[0])[:, None] + done + jnp.arange(ROUND_PAGES)[None, :]).reshape(-1)
        hit = seat[None, :] == seats[:, None]
        seat_slot = masked_pick(hit, slot[None, :])
        seat_target = jnp.where(jnp.any(hit & (dst == me)[None, :], axis=1), masked_pick(hit, target[None, :]), buf.shape[0])
        my_slots = lax.dynamic_slice_in_dim(seat_slot, me * ROUND_PAGES, ROUND_PAGES)
        pages = jnp.stack([jnp.take(k_pool, my_slots, axis=0), jnp.take(v_pool, my_slots, axis=0)], axis=1)
        gathered = lax.all_gather(pages, 'kv', axis=0, tiled=True)
        return done + ROUND_PAGES, buf.at[seat_target].set(gathered, mode='drop')

    return lax.while_loop(lambda carry: carry[0] < most, body, (jnp.zeros((), I32), buffer))[1]


def solution(mesh):
    group_size = mesh.shape['kv']
    pool_spec = P(('rep', 'kv'))
    tok_spec = P(None, ('rep', 'kv'), None)

    def device_fn(embeds, w_query, w_key, w_value, w_out, w_up, w_down, k_pool, v_pool, new_table, seq_lens, mig_src, mig_dst):
        me = lax.axis_index('kv')
        slots, layers, page_len, kv_heads, head_dim = k_pool.shape
        per_dev, width = embeds.shape[1:]
        seq_count, page_count = new_table.shape
        num_heads = w_query.shape[2] // head_dim
        pairs = [(i, i ^ 1) for i in range(group_size)]

        remap = new_table[:, :, None] == mig_dst
        is_moved = jnp.any(remap, axis=-1)
        old_table = jnp.where(is_moved, masked_pick(remap, mig_src), new_table)
        page_src = old_table // slots
        page_slot = old_table % slots

        page_ids = jnp.arange(page_count, dtype=I32)[None, :]
        page_rows = jnp.where(page_ids == 0, page_len, seq_lens[:, None] - page_len)

        src_dev, dst_dev = mig_src // slots, mig_dst // slots
        clear_slot = jnp.where(src_dev == me, mig_src % slots, -1)
        fill_slot = jnp.where(dst_dev == me, mig_dst % slots, -1)
        mig_meta = jnp.stack([clear_slot, fill_slot]).astype(I32)
        moved_cap = mig_src.shape[0] * MOVED_ROWS
        moved_rows = jnp.sum(jnp.where(remap, page_rows[:, :, None], 0), axis=(0, 1))
        moved_first = excl_cumsum(moved_rows)
        moved_fits = moved_first + moved_rows <= moved_cap
        moved_meta = jnp.stack([jnp.where(moved_fits, clear_slot, -1), moved_first, moved_rows])
        moved_out = pack_rows((0,), k_pool, v_pool, moved_meta, moved_cap)[0]
        moved_out, new_table, page_src, page_slot = lax.optimization_barrier((moved_out, new_table, page_src, page_slot))
        moved = [lax.psum(moved_out, 'kv')]

        dev, pos = place_sequences(page_src[:, 0], group_size, per_dev)
        place = dev * per_dev + pos

        is_local = page_src == dev[:, None]
        in_moved = jnp.any(remap & moved_fits, axis=-1) & ~is_local
        same_dev_earlier = (dev[None, :] == dev[:, None]) & (pos[None, :] < pos[:, None])
        near_cap = per_dev * NEAR_ROWS
        by_next = (page_src[:, 1] == (dev + 1) % group_size) & ~is_moved[:, 1]
        near_first = masked_pick(same_dev_earlier & by_next[None, :], page_rows[None, :, 1])
        by_next = by_next & (near_first + page_rows[:, 1] <= near_cap)
        is_near = (page_ids == 1) & by_next[:, None]

        prev = (me + group_size - 1) % group_size
        prev_seat = prev * per_dev + jnp.arange(per_dev, dtype=I32)
        from_here = (place[None, :] == prev_seat[:, None]) & by_next[None, :]
        near_facts = jnp.stack([page_slot[:, 1] + 1, near_first, page_rows[:, 1]])
        near_meta = masked_pick(from_here[None, :, :], near_facts[:, None, :]) - jnp.array([[1], [0], [0]])
        other_shape = (per_dev * page_count, 2) + k_pool.shape[1:]
        far_shape = (seq_count, 2, STEPS, kv_heads, head_dim)
        my_dev = lax.dynamic_slice_in_dim(dev, me * per_dev, per_dev)
        my_pos = lax.dynamic_slice_in_dim(pos, me * per_dev, per_dev)
        home = jnp.arange(seq_count, dtype=I32) // per_dev
        distance = (dev - home) % group_size
        my_distance = (my_dev - me) % group_size
        at_pos = my_pos[None, :] == jnp.arange(per_dev, dtype=I32)[:, None]
        counts = jnp.sum(distance[None, :] == jnp.arange(group_size, dtype=I32)[:, None], axis=1)
        most = jnp.argmax(counts).astype(I32)
        all_same = counts[most] == seq_count

        def send_embeds(step_away):
            sel = (at_pos & (my_distance == step_away)[None, :]).astype(embeds.dtype)
            rows = jnp.einsum('pb,tbd->ptd', sel, embeds, preferred_element_type=jnp.float32).astype(embeds.dtype)
            return lax.ppermute(rows, 'kv', shift_by(group_size, step_away)) if step_away else rows

        def send_most(step_away, near_meta, clear_slot):
            rows = send_embeds(step_away)
            packed = pack_rows(tuple(range(layers)), k_pool, v_pool, near_meta, near_cap, [other_shape, far_shape, far_shape])
            return rows, packed, copy_pools(k_pool, v_pool), pack_pages(tuple(range(layers)), k_pool, v_pool, clear_slot)

        def send_rest(hidden):
            for step_away in range(group_size):
                hidden = lax.cond((counts[step_away] > 0) & (most != step_away), lambda rows, step_away=step_away: rows + send_embeds(step_away), lambda rows: rows, hidden)
            return hidden

        hidden, packed, (k_base, v_base), full_out = lax.switch(most, [functools.partial(send_most, step_away) for step_away in range(group_size)], gate(near_meta.astype(I32)), clear_slot)
        *near_out, other, far_0, far_1 = packed
        full_out = list(full_out)
        hidden = lax.cond(all_same, lambda rows: rows, send_rest, hidden)
        hidden = hidden.reshape(per_dev * STEPS, width)
        near = [lax.ppermute(near_out[0], 'kv', shift_by(group_size, -1))]

        wanted = ~(is_local | in_moved | is_near)
        kind = jnp.where(is_local, LOCAL, jnp.where(in_moved, MOVED, jnp.where(is_near, NEXT, OTHER)))
        target = pos[:, None] * page_count + page_ids
        entry_dst = jnp.broadcast_to(dev[:, None], page_src.shape)

        def fetch_other(buffer):
            return other_pages(k_pool, v_pool, buffer, page_src.reshape(-1), page_slot.reshape(-1), entry_dst.reshape(-1), target.reshape(-1), wanted.reshape(-1), me, group_size)

        other, moved[0] = lax.optimization_barrier((other, moved[0]))
        other = lax.cond(jnp.any(wanted), fetch_other, lambda buffer: buffer, other)
        mine = place[None, :] == (me * per_dev + jnp.arange(per_dev, dtype=I32))[:, None]
        facts = []
        for layer in range(layers):
            moved_at = masked_pick(remap, moved_first) if layer == 0 else masked_pick(remap, jnp.arange(mig_src.shape[0], dtype=I32)) * page_len
            index = jnp.where(is_local, page_slot, jnp.where(in_moved, moved_at, jnp.where(is_near, near_first[:, None], target)))
            facts.append(jnp.stack([kind[:, 0], index[:, 0], kind[:, 1], index[:, 1], seq_lens]))
        attend_meta = masked_pick(mine[None, None, :, :], jnp.stack(facts)[:, :, None, :]).astype(I32)

        row_dst = new_table[:, 1] // slots
        is_far = (row_dst != dev) & (row_dst != (dev + 1) % group_size)
        writes = new_table[None, :, 1] == (me * slots + jnp.arange(slots, dtype=I32))[:, None]
        owner_facts = jnp.stack([jnp.where(is_far, 0, 1 + pos + jnp.where(row_dst == dev, 0, per_dev)), seq_lens - page_len, jnp.where(is_far, 1 + place, 0)])
        owner_meta = (masked_pick(writes[None, :, :], owner_facts[:, None, :]) - jnp.array([[1], [0], [1]])).astype(I32)

        own_rows, prev_rows = [], []
        for layer in range(layers):
            queries = dense(hidden, w_query[layer]).astype(jnp.bfloat16)
            new_keys = dense(hidden, w_key[layer]).astype(jnp.bfloat16)
            new_vals = dense(hidden, w_value[layer]).astype(jnp.bfloat16)
            rows = jnp.stack([new_keys, new_vals]).reshape(2, per_dev, STEPS, kv_heads, head_dim).transpose(1, 0, 2, 3, 4)
            own_rows.append(rows)
            prev_rows.append(lax.ppermute(rows, 'kv', shift_by(group_size, 1)))
            q_rows = queries.reshape(per_dev, STEPS, num_heads, head_dim)
            if layer == 0:
                for after in range(layers - 1, -1, -1):
                    full_out[after], moved[-1] = lax.optimization_barrier((full_out[after], moved[-1]))
                    moved.append(lax.psum(full_out[after], 'kv'))
                moved = [moved[0]] + moved[:0:-1]
            if layer + 1 < layers:
                near_next, near[layer] = lax.optimization_barrier((near_out[layer + 1], near[layer]))
                near.append(lax.ppermute(near_next, 'kv', shift_by(group_size, -1)))
            attn = attend(layer, q_rows, rows, k_pool, v_pool, moved[layer if layer == 0 else layer + 1], near[layer], other, attend_meta[layer]).reshape(per_dev * STEPS, num_heads * head_dim)
            hidden = (hidden.astype(jnp.float32) + dense(attn, w_out[layer])).astype(jnp.bfloat16)
            hidden = pair_mlp(hidden, w_up, w_down, layer, me % 2, pairs)

        hidden, moved[1], *far_in = lax.optimization_barrier((hidden, moved[1], *own_rows))
        far_rows = lax.cond(jnp.any(is_far), lambda own, far: [lax.all_gather(rows, 'kv', axis=0, tiled=True) for rows in own], lambda own, far: far, far_in, [far_0, far_1])
        hidden = hidden.reshape(per_dev, STEPS, width)

        def bring_home(step_away, total):
            rows = lax.ppermute(hidden, 'kv', shift_by(group_size, -step_away)) if step_away else hidden
            sel = (at_pos & (my_distance == step_away)[None, :]).astype(hidden.dtype)
            return total + jnp.einsum('pb,ptd->tbd', sel, rows, preferred_element_type=jnp.float32).astype(hidden.dtype)

        def bring_most(step_away, k_base, v_base):
            rows = lax.ppermute(hidden, 'kv', shift_by(group_size, -step_away)) if step_away else hidden
            k_out, v_out = finish_pools(k_base, v_base, moved[1:], own_rows, prev_rows, far_rows, mig_meta, owner_meta)
            sel = (at_pos & (my_distance == step_away)[None, :]).astype(hidden.dtype)
            return jnp.einsum('pb,ptd->tbd', sel, rows, preferred_element_type=jnp.float32).astype(hidden.dtype), k_out, v_out

        y_out, k_out, v_out = lax.switch(most, [functools.partial(bring_most, step_away) for step_away in range(group_size)], k_base, v_base)

        def bring_rest(y_out):
            for step_away in range(group_size):
                y_out = lax.cond((counts[step_away] > 0) & (most != step_away), functools.partial(bring_home, step_away), lambda same: same, y_out)
            return y_out

        y_out = lax.cond(all_same, lambda same: same, bring_rest, y_out)
        return y_out, k_out, v_out

    return jax.shard_map(device_fn, mesh=mesh, in_specs=(tok_spec, P(), P(), P(), P(), P(), P(), pool_spec, pool_spec, P('rep', None), P('rep'), P('rep'), P('rep')), out_specs=(tok_spec, pool_spec, pool_spec), check_vma=False)
```

```python
import functools

import jax
import jax.numpy as jnp
from jax import lax
from jax.experimental import pallas as pl
from jax.experimental.pallas import tpu as pltpu
from jax.sharding import PartitionSpec as P


STEPS = 2
I32 = jnp.int32


def excl_cumsum(values):
    n = values.shape[0]
    before = jnp.arange(n)[None, :] < jnp.arange(n)[:, None]
    return jnp.sum(jnp.where(before, values[None, :], 0), axis=1)


def masked_pick(mask, values):
    return jnp.sum(jnp.where(mask, values, 0), axis=-1)


def place_sequences(pref, group_size, per_dev):
    count = pref.shape[0]
    ids = jnp.arange(count)
    earlier = ids[None, :] < ids[:, None]
    rank = jnp.sum((pref[None, :] == pref[:, None]) & earlier, axis=1)
    wanted = jnp.sum(pref[None, :] == jnp.arange(group_size)[:, None], axis=1)
    free = jnp.maximum(per_dev - wanted, 0)
    free_end = excl_cumsum(free) + free
    over = rank >= per_dev
    over_rank = jnp.sum(over[None, :] & earlier, axis=1)
    spill = jnp.sum(over_rank[:, None] >= free_end[None, :], axis=1)
    dev = jnp.where(over, spill, pref)
    pos = jnp.sum((dev[None, :] == dev[:, None]) & earlier, axis=1)
    return dev.astype(I32), pos.astype(I32)


def any_spec():
    return pl.BlockSpec(memory_space=pl.ANY)


def smem_spec():
    return pl.BlockSpec(memory_space=pltpu.SMEM)


def vmem_spec():
    return pl.BlockSpec(memory_space=pltpu.VMEM)


def start(copy):
    copy.start()


def wait(copy):
    copy.wait()


def for_all(count, table, row, make, act):
    def body(e, carry):
        @pl.when(table[row, e] >= 0)
        def _():
            for copy in make(e):
                act(copy)

        return carry

    lax.fori_loop(0, count, body, 0)


def page_copies(layer, k_pool, v_pool, slot, k_dst, v_dst, sem):
    return (pltpu.make_async_copy(k_pool.at[slot, layer], k_dst, sem), pltpu.make_async_copy(v_pool.at[slot, layer], v_dst, sem))


def pack_pages_kernel(layers, meta, k_pool, v_pool, *rest):
    outs = rest[:len(layers)]
    stage, in_sem, out_sem = rest[-3:]
    page_len = k_pool.shape[2]
    count = stage.shape[2] // page_len

    def fetch(at):
        def make(e):
            part = pl.ds(e * page_len, page_len)
            return page_copies(layers[at], k_pool, v_pool, meta[0, e], stage.at[at, 0, part], stage.at[at, 1, part], in_sem.at[at])

        return make

    for at in range(len(layers)):
        for_all(count, meta, 0, fetch(at), start)

    def wipe(e, carry):
        @pl.when(meta[0, e] < 0)
        def _():
            for at in range(len(layers)):
                for which in range(2):
                    stage[at, which, pl.ds(e * page_len, page_len)] = jnp.zeros((page_len,) + stage.shape[3:], stage.dtype)

        return carry

    lax.fori_loop(0, count, wipe, 0)
    for at in range(len(layers)):
        for_all(count, meta, 0, fetch(at), wait)
        pltpu.make_async_copy(stage.at[at], outs[at], out_sem.at[at]).start()
    for at in range(len(layers)):
        pltpu.make_async_copy(stage.at[at], outs[at], out_sem.at[at]).wait()


def pack_pages(layers, k_pool, v_pool, slot_of):
    shape = (2, slot_of.shape[0] * k_pool.shape[2]) + k_pool.shape[3:]
    return pl.pallas_call(
        functools.partial(pack_pages_kernel, layers),
        out_shape=[jax.ShapeDtypeStruct(shape, k_pool.dtype)] * len(layers),
        in_specs=[smem_spec(), any_spec(), any_spec()],
        out_specs=[any_spec()] * len(layers),
        scratch_shapes=[pltpu.VMEM((len(layers),) + shape, k_pool.dtype), pltpu.SemaphoreType.DMA((len(layers),)), pltpu.SemaphoreType.DMA((len(layers),))],
        cost_estimate=pl.CostEstimate(flops=10 ** 10, bytes_accessed=10 ** 7, transcendentals=0),
    )(slot_of[None, :].astype(I32), k_pool, v_pool)


def pack_rows_kernel(layers, meta, k_pool, v_pool, *rest):
    outs = rest[:len(layers)]
    pages, stage, in_sem, out_sem = rest[-4:]
    count = pages.shape[1]
    page_len = k_pool.shape[2]

    def fetch(at):
        return lambda e: page_copies(layers[at], k_pool, v_pool, meta[0, e], pages.at[at, e, 0], pages.at[at, e, 1], in_sem.at[at])

    for at in range(len(layers)):
        for_all(count, meta, 0, fetch(at), start)
    nothing = jnp.zeros((page_len,) + stage.shape[3:], stage.dtype)

    def wipe(i, carry):
        for at in range(len(layers)):
            for which in range(2):
                stage[at, which, pl.ds(i * page_len, page_len)] = nothing
        return carry

    lax.fori_loop(0, stage.shape[2] // page_len, wipe, 0)
    for at in range(len(layers)):
        for_all(count, meta, 0, fetch(at), wait)

        def place(e, carry):
            @pl.when(meta[0, e] >= 0)
            def _():
                for which in range(2):
                    stage[at, which, pl.ds(meta[1, e], page_len)] = pages[at, e, which]
                    stage[at, which, pl.ds(meta[1, e] + meta[2, e], page_len)] = nothing

            return carry

        lax.fori_loop(0, count, place, 0)
        pltpu.make_async_copy(stage.at[at], outs[at], out_sem.at[at]).start()
    for at in range(len(layers)):
        pltpu.make_async_copy(stage.at[at], outs[at], out_sem.at[at]).wait()


def pack_rows(layers, k_pool, v_pool, meta, cap, spare=()):
    count = meta.shape[1]
    page_len = k_pool.shape[2]
    shape = (2, cap + 2 * page_len) + k_pool.shape[3:]
    outs = [jax.ShapeDtypeStruct(shape, k_pool.dtype)] * len(layers) + [jax.ShapeDtypeStruct(s, k_pool.dtype) for s in spare]
    return pl.pallas_call(
        functools.partial(pack_rows_kernel, layers),
        out_shape=outs,
        in_specs=[smem_spec(), any_spec(), any_spec()],
        out_specs=[any_spec()] * len(outs),
        scratch_shapes=[
            pltpu.VMEM((len(layers), count, 2) + k_pool.shape[2:], k_pool.dtype),
            pltpu.VMEM((len(layers),) + shape, k_pool.dtype),
            pltpu.SemaphoreType.DMA((len(layers),)),
            pltpu.SemaphoreType.DMA((len(layers),)),
        ],
        cost_estimate=pl.CostEstimate(flops=10 ** 10, bytes_accessed=10 ** 7, transcendentals=0),
    )(meta.astype(I32), k_pool, v_pool)


def gate(value):
    def kernel(src, dst):
        dst[...] = src[...]

    return pl.pallas_call(kernel, out_shape=jax.ShapeDtypeStruct(value.shape, value.dtype), name='gate')(value)


LOCAL, MOVED, NEXT, OTHER = range(4)
MOVED_ROWS = 10
NEAR_ROWS = 9


def attend_kernel(layer, seqs, page_len, q_per_kv, unroll, meta, q_ref, new_ref, k_pool, v_pool, moved, near, other, out_ref, k_buf, v_buf, k_sem, v_sem):
    kv_heads, head_dim = k_buf.shape[2:]

    def launch(j, carry):
        for page in range(2):
            kind = meta[2 * page, j]
            index = meta[2 * page + 1, j]

            def both(k_src, v_src):
                dst = pl.ds(page * page_len, page_len)
                pltpu.make_async_copy(k_src, k_buf.at[j, dst], k_sem.at[j]).start()
                pltpu.make_async_copy(v_src, v_buf.at[j, dst], v_sem.at[j]).start()

            @pl.when(kind == LOCAL)
            def _():
                both(k_pool.at[index, layer], v_pool.at[index, layer])

            @pl.when(kind > LOCAL)
            def _():
                part = pl.ds(index, page_len)

                @pl.when(kind == MOVED)
                def _():
                    both(moved.at[0, part], moved.at[1, part])

                @pl.when(kind == NEXT)
                def _():
                    both(near.at[0, part], near.at[1, part])

                @pl.when(kind == OTHER)
                def _():
                    both(other.at[index, 0, layer], other.at[index, 1, layer])
        return carry

    lax.fori_loop(0, seqs, launch, 0)

    rows = STEPS * kv_heads * q_per_kv
    cols = 2 * page_len * kv_heads
    row_id = lax.broadcasted_iota(I32, (rows, cols), 0)
    col_id = lax.broadcasted_iota(I32, (rows, cols), 1)
    row_step = row_id // (kv_heads * q_per_kv)
    own_head = (col_id % kv_heads) == (row_id % (kv_heads * q_per_kv)) // q_per_kv
    lag = jnp.where(own_head, col_id // kv_heads - row_step, 1 << 20)

    def body(i, carry):
        for u in range(unroll):
            j = i * unroll + u
            pltpu.make_async_copy(k_buf.at[j], k_buf.at[j], k_sem.at[j]).wait()
            pltpu.make_async_copy(v_buf.at[j], v_buf.at[j], v_sem.at[j]).wait()
        for u in range(unroll):
            j = i * unroll + u
            length = meta[4, j]
            for step in range(STEPS):
                k_buf[j, length + step] = new_ref[j, 0, step]
                v_buf[j, length + step] = new_ref[j, 1, step]
        ids = [i * unroll + u for u in range(unroll)]
        queries = [jnp.concatenate([q_ref[step, j] for step in range(STEPS)]) for j in ids]
        scores = [lax.dot_general(query, k_buf[j].reshape(cols, head_dim), (((1,), (1,)), ((), ())), preferred_element_type=jnp.float32) for j, query in zip(ids, queries)]
        scores = [jnp.where(lag <= meta[4, j], score * head_dim ** -0.5, -jnp.inf) for j, score in zip(ids, scores)]
        probs = [jnp.exp(score - jnp.max(score, axis=1, keepdims=True)) for score in scores]
        totals = [jnp.sum(prob, axis=1, keepdims=True) for prob in probs]
        outs = [jnp.dot(prob.astype(v_buf.dtype), v_buf[j].reshape(cols, head_dim), preferred_element_type=jnp.float32) / total for j, prob, total in zip(ids, probs, totals)]
        for j, out in zip(ids, outs):
            for step in range(STEPS):
                out_ref[step, j] = out[step * (rows // STEPS):(step + 1) * (rows // STEPS)].astype(out_ref.dtype)
        return carry

    lax.fori_loop(0, seqs // unroll, body, 0)


def attend(layer, queries, new_rows, k_pool, v_pool, moved, near, other, meta):
    seqs = queries.shape[1]
    page_len, kv_heads, head_dim = k_pool.shape[2:]
    num_heads = queries.shape[2]
    buf = pltpu.VMEM((seqs, 2 * page_len, kv_heads, head_dim), k_pool.dtype)
    return pl.pallas_call(
        functools.partial(attend_kernel, layer, seqs, page_len, num_heads // kv_heads, 8),
        out_shape=jax.ShapeDtypeStruct(queries.shape, queries.dtype),
        in_specs=[smem_spec(), vmem_spec(), vmem_spec()] + [any_spec()] * 5,
        out_specs=vmem_spec(),
        scratch_shapes=[buf, buf, pltpu.SemaphoreType.DMA((seqs,)), pltpu.SemaphoreType.DMA((seqs,))],
        cost_estimate=pl.CostEstimate(flops=10 ** 10, bytes_accessed=10 ** 7, transcendentals=10 ** 6),
    )(meta, queries, new_rows, k_pool, v_pool, moved, near, other)


COPY_SLOTS = 16


def copy_kernel(k_pool, v_pool, k_out, v_out, stage, in_sem, out_sem):
    chunks = k_pool.shape[0] // COPY_SLOTS
    for pool, which in ((k_pool, 0), (v_pool, 1)):
        for c in range(chunks):
            part = pl.ds(c * COPY_SLOTS, COPY_SLOTS)
            pltpu.make_async_copy(pool.at[part], stage.at[which, part], in_sem.at[which, c]).start()
    for pool, out, which in ((k_pool, k_out, 0), (v_pool, v_out, 1)):
        for c in range(chunks):
            part = pl.ds(c * COPY_SLOTS, COPY_SLOTS)
            pltpu.make_async_copy(pool.at[part], stage.at[which, part], in_sem.at[which, c]).wait()
            pltpu.make_async_copy(stage.at[which, part], out.at[part], out_sem.at[which, c]).start()
    for out, which in ((k_out, 0), (v_out, 1)):
        for c in range(chunks):
            part = pl.ds(c * COPY_SLOTS, COPY_SLOTS)
            pltpu.make_async_copy(stage.at[which, part], out.at[part], out_sem.at[which, c]).wait()


def copy_pools(k_pool, v_pool):
    chunks = k_pool.shape[0] // COPY_SLOTS
    pool = jax.ShapeDtypeStruct(k_pool.shape, k_pool.dtype)
    return pl.pallas_call(
        copy_kernel,
        out_shape=[pool, pool],
        in_specs=[any_spec(), any_spec()],
        out_specs=[any_spec(), any_spec()],
        scratch_shapes=[pltpu.VMEM((2,) + k_pool.shape, k_pool.dtype), pltpu.SemaphoreType.DMA((2, chunks)), pltpu.SemaphoreType.DMA((2, chunks))],
        cost_estimate=pl.CostEstimate(flops=10 ** 10, bytes_accessed=10 ** 7, transcendentals=0),
        name='copy_pools',
    )(k_pool, v_pool)


def finish_kernel(layers, slots, entries, mig, owner, k_in, v_in, *rest):
    del k_in, v_in
    moved, own, prev, far = (rest[i * layers:(i + 1) * layers] for i in range(4))
    k_out, v_out, zeros, stage, row_stage, far_stage, zero_sem, in_sem, out_sem, row_in_sem, row_sem, far_sem = rest[4 * layers:]
    page_len = k_out.shape[2]
    seats = own[0].shape[0]

    def fetch(e):
        part = pl.ds(e * page_len, page_len)
        return [pltpu.make_async_copy(moved[layer].at[which, part], stage.at[e, layer, which], in_sem.at[e]) for layer in range(layers) for which in range(2)]

    def put(e):
        return [pltpu.make_async_copy(stage.at[e, layer, which], out.at[mig[1, e], layer], out_sem.at[0]) for layer in range(layers) for which, out in enumerate((k_out, v_out))]

    def clear(e):
        return [pltpu.make_async_copy(zeros, out.at[mig[0, e]], zero_sem.at[0]) for out in (k_out, v_out)]

    def load(layer):
        return (pltpu.make_async_copy(own[layer], row_stage.at[layer, pl.ds(0, seats)], row_in_sem.at[layer]),
                pltpu.make_async_copy(prev[layer], row_stage.at[layer, pl.ds(seats, seats)], row_in_sem.at[layer]))

    def fill(j):
        dst = pl.ds(owner[1, j], STEPS)
        return [pltpu.make_async_copy(row_stage.at[layer, owner[0, j], which], out.at[j, layer, dst], row_sem.at[0]) for layer in range(layers) for which, out in enumerate((k_out, v_out))]

    for_all(entries, mig, 1, fetch, start)
    for layer in range(layers):
        for copy in load(layer):
            copy.start()
    zeros[...] = jnp.zeros_like(zeros)

    def relay(e, carry):
        @pl.when(mig[1, e] >= 0)
        def _():
            for copy in fetch(e):
                copy.wait()
            for copy in put(e):
                copy.start()

        return carry

    lax.fori_loop(0, entries, relay, 0)
    for_all(entries, mig, 0, clear, start)
    for_all(entries, mig, 1, put, wait)
    for layer in range(layers):
        for copy in load(layer):
            copy.wait()
    for_all(slots, owner, 0, fill, start)

    def from_far(j, carry):
        @pl.when(owner[2, j] >= 0)
        def _():
            dst = pl.ds(owner[1, j], STEPS)
            for layer in range(layers):
                copy = pltpu.make_async_copy(far[layer].at[owner[2, j]], far_stage, far_sem.at[0])
                copy.start()
                copy.wait()
                for which, out in enumerate((k_out, v_out)):
                    copy = pltpu.make_async_copy(far_stage.at[which], out.at[j, layer, dst], far_sem.at[0])
                    copy.start()
                    copy.wait()

        return carry

    lax.fori_loop(0, slots, from_far, 0)
    for_all(entries, mig, 0, clear, wait)
    for_all(slots, owner, 0, fill, wait)


def finish_pools(k_pool, v_pool, moved, own, prev, far, mig, owner):
    slots, layers = k_pool.shape[:2]
    entries = mig.shape[1]
    pool = jax.ShapeDtypeStruct(k_pool.shape, k_pool.dtype)
    row_shape = own[0].shape
    return pl.pallas_call(
        functools.partial(finish_kernel, layers, slots, entries),
        out_shape=[pool, pool],
        in_specs=[smem_spec(), smem_spec()] + [any_spec()] * (2 + 4 * layers),
        out_specs=[any_spec(), any_spec()],
        input_output_aliases={2: 0, 3: 1},
        scratch_shapes=[
            pltpu.VMEM(k_pool.shape[1:], k_pool.dtype),
            pltpu.VMEM((entries, layers, 2) + k_pool.shape[2:], k_pool.dtype),
            pltpu.VMEM((layers, 2 * row_shape[0]) + row_shape[1:], k_pool.dtype),
            pltpu.VMEM(row_shape[1:], k_pool.dtype),
            pltpu.SemaphoreType.DMA((1,)),
            pltpu.SemaphoreType.DMA((entries,)),
            pltpu.SemaphoreType.DMA((1,)),
            pltpu.SemaphoreType.DMA((layers,)),
            pltpu.SemaphoreType.DMA((1,)),
            pltpu.SemaphoreType.DMA((1,)),
        ],
        cost_estimate=pl.CostEstimate(flops=10 ** 10, bytes_accessed=10 ** 7, transcendentals=0),
        name='finish_pools',
    )(mig, owner, k_pool, v_pool, *moved, *own, *prev, *far)


def dense(hidden, weight):
    return jnp.dot(hidden, weight, preferred_element_type=jnp.float32)


def pair_mlp(hidden, w_up, w_down, layer, core, pairs):
    rows = hidden.shape[0]
    width, full = w_up.shape[1:]
    half = full // 2
    both = jnp.concatenate([hidden, lax.ppermute(hidden, 'kv', pairs)])
    up_proj = dense(both, lax.dynamic_slice(w_up, (layer, 0, core * half), (1, width, half))[0]).astype(jnp.bfloat16)
    act = jax.nn.gelu(up_proj.astype(jnp.float32), approximate=True).astype(jnp.bfloat16)
    part = dense(act, lax.dynamic_slice(w_down, (layer, core * half, 0), (1, half, width))[0])
    rest = lax.ppermute(part[rows:], 'kv', pairs)
    return (hidden.astype(jnp.float32) + (part[:rows] + rest)).astype(jnp.bfloat16)


def shift_by(count, distance):
    return [(i, (i + distance) % count) for i in range(count)]


ROUND_PAGES = 8


def other_pages(k_pool, v_pool, buffer, src, slot, dst, target, wanted, me, group_size):
    entry_ids = jnp.arange(src.shape[0])
    rank = masked_pick((src[None, :] == src[:, None]) & wanted[None, :] & (entry_ids[None, :] < entry_ids[:, None]), 1)
    most = jnp.max(jnp.where(wanted, rank + 1, 0))
    seat = jnp.where(wanted, src * src.shape[0] + rank, -1)

    def body(carry):
        done, buf = carry
        seats = ((jnp.arange(group_size) * src.shape[0])[:, None] + done + jnp.arange(ROUND_PAGES)[None, :]).reshape(-1)
        hit = seat[None, :] == seats[:, None]
        seat_slot = masked_pick(hit, slot[None, :])
        seat_target = jnp.where(jnp.any(hit & (dst == me)[None, :], axis=1), masked_pick(hit, target[None, :]), buf.shape[0])
        my_slots = lax.dynamic_slice_in_dim(seat_slot, me * ROUND_PAGES, ROUND_PAGES)
        pages = jnp.stack([jnp.take(k_pool, my_slots, axis=0), jnp.take(v_pool, my_slots, axis=0)], axis=1)
        gathered = lax.all_gather(pages, 'kv', axis=0, tiled=True)
        return done + ROUND_PAGES, buf.at[seat_target].set(gathered, mode='drop')

    return lax.while_loop(lambda carry: carry[0] < most, body, (jnp.zeros((), I32), buffer))[1]


def solution(mesh):
    group_size = mesh.shape['kv']
    pool_spec = P(('rep', 'kv'))
    tok_spec = P(None, ('rep', 'kv'), None)

    def device_fn(embeds, w_query, w_key, w_value, w_out, w_up, w_down, k_pool, v_pool, new_table, seq_lens, mig_src, mig_dst):
        me = lax.axis_index('kv')
        slots, layers, page_len, kv_heads, head_dim = k_pool.shape
        per_dev, width = embeds.shape[1:]
        seq_count, page_count = new_table.shape
        num_heads = w_query.shape[2] // head_dim
        pairs = [(i, i ^ 1) for i in range(group_size)]

        remap = new_table[:, :, None] == mig_dst
        is_moved = jnp.any(remap, axis=-1)
        old_table = jnp.where(is_moved, masked_pick(remap, mig_src), new_table)
        page_src = old_table // slots
        page_slot = old_table % slots

        page_ids = jnp.arange(page_count, dtype=I32)[None, :]
        page_rows = jnp.where(page_ids == 0, page_len, seq_lens[:, None] - page_len)

        src_dev, dst_dev = mig_src // slots, mig_dst // slots
        clear_slot = jnp.where(src_dev == me, mig_src % slots, -1)
        fill_slot = jnp.where(dst_dev == me, mig_dst % slots, -1)
        mig_meta = jnp.stack([clear_slot, fill_slot]).astype(I32)
        moved_cap = mig_src.shape[0] * MOVED_ROWS
        moved_rows = jnp.sum(jnp.where(remap, page_rows[:, :, None], 0), axis=(0, 1))
        moved_first = excl_cumsum(moved_rows)
        moved_fits = moved_first + moved_rows <= moved_cap
        moved_meta = jnp.stack([jnp.where(moved_fits, clear_slot, -1), moved_first, moved_rows])
        moved_out = pack_rows((0,), k_pool, v_pool, moved_meta, moved_cap)[0]
        moved_out, new_table, page_src, page_slot = lax.optimization_barrier((moved_out, new_table, page_src, page_slot))
        moved = [lax.psum(moved_out, 'kv')]

        dev, pos = place_sequences(page_src[:, 0], group_size, per_dev)
        place = dev * per_dev + pos

        is_local = page_src == dev[:, None]
        in_moved = jnp.any(remap & moved_fits, axis=-1) & ~is_local
        same_dev_earlier = (dev[None, :] == dev[:, None]) & (pos[None, :] < pos[:, None])
        near_cap = per_dev * NEAR_ROWS
        by_next = (page_src[:, 1] == (dev + 1) % group_size) & ~is_moved[:, 1]
        near_first = masked_pick(same_dev_earlier & by_next[None, :], page_rows[None, :, 1])
        by_next = by_next & (near_first + page_rows[:, 1] <= near_cap)
        is_near = (page_ids == 1) & by_next[:, None]

        prev = (me + group_size - 1) % group_size
        prev_seat = prev * per_dev + jnp.arange(per_dev, dtype=I32)
        from_here = (place[None, :] == prev_seat[:, None]) & by_next[None, :]
        near_facts = jnp.stack([page_slot[:, 1] + 1, near_first, page_rows[:, 1]])
        near_meta = masked_pick(from_here[None, :, :], near_facts[:, None, :]) - jnp.array([[1], [0], [0]])
        other_shape = (per_dev * page_count, 2) + k_pool.shape[1:]
        far_shape = (seq_count, 2, STEPS, kv_heads, head_dim)
        my_dev = lax.dynamic_slice_in_dim(dev, me * per_dev, per_dev)
        my_pos = lax.dynamic_slice_in_dim(pos, me * per_dev, per_dev)
        home = jnp.arange(seq_count, dtype=I32) // per_dev
        distance = (dev - home) % group_size
        my_distance = (my_dev - me) % group_size
        at_pos = my_pos[None, :] == jnp.arange(per_dev, dtype=I32)[:, None]
        counts = jnp.sum(distance[None, :] == jnp.arange(group_size, dtype=I32)[:, None], axis=1)
        most = jnp.argmax(counts).astype(I32)
        all_same = counts[most] == seq_count

        def send_embeds(step_away):
            sel = (at_pos & (my_distance == step_away)[None, :]).astype(embeds.dtype)
            rows = jnp.einsum('pb,tbd->tpd', sel, embeds, preferred_element_type=jnp.float32).astype(embeds.dtype)
            return lax.ppermute(rows, 'kv', shift_by(group_size, step_away)) if step_away else rows

        def send_most(step_away, near_meta, clear_slot):
            rows = send_embeds(step_away)
            packed = pack_rows(tuple(range(layers)), k_pool, v_pool, near_meta, near_cap, [other_shape, far_shape, far_shape])
            return rows, packed, copy_pools(k_pool, v_pool), pack_pages(tuple(range(layers)), k_pool, v_pool, clear_slot)

        def send_rest(hidden):
            for step_away in range(group_size):
                hidden = lax.cond((counts[step_away] > 0) & (most != step_away), lambda rows, step_away=step_away: rows + send_embeds(step_away), lambda rows: rows, hidden)
            return hidden

        hidden, packed, (k_base, v_base), full_out = lax.switch(most, [functools.partial(send_most, step_away) for step_away in range(group_size)], gate(near_meta.astype(I32)), clear_slot)
        *near_out, other, far_0, far_1 = packed
        full_out = list(full_out)
        hidden = lax.optimization_barrier(lax.cond(all_same, lambda rows: rows, send_rest, hidden))
        hidden = hidden.reshape(STEPS * per_dev, width)
        near = [lax.ppermute(near_out[0], 'kv', shift_by(group_size, -1))]

        wanted = ~(is_local | in_moved | is_near)
        kind = jnp.where(is_local, LOCAL, jnp.where(in_moved, MOVED, jnp.where(is_near, NEXT, OTHER)))
        target = pos[:, None] * page_count + page_ids
        entry_dst = jnp.broadcast_to(dev[:, None], page_src.shape)

        def fetch_other(buffer):
            return other_pages(k_pool, v_pool, buffer, page_src.reshape(-1), page_slot.reshape(-1), entry_dst.reshape(-1), target.reshape(-1), wanted.reshape(-1), me, group_size)

        other, moved[0] = lax.optimization_barrier((other, moved[0]))
        other = lax.cond(jnp.any(wanted), fetch_other, lambda buffer: buffer, other)
        mine = place[None, :] == (me * per_dev + jnp.arange(per_dev, dtype=I32))[:, None]
        facts = []
        for layer in range(layers):
            moved_at = masked_pick(remap, moved_first) if layer == 0 else masked_pick(remap, jnp.arange(mig_src.shape[0], dtype=I32)) * page_len
            index = jnp.where(is_local, page_slot, jnp.where(in_moved, moved_at, jnp.where(is_near, near_first[:, None], target)))
            facts.append(jnp.stack([kind[:, 0], index[:, 0], kind[:, 1], index[:, 1], seq_lens]))
        attend_meta = masked_pick(mine[None, None, :, :], jnp.stack(facts)[:, :, None, :]).astype(I32)

        row_dst = new_table[:, 1] // slots
        is_far = (row_dst != dev) & (row_dst != (dev + 1) % group_size)
        writes = new_table[None, :, 1] == (me * slots + jnp.arange(slots, dtype=I32))[:, None]
        owner_facts = jnp.stack([jnp.where(is_far, 0, 1 + pos + jnp.where(row_dst == dev, 0, per_dev)), seq_lens - page_len, jnp.where(is_far, 1 + place, 0)])
        owner_meta = (masked_pick(writes[None, :, :], owner_facts[:, None, :]) - jnp.array([[1], [0], [1]])).astype(I32)

        own_rows, prev_rows = [], []
        for layer in range(layers):
            queries = dense(hidden, w_query[layer]).astype(jnp.bfloat16)
            new_keys = dense(hidden, w_key[layer]).astype(jnp.bfloat16)
            new_vals = dense(hidden, w_value[layer]).astype(jnp.bfloat16)
            rows = jnp.stack([new_keys, new_vals]).reshape(2, STEPS, per_dev, kv_heads, head_dim).transpose(2, 0, 1, 3, 4)
            own_rows.append(rows)
            prev_rows.append(lax.ppermute(rows, 'kv', shift_by(group_size, 1)))
            q_rows = queries.reshape(STEPS, per_dev, num_heads, head_dim)
            if layer == 0:
                for after in range(layers - 1, -1, -1):
                    full_out[after], moved[-1] = lax.optimization_barrier((full_out[after], moved[-1]))
                    moved.append(lax.psum(full_out[after], 'kv'))
                moved = [moved[0]] + moved[:0:-1]
            if layer + 1 < layers:
                near_next, near[layer] = lax.optimization_barrier((near_out[layer + 1], near[layer]))
                near.append(lax.ppermute(near_next, 'kv', shift_by(group_size, -1)))
            attn = attend(layer, q_rows, rows, k_pool, v_pool, moved[layer if layer == 0 else layer + 1], near[layer], other, attend_meta[layer]).reshape(STEPS * per_dev, num_heads * head_dim)
            hidden = (hidden.astype(jnp.float32) + dense(attn, w_out[layer])).astype(jnp.bfloat16)
            hidden = pair_mlp(hidden, w_up, w_down, layer, me % 2, pairs)

        hidden, moved[1], *far_in = lax.optimization_barrier((hidden, moved[1], *own_rows))
        far_rows = lax.cond(jnp.any(is_far), lambda own, far: [lax.all_gather(rows, 'kv', axis=0, tiled=True) for rows in own], lambda own, far: far, far_in, [far_0, far_1])
        hidden = lax.optimization_barrier(hidden).reshape(STEPS, per_dev, width)

        def bring_home(step_away, total):
            rows = lax.ppermute(hidden, 'kv', shift_by(group_size, -step_away)) if step_away else hidden
            sel = (at_pos & (my_distance == step_away)[None, :]).astype(hidden.dtype)
            return total + jnp.einsum('pb,tpd->tbd', sel, rows, preferred_element_type=jnp.float32).astype(hidden.dtype)

        def bring_most(step_away, k_base, v_base):
            rows = lax.ppermute(hidden, 'kv', shift_by(group_size, -step_away)) if step_away else hidden
            k_out, v_out = finish_pools(k_base, v_base, moved[1:], own_rows, prev_rows, far_rows, mig_meta, owner_meta)
            sel = (at_pos & (my_distance == step_away)[None, :]).astype(hidden.dtype)
            return jnp.einsum('pb,tpd->tbd', sel, rows, preferred_element_type=jnp.float32).astype(hidden.dtype), k_out, v_out

        y_out, k_out, v_out = lax.switch(most, [functools.partial(bring_most, step_away) for step_away in range(group_size)], k_base, v_base)

        def bring_rest(y_out):
            for step_away in range(group_size):
                y_out = lax.cond((counts[step_away] > 0) & (most != step_away), functools.partial(bring_home, step_away), lambda same: same, y_out)
            return y_out

        y_out = lax.cond(all_same, lambda same: same, bring_rest, y_out)
        return y_out, k_out, v_out

    return jax.shard_map(device_fn, mesh=mesh, in_specs=(tok_spec, P(), P(), P(), P(), P(), P(), pool_spec, pool_spec, P('rep', None), P('rep'), P('rep'), P('rep')), out_specs=(tok_spec, pool_spec, pool_spec), check_vma=False)
```

```python
import functools

import jax
import jax.numpy as jnp
from jax import lax
from jax.experimental import pallas as pl
from jax.experimental.pallas import tpu as pltpu
from jax.sharding import PartitionSpec as P


STEPS = 2
I32 = jnp.int32


def excl_cumsum(values):
    n = values.shape[0]
    before = jnp.arange(n)[None, :] < jnp.arange(n)[:, None]
    return jnp.sum(jnp.where(before, values[None, :], 0), axis=1)


def masked_pick(mask, values):
    return jnp.sum(jnp.where(mask, values, 0), axis=-1)


def place_sequences(pref, group_size, per_dev):
    count = pref.shape[0]
    ids = jnp.arange(count)
    earlier = ids[None, :] < ids[:, None]
    rank = jnp.sum((pref[None, :] == pref[:, None]) & earlier, axis=1)
    wanted = jnp.sum(pref[None, :] == jnp.arange(group_size)[:, None], axis=1)
    free = jnp.maximum(per_dev - wanted, 0)
    free_end = excl_cumsum(free) + free
    over = rank >= per_dev
    over_rank = jnp.sum(over[None, :] & earlier, axis=1)
    spill = jnp.sum(over_rank[:, None] >= free_end[None, :], axis=1)
    dev = jnp.where(over, spill, pref)
    pos = jnp.sum((dev[None, :] == dev[:, None]) & earlier, axis=1)
    return dev.astype(I32), pos.astype(I32)


def any_spec():
    return pl.BlockSpec(memory_space=pl.ANY)


def smem_spec():
    return pl.BlockSpec(memory_space=pltpu.SMEM)


def vmem_spec():
    return pl.BlockSpec(memory_space=pltpu.VMEM)


def start(copy):
    copy.start()


def wait(copy):
    copy.wait()


def for_all(count, table, row, make, act):
    def body(e, carry):
        @pl.when(table[row, e] >= 0)
        def _():
            for copy in make(e):
                act(copy)

        return carry

    lax.fori_loop(0, count, body, 0)


def page_copies(layer, k_pool, v_pool, slot, k_dst, v_dst, sem):
    return (pltpu.make_async_copy(k_pool.at[slot, layer], k_dst, sem), pltpu.make_async_copy(v_pool.at[slot, layer], v_dst, sem))


def pack_pages_kernel(layers, meta, k_pool, v_pool, *rest):
    outs = rest[:len(layers)]
    stage, in_sem, out_sem = rest[-3:]
    page_len = k_pool.shape[2]
    count = stage.shape[2] // page_len

    def fetch(at):
        def make(e):
            part = pl.ds(e * page_len, page_len)
            return page_copies(layers[at], k_pool, v_pool, meta[0, e], stage.at[at, 0, part], stage.at[at, 1, part], in_sem.at[at])

        return make

    for at in range(len(layers)):
        for_all(count, meta, 0, fetch(at), start)

    def wipe(e, carry):
        @pl.when(meta[0, e] < 0)
        def _():
            for at in range(len(layers)):
                for which in range(2):
                    stage[at, which, pl.ds(e * page_len, page_len)] = jnp.zeros((page_len,) + stage.shape[3:], stage.dtype)

        return carry

    lax.fori_loop(0, count, wipe, 0)
    for at in range(len(layers)):
        for_all(count, meta, 0, fetch(at), wait)
        pltpu.make_async_copy(stage.at[at], outs[at], out_sem.at[at]).start()
    for at in range(len(layers)):
        pltpu.make_async_copy(stage.at[at], outs[at], out_sem.at[at]).wait()


def pack_pages(layers, k_pool, v_pool, slot_of):
    shape = (2, slot_of.shape[0] * k_pool.shape[2]) + k_pool.shape[3:]
    return pl.pallas_call(
        functools.partial(pack_pages_kernel, layers),
        out_shape=[jax.ShapeDtypeStruct(shape, k_pool.dtype)] * len(layers),
        in_specs=[smem_spec(), any_spec(), any_spec()],
        out_specs=[any_spec()] * len(layers),
        scratch_shapes=[pltpu.VMEM((len(layers),) + shape, k_pool.dtype), pltpu.SemaphoreType.DMA((len(layers),)), pltpu.SemaphoreType.DMA((len(layers),))],
        cost_estimate=pl.CostEstimate(flops=10 ** 10, bytes_accessed=10 ** 7, transcendentals=0),
    )(slot_of[None, :].astype(I32), k_pool, v_pool)


def pack_rows_kernel(layers, meta, k_pool, v_pool, *rest):
    outs = rest[:len(layers)]
    pages, stage, in_sem, out_sem = rest[-4:]
    count = pages.shape[1]
    page_len = k_pool.shape[2]

    def fetch(at):
        return lambda e: page_copies(layers[at], k_pool, v_pool, meta[0, e], pages.at[at, e, 0], pages.at[at, e, 1], in_sem.at[at])

    for at in range(len(layers)):
        for_all(count, meta, 0, fetch(at), start)
    nothing = jnp.zeros((page_len,) + stage.shape[3:], stage.dtype)

    def wipe(i, carry):
        for at in range(len(layers)):
            for which in range(2):
                stage[at, which, pl.ds(i * page_len, page_len)] = nothing
        return carry

    lax.fori_loop(0, stage.shape[2] // page_len, wipe, 0)
    for at in range(len(layers)):
        for_all(count, meta, 0, fetch(at), wait)

        def place(e, carry):
            @pl.when(meta[0, e] >= 0)
            def _():
                for which in range(2):
                    stage[at, which, pl.ds(meta[1, e], page_len)] = pages[at, e, which]
                    stage[at, which, pl.ds(meta[1, e] + meta[2, e], page_len)] = nothing

            return carry

        lax.fori_loop(0, count, place, 0)
        pltpu.make_async_copy(stage.at[at], outs[at], out_sem.at[at]).start()
    for at in range(len(layers)):
        pltpu.make_async_copy(stage.at[at], outs[at], out_sem.at[at]).wait()


def pack_rows(layers, k_pool, v_pool, meta, cap, spare=()):
    count = meta.shape[1]
    page_len = k_pool.shape[2]
    shape = (2, cap + page_len) + k_pool.shape[3:]
    outs = [jax.ShapeDtypeStruct(shape, k_pool.dtype)] * len(layers) + [jax.ShapeDtypeStruct(s, k_pool.dtype) for s in spare]
    return pl.pallas_call(
        functools.partial(pack_rows_kernel, layers),
        out_shape=outs,
        in_specs=[smem_spec(), any_spec(), any_spec()],
        out_specs=[any_spec()] * len(outs),
        scratch_shapes=[
            pltpu.VMEM((len(layers), count, 2) + k_pool.shape[2:], k_pool.dtype),
            pltpu.VMEM((len(layers),) + shape, k_pool.dtype),
            pltpu.SemaphoreType.DMA((len(layers),)),
            pltpu.SemaphoreType.DMA((len(layers),)),
        ],
        cost_estimate=pl.CostEstimate(flops=10 ** 10, bytes_accessed=10 ** 7, transcendentals=0),
    )(meta.astype(I32), k_pool, v_pool)


def gate(value):
    def kernel(src, dst):
        dst[...] = src[...]

    return pl.pallas_call(kernel, out_shape=jax.ShapeDtypeStruct(value.shape, value.dtype), name='gate')(value)


LOCAL, MOVED, NEXT, OTHER = range(4)
MOVED_ROWS = 9
NEAR_ROWS = 9


def attend_kernel(layer, seqs, page_len, q_per_kv, unroll, meta, q_ref, new_ref, k_pool, v_pool, moved, near, other, out_ref, k_buf, v_buf, k_sem, v_sem):
    kv_heads, head_dim = k_buf.shape[2:]

    def launch(j, carry):
        for page in range(2):
            kind = meta[2 * page, j]
            index = meta[2 * page + 1, j]

            def both(k_src, v_src):
                dst = pl.ds(page * page_len, page_len)
                pltpu.make_async_copy(k_src, k_buf.at[j, dst], k_sem.at[j]).start()
                pltpu.make_async_copy(v_src, v_buf.at[j, dst], v_sem.at[j]).start()

            @pl.when(kind == LOCAL)
            def _():
                both(k_pool.at[index, layer], v_pool.at[index, layer])

            @pl.when(kind > LOCAL)
            def _():
                part = pl.ds(index, page_len)

                @pl.when(kind == MOVED)
                def _():
                    both(moved.at[0, part], moved.at[1, part])

                @pl.when(kind == NEXT)
                def _():
                    both(near.at[0, part], near.at[1, part])

                @pl.when(kind == OTHER)
                def _():
                    both(other.at[index, 0, layer], other.at[index, 1, layer])
        return carry

    lax.fori_loop(0, seqs, launch, 0)

    rows = STEPS * kv_heads * q_per_kv
    cols = 2 * page_len * kv_heads
    row_id = lax.broadcasted_iota(I32, (rows, cols), 0)
    col_id = lax.broadcasted_iota(I32, (rows, cols), 1)
    row_step = row_id // (kv_heads * q_per_kv)
    own_head = (col_id % kv_heads) == (row_id % (kv_heads * q_per_kv)) // q_per_kv
    lag = jnp.where(own_head, col_id // kv_heads - row_step, 1 << 20)

    def body(i, carry):
        for u in range(unroll):
            j = i * unroll + u
            pltpu.make_async_copy(k_buf.at[j], k_buf.at[j], k_sem.at[j]).wait()
            pltpu.make_async_copy(v_buf.at[j], v_buf.at[j], v_sem.at[j]).wait()
        for u in range(unroll):
            j = i * unroll + u
            length = meta[4, j]
            for step in range(STEPS):
                k_buf[j, length + step] = new_ref[j, 0, step]
                v_buf[j, length + step] = new_ref[j, 1, step]
        ids = [i * unroll + u for u in range(unroll)]
        queries = [jnp.concatenate([q_ref[step, j] for step in range(STEPS)]) for j in ids]
        scores = [lax.dot_general(query, k_buf[j].reshape(cols, head_dim), (((1,), (1,)), ((), ())), preferred_element_type=jnp.float32) for j, query in zip(ids, queries)]
        scores = [jnp.where(lag <= meta[4, j], score * head_dim ** -0.5, -jnp.inf) for j, score in zip(ids, scores)]
        probs = [jnp.exp(score - jnp.max(score, axis=1, keepdims=True)) for score in scores]
        totals = [jnp.sum(prob, axis=1, keepdims=True) for prob in probs]
        outs = [jnp.dot(prob.astype(v_buf.dtype), v_buf[j].reshape(cols, head_dim), preferred_element_type=jnp.float32) / total for j, prob, total in zip(ids, probs, totals)]
        for j, out in zip(ids, outs):
            for step in range(STEPS):
                out_ref[step, j] = out[step * (rows // STEPS):(step + 1) * (rows // STEPS)].astype(out_ref.dtype)
        return carry

    lax.fori_loop(0, seqs // unroll, body, 0)


def attend(layer, queries, new_rows, k_pool, v_pool, moved, near, other, meta):
    seqs = queries.shape[1]
    page_len, kv_heads, head_dim = k_pool.shape[2:]
    num_heads = queries.shape[2]
    buf = pltpu.VMEM((seqs, 2 * page_len, kv_heads, head_dim), k_pool.dtype)
    return pl.pallas_call(
        functools.partial(attend_kernel, layer, seqs, page_len, num_heads // kv_heads, 8),
        out_shape=jax.ShapeDtypeStruct(queries.shape, queries.dtype),
        in_specs=[smem_spec(), vmem_spec(), vmem_spec()] + [any_spec()] * 5,
        out_specs=vmem_spec(),
        scratch_shapes=[buf, buf, pltpu.SemaphoreType.DMA((seqs,)), pltpu.SemaphoreType.DMA((seqs,))],
        cost_estimate=pl.CostEstimate(flops=10 ** 10, bytes_accessed=10 ** 7, transcendentals=10 ** 6),
    )(meta, queries, new_rows, k_pool, v_pool, moved, near, other)


COPY_SLOTS = 16


def copy_kernel(k_pool, v_pool, k_out, v_out, stage, in_sem, out_sem):
    chunks = k_pool.shape[0] // COPY_SLOTS
    for pool, which in ((k_pool, 0), (v_pool, 1)):
        for c in range(chunks):
            part = pl.ds(c * COPY_SLOTS, COPY_SLOTS)
            pltpu.make_async_copy(pool.at[part], stage.at[which, part], in_sem.at[which, c]).start()
    for pool, out, which in ((k_pool, k_out, 0), (v_pool, v_out, 1)):
        for c in range(chunks):
            part = pl.ds(c * COPY_SLOTS, COPY_SLOTS)
            pltpu.make_async_copy(pool.at[part], stage.at[which, part], in_sem.at[which, c]).wait()
            pltpu.make_async_copy(stage.at[which, part], out.at[part], out_sem.at[which, c]).start()
    for out, which in ((k_out, 0), (v_out, 1)):
        for c in range(chunks):
            part = pl.ds(c * COPY_SLOTS, COPY_SLOTS)
            pltpu.make_async_copy(stage.at[which, part], out.at[part], out_sem.at[which, c]).wait()


def copy_pools(k_pool, v_pool):
    chunks = k_pool.shape[0] // COPY_SLOTS
    pool = jax.ShapeDtypeStruct(k_pool.shape, k_pool.dtype)
    return pl.pallas_call(
        copy_kernel,
        out_shape=[pool, pool],
        in_specs=[any_spec(), any_spec()],
        out_specs=[any_spec(), any_spec()],
        scratch_shapes=[pltpu.VMEM((2,) + k_pool.shape, k_pool.dtype), pltpu.SemaphoreType.DMA((2, chunks)), pltpu.SemaphoreType.DMA((2, chunks))],
        cost_estimate=pl.CostEstimate(flops=10 ** 10, bytes_accessed=10 ** 7, transcendentals=0),
        name='copy_pools',
    )(k_pool, v_pool)


def finish_kernel(layers, slots, entries, mig, owner, k_in, v_in, *rest):
    del k_in, v_in
    moved, own, prev, far = (rest[i * layers:(i + 1) * layers] for i in range(4))
    k_out, v_out, zeros, stage, row_stage, far_stage, zero_sem, in_sem, out_sem, row_in_sem, row_sem, far_sem = rest[4 * layers:]
    page_len = k_out.shape[2]
    seats = own[0].shape[0]

    def fetch(e):
        part = pl.ds(e * page_len, page_len)
        return [pltpu.make_async_copy(moved[layer].at[which, part], stage.at[e, layer, which], in_sem.at[e]) for layer in range(layers) for which in range(2)]

    def put(e):
        return [pltpu.make_async_copy(stage.at[e, layer, which], out.at[mig[1, e], layer], out_sem.at[0]) for layer in range(layers) for which, out in enumerate((k_out, v_out))]

    def clear(e):
        return [pltpu.make_async_copy(zeros, out.at[mig[0, e]], zero_sem.at[0]) for out in (k_out, v_out)]

    def load(layer):
        return (pltpu.make_async_copy(own[layer], row_stage.at[layer, pl.ds(0, seats)], row_in_sem.at[layer]),
                pltpu.make_async_copy(prev[layer], row_stage.at[layer, pl.ds(seats, seats)], row_in_sem.at[layer]))

    def fill(j):
        dst = pl.ds(owner[1, j], STEPS)
        return [pltpu.make_async_copy(row_stage.at[layer, owner[0, j], which], out.at[j, layer, dst], row_sem.at[0]) for layer in range(layers) for which, out in enumerate((k_out, v_out))]

    for_all(entries, mig, 1, fetch, start)
    for layer in range(layers):
        for copy in load(layer):
            copy.start()
    zeros[...] = jnp.zeros_like(zeros)

    def relay(e, carry):
        @pl.when(mig[1, e] >= 0)
        def _():
            for copy in fetch(e):
                copy.wait()
            for copy in put(e):
                copy.start()

        return carry

    lax.fori_loop(0, entries, relay, 0)
    for_all(entries, mig, 0, clear, start)
    for_all(entries, mig, 1, put, wait)
    for layer in range(layers):
        for copy in load(layer):
            copy.wait()
    for_all(slots, owner, 0, fill, start)

    def from_far(j, carry):
        @pl.when(owner[2, j] >= 0)
        def _():
            dst = pl.ds(owner[1, j], STEPS)
            for layer in range(layers):
                copy = pltpu.make_async_copy(far[layer].at[owner[2, j]], far_stage, far_sem.at[0])
                copy.start()
                copy.wait()
                for which, out in enumerate((k_out, v_out)):
                    copy = pltpu.make_async_copy(far_stage.at[which], out.at[j, layer, dst], far_sem.at[0])
                    copy.start()
                    copy.wait()

        return carry

    lax.fori_loop(0, slots, from_far, 0)
    for_all(entries, mig, 0, clear, wait)
    for_all(slots, owner, 0, fill, wait)


def finish_pools(k_pool, v_pool, moved, own, prev, far, mig, owner):
    slots, layers = k_pool.shape[:2]
    entries = mig.shape[1]
    pool = jax.ShapeDtypeStruct(k_pool.shape, k_pool.dtype)
    row_shape = own[0].shape
    return pl.pallas_call(
        functools.partial(finish_kernel, layers, slots, entries),
        out_shape=[pool, pool],
        in_specs=[smem_spec(), smem_spec()] + [any_spec()] * (2 + 4 * layers),
        out_specs=[any_spec(), any_spec()],
        input_output_aliases={2: 0, 3: 1},
        scratch_shapes=[
            pltpu.VMEM(k_pool.shape[1:], k_pool.dtype),
            pltpu.VMEM((entries, layers, 2) + k_pool.shape[2:], k_pool.dtype),
            pltpu.VMEM((layers, 2 * row_shape[0]) + row_shape[1:], k_pool.dtype),
            pltpu.VMEM(row_shape[1:], k_pool.dtype),
            pltpu.SemaphoreType.DMA((1,)),
            pltpu.SemaphoreType.DMA((entries,)),
            pltpu.SemaphoreType.DMA((1,)),
            pltpu.SemaphoreType.DMA((layers,)),
            pltpu.SemaphoreType.DMA((1,)),
            pltpu.SemaphoreType.DMA((1,)),
        ],
        cost_estimate=pl.CostEstimate(flops=10 ** 10, bytes_accessed=10 ** 7, transcendentals=0),
        name='finish_pools',
    )(mig, owner, k_pool, v_pool, *moved, *own, *prev, *far)


def dense(hidden, weight):
    return jnp.dot(hidden, weight, preferred_element_type=jnp.float32)


def pair_mlp(hidden, w_up, w_down, layer, core, pairs):
    rows = hidden.shape[0]
    width, full = w_up.shape[1:]
    half = full // 2
    both = jnp.concatenate([hidden, lax.ppermute(hidden, 'kv', pairs)])
    up_proj = dense(both, lax.dynamic_slice(w_up, (layer, 0, core * half), (1, width, half))[0]).astype(jnp.bfloat16)
    act = jax.nn.gelu(up_proj.astype(jnp.float32), approximate=True).astype(jnp.bfloat16)
    part = dense(act, lax.dynamic_slice(w_down, (layer, core * half, 0), (1, half, width))[0])
    rest = lax.ppermute(part[rows:], 'kv', pairs)
    return (hidden.astype(jnp.float32) + (part[:rows] + rest)).astype(jnp.bfloat16)


def shift_by(count, distance):
    return [(i, (i + distance) % count) for i in range(count)]


ROUND_PAGES = 8


def other_pages(k_pool, v_pool, buffer, src, slot, dst, target, wanted, me, group_size):
    entry_ids = jnp.arange(src.shape[0])
    rank = masked_pick((src[None, :] == src[:, None]) & wanted[None, :] & (entry_ids[None, :] < entry_ids[:, None]), 1)
    most = jnp.max(jnp.where(wanted, rank + 1, 0))
    seat = jnp.where(wanted, src * src.shape[0] + rank, -1)

    def body(carry):
        done, buf = carry
        seats = ((jnp.arange(group_size) * src.shape[0])[:, None] + done + jnp.arange(ROUND_PAGES)[None, :]).reshape(-1)
        hit = seat[None, :] == seats[:, None]
        seat_slot = masked_pick(hit, slot[None, :])
        seat_target = jnp.where(jnp.any(hit & (dst == me)[None, :], axis=1), masked_pick(hit, target[None, :]), buf.shape[0])
        my_slots = lax.dynamic_slice_in_dim(seat_slot, me * ROUND_PAGES, ROUND_PAGES)
        pages = jnp.stack([jnp.take(k_pool, my_slots, axis=0), jnp.take(v_pool, my_slots, axis=0)], axis=1)
        gathered = lax.all_gather(pages, 'kv', axis=0, tiled=True)
        return done + ROUND_PAGES, buf.at[seat_target].set(gathered, mode='drop')

    return lax.while_loop(lambda carry: carry[0] < most, body, (jnp.zeros((), I32), buffer))[1]


def solution(mesh):
    group_size = mesh.shape['kv']
    pool_spec = P(('rep', 'kv'))
    tok_spec = P(None, ('rep', 'kv'), None)

    def device_fn(embeds, w_query, w_key, w_value, w_out, w_up, w_down, k_pool, v_pool, new_table, seq_lens, mig_src, mig_dst):
        me = lax.axis_index('kv')
        slots, layers, page_len, kv_heads, head_dim = k_pool.shape
        per_dev, width = embeds.shape[1:]
        seq_count, page_count = new_table.shape
        num_heads = w_query.shape[2] // head_dim
        pairs = [(i, i ^ 1) for i in range(group_size)]

        remap = new_table[:, :, None] == mig_dst
        is_moved = jnp.any(remap, axis=-1)
        old_table = jnp.where(is_moved, masked_pick(remap, mig_src), new_table)
        page_src = old_table // slots
        page_slot = old_table % slots

        page_ids = jnp.arange(page_count, dtype=I32)[None, :]
        page_rows = jnp.where(page_ids == 0, page_len, seq_lens[:, None] - page_len)

        src_dev, dst_dev = mig_src // slots, mig_dst // slots
        clear_slot = jnp.where(src_dev == me, mig_src % slots, -1)
        fill_slot = jnp.where(dst_dev == me, mig_dst % slots, -1)
        mig_meta = jnp.stack([clear_slot, fill_slot]).astype(I32)
        moved_cap = mig_src.shape[0] * MOVED_ROWS
        moved_rows = jnp.sum(jnp.where(remap, page_rows[:, :, None], 0), axis=(0, 1))
        moved_first = excl_cumsum(moved_rows)
        moved_fits = moved_first + moved_rows <= moved_cap
        moved_meta = jnp.stack([jnp.where(moved_fits, clear_slot, -1), moved_first, moved_rows])
        moved_out = pack_rows((0,), k_pool, v_pool, moved_meta, moved_cap)[0]
        moved_out, new_table, page_src, page_slot = lax.optimization_barrier((moved_out, new_table, page_src, page_slot))
        moved = [lax.psum(moved_out, 'kv')]

        dev, pos = place_sequences(page_src[:, 0], group_size, per_dev)
        place = dev * per_dev + pos

        is_local = page_src == dev[:, None]
        in_moved = jnp.any(remap & moved_fits, axis=-1) & ~is_local
        same_dev_earlier = (dev[None, :] == dev[:, None]) & (pos[None, :] < pos[:, None])
        near_cap = per_dev * NEAR_ROWS
        by_next = (page_src[:, 1] == (dev + 1) % group_size) & ~is_moved[:, 1]
        near_first = masked_pick(same_dev_earlier & by_next[None, :], page_rows[None, :, 1])
        by_next = by_next & (near_first + page_rows[:, 1] <= near_cap)
        is_near = (page_ids == 1) & by_next[:, None]

        prev = (me + group_size - 1) % group_size
        prev_seat = prev * per_dev + jnp.arange(per_dev, dtype=I32)
        from_here = (place[None, :] == prev_seat[:, None]) & by_next[None, :]
        near_facts = jnp.stack([page_slot[:, 1] + 1, near_first, page_rows[:, 1]])
        near_meta = masked_pick(from_here[None, :, :], near_facts[:, None, :]) - jnp.array([[1], [0], [0]])
        other_shape = (per_dev * page_count, 2) + k_pool.shape[1:]
        far_shape = (seq_count, 2, STEPS, kv_heads, head_dim)
        my_dev = lax.dynamic_slice_in_dim(dev, me * per_dev, per_dev)
        my_pos = lax.dynamic_slice_in_dim(pos, me * per_dev, per_dev)
        home = jnp.arange(seq_count, dtype=I32) // per_dev
        distance = (dev - home) % group_size
        my_distance = (my_dev - me) % group_size
        at_pos = my_pos[None, :] == jnp.arange(per_dev, dtype=I32)[:, None]
        counts = jnp.sum(distance[None, :] == jnp.arange(group_size, dtype=I32)[:, None], axis=1)
        most = jnp.argmax(counts).astype(I32)
        all_same = counts[most] == seq_count

        def send_embeds(step_away):
            sel = (at_pos & (my_distance == step_away)[None, :]).astype(embeds.dtype)
            rows = jnp.einsum('pb,tbd->tpd', sel, embeds, preferred_element_type=jnp.float32).astype(embeds.dtype)
            return lax.ppermute(rows, 'kv', shift_by(group_size, step_away)) if step_away else rows

        def send_most(step_away, near_meta, clear_slot):
            rows = send_embeds(step_away)
            packed = pack_rows(tuple(range(layers)), k_pool, v_pool, near_meta, near_cap, [other_shape, far_shape, far_shape])
            return rows, packed, copy_pools(k_pool, v_pool), pack_pages(tuple(range(layers)), k_pool, v_pool, clear_slot)

        def send_rest(hidden):
            for step_away in range(group_size):
                hidden = lax.cond((counts[step_away] > 0) & (most != step_away), lambda rows, step_away=step_away: rows + send_embeds(step_away), lambda rows: rows, hidden)
            return hidden

        hidden, packed, (k_base, v_base), full_out = lax.switch(most, [functools.partial(send_most, step_away) for step_away in range(group_size)], gate(near_meta.astype(I32)), clear_slot)
        *near_out, other, far_0, far_1 = packed
        full_out = list(full_out)
        hidden = lax.optimization_barrier(lax.while_loop(lambda carry: carry[0], lambda carry: (jnp.zeros((), bool), send_rest(carry[1])), (~all_same, hidden))[1])
        hidden = hidden.reshape(STEPS * per_dev, width)
        near = [lax.ppermute(near_out[0], 'kv', shift_by(group_size, -1))]

        wanted = ~(is_local | in_moved | is_near)
        kind = jnp.where(is_local, LOCAL, jnp.where(in_moved, MOVED, jnp.where(is_near, NEXT, OTHER)))
        target = pos[:, None] * page_count + page_ids
        entry_dst = jnp.broadcast_to(dev[:, None], page_src.shape)

        def fetch_other(buffer):
            return other_pages(k_pool, v_pool, buffer, page_src.reshape(-1), page_slot.reshape(-1), entry_dst.reshape(-1), target.reshape(-1), wanted.reshape(-1), me, group_size)

        other, moved[0] = lax.optimization_barrier((other, moved[0]))
        other = lax.cond(jnp.any(wanted), fetch_other, lambda buffer: buffer, other)
        mine = place[None, :] == (me * per_dev + jnp.arange(per_dev, dtype=I32))[:, None]
        facts = []
        for layer in range(layers):
            moved_at = masked_pick(remap, moved_first) if layer == 0 else masked_pick(remap, jnp.arange(mig_src.shape[0], dtype=I32)) * page_len
            index = jnp.where(is_local, page_slot, jnp.where(in_moved, moved_at, jnp.where(is_near, near_first[:, None], target)))
            facts.append(jnp.stack([kind[:, 0], index[:, 0], kind[:, 1], index[:, 1], seq_lens]))
        attend_meta = masked_pick(mine[None, None, :, :], jnp.stack(facts)[:, :, None, :]).astype(I32)

        row_dst = new_table[:, 1] // slots
        is_far = (row_dst != dev) & (row_dst != (dev + 1) % group_size)
        writes = new_table[None, :, 1] == (me * slots + jnp.arange(slots, dtype=I32))[:, None]
        owner_facts = jnp.stack([jnp.where(is_far, 0, 1 + pos + jnp.where(row_dst == dev, 0, per_dev)), seq_lens - page_len, jnp.where(is_far, 1 + place, 0)])
        owner_meta = (masked_pick(writes[None, :, :], owner_facts[:, None, :]) - jnp.array([[1], [0], [1]])).astype(I32)

        own_rows, prev_rows = [], []
        for layer in range(layers):
            queries = dense(hidden, w_query[layer]).astype(jnp.bfloat16)
            new_keys = dense(hidden, w_key[layer]).astype(jnp.bfloat16)
            new_vals = dense(hidden, w_value[layer]).astype(jnp.bfloat16)
            rows = jnp.stack([new_keys, new_vals]).reshape(2, STEPS, per_dev, kv_heads, head_dim).transpose(2, 0, 1, 3, 4)
            own_rows.append(rows)
            prev_rows.append(lax.ppermute(rows, 'kv', shift_by(group_size, 1)))
            q_rows = queries.reshape(STEPS, per_dev, num_heads, head_dim)
            if layer == 0:
                for after in range(layers - 1, -1, -1):
                    full_out[after], moved[-1] = lax.optimization_barrier((full_out[after], moved[-1]))
                    moved.append(lax.psum(full_out[after], 'kv'))
                moved = [moved[0]] + moved[:0:-1]
            if layer + 1 < layers:
                near_next, near[layer] = lax.optimization_barrier((near_out[layer + 1], near[layer]))
                near.append(lax.ppermute(near_next, 'kv', shift_by(group_size, -1)))
            attn = attend(layer, q_rows, rows, k_pool, v_pool, moved[layer if layer == 0 else layer + 1], near[layer], other, attend_meta[layer]).reshape(STEPS * per_dev, num_heads * head_dim)
            hidden = (hidden.astype(jnp.float32) + dense(attn, w_out[layer])).astype(jnp.bfloat16)
            hidden = pair_mlp(hidden, w_up, w_down, layer, me % 2, pairs)

        hidden, moved[1], *far_in = lax.optimization_barrier((hidden, moved[1], *own_rows))
        far_rows = lax.cond(jnp.any(is_far), lambda own, far: [lax.all_gather(rows, 'kv', axis=0, tiled=True) for rows in own], lambda own, far: far, far_in, [far_0, far_1])
        hidden = lax.optimization_barrier(hidden).reshape(STEPS, per_dev, width)

        def bring_home(step_away, total):
            rows = lax.ppermute(hidden, 'kv', shift_by(group_size, -step_away)) if step_away else hidden
            sel = (at_pos & (my_distance == step_away)[None, :]).astype(hidden.dtype)
            return total + jnp.einsum('pb,tpd->tbd', sel, rows, preferred_element_type=jnp.float32).astype(hidden.dtype)

        def bring_most(step_away, k_base, v_base):
            rows = lax.ppermute(hidden, 'kv', shift_by(group_size, -step_away)) if step_away else hidden
            k_out, v_out = finish_pools(k_base, v_base, moved[1:], own_rows, prev_rows, far_rows, mig_meta, owner_meta)
            sel = (at_pos & (my_distance == step_away)[None, :]).astype(hidden.dtype)
            return jnp.einsum('pb,tpd->tbd', sel, rows, preferred_element_type=jnp.float32).astype(hidden.dtype), k_out, v_out

        y_out, k_out, v_out = lax.switch(most, [functools.partial(bring_most, step_away) for step_away in range(group_size)], k_base, v_base)

        def bring_rest(y_out):
            for step_away in range(group_size):
                y_out = lax.cond((counts[step_away] > 0) & (most != step_away), functools.partial(bring_home, step_away), lambda same: same, y_out)
            return y_out

        y_out = lax.cond(all_same, lambda same: same, bring_rest, y_out)
        return y_out, k_out, v_out

    return jax.shard_map(device_fn, mesh=mesh, in_specs=(tok_spec, P(), P(), P(), P(), P(), P(), pool_spec, pool_spec, P('rep', None), P('rep'), P('rep'), P('rep')), out_specs=(tok_spec, pool_spec, pool_spec), check_vma=False)
```
